32 devices in a mesh: fsdp: 4 (over z), ctx: 4 (over x, core), tp: 2 (over y).
Axes of the slice: x: 2, y: 2, z: 4, core: 2. Of those that a mesh axis runs over, the one named last changes fastest.
Arguments:
- layer_in: bfloat16 [4, 1024, 1024], P('fsdp', 'ctx'), may hold values from -6 to 6
- segment_ids: int32 [4, 1024], P('fsdp', 'ctx'), may hold values from 0 to 18, as said below
- valid_mask: int32 [4, 1024], P('fsdp', 'ctx'), may hold values from 0 to 1, as said below
- teacher: bfloat16 [4, 1024, 1024], P('fsdp', 'ctx'), may hold values from -6 to 6
- attn_gain: bfloat16 [1024], P('fsdp'), may hold values from 0.099609375 to 1.8984375
- w_query: bfloat16 [1024, 256], P('fsdp', 'tp'), may hold values from -0.1875 to 0.1875
- w_key: bfloat16 [1024, 256], P('fsdp', 'tp'), may hold values from -0.1875 to 0.1875
- w_value: bfloat16 [1024, 1024], P('fsdp', 'tp'), may hold values from -0.1875 to 0.1875
- w_out: bfloat16 [1024, 1024], P('tp', 'fsdp'), may hold values from -2 to 2
- ffn_gain: bfloat16 [1024], P('fsdp'), may hold values from 0.099609375 to 1.8984375
- w_gate: bfloat16 [1024, 2752], P('fsdp', 'tp'), may hold values from -0.1875 to 0.1875
- w_up: bfloat16 [1024, 2752], P('fsdp', 'tp'), may hold values from -0.1875 to 0.1875
- w_down: bfloat16 [2752, 1024], P('tp', 'fsdp'), may hold values from -0.109375 to 0.109375
Outputs:
- layer_out: bfloat16 [4, 1024, 1024], P('fsdp', 'ctx')
- grad_in: bfloat16 [4, 1024, 1024], P('fsdp', 'ctx')
- grad_attn_gain: float32 [1024], P('fsdp')
- grad_query: float32 [1024, 256], P('fsdp', 'tp')
- grad_key: float32 [1024, 256], P('fsdp', 'tp')
- grad_value: float32 [1024, 1024], P('fsdp', 'tp')
- grad_out: float32 [1024, 1024], P('tp', 'fsdp')
- grad_ffn_gain: float32 [1024], P('fsdp')
- grad_gate: float32 [1024, 2752], P('fsdp', 'tp')
- grad_up: float32 [1024, 2752], P('fsdp', 'tp')
- grad_down: float32 [2752, 1024], P('tp', 'fsdp')
- loss_value: float32 [], replicated
The draws below stay inside these ranges and needn't reach their ends.
Inputs may be any that keep to these rules, and one draw needn't show every extreme that they name: `segment_ids`: within each sequence the ids of valid tokens start at 0 and rise by 0 or 1 from one token to the next; equal ids in a sequence mark one document. Padding tokens carry the largest id, which no document has. `valid_mask`: in each sequence the valid tokens come first; the padding tokens after them, where there are any.
All inputs are finite; a program needn't handle non-finite values.
Results may differ from the reference program's by a relative error of at most 0.014.
Values may be sent and summed in bfloat16 or wider, within the bound.
A program may use at most 128 MiB of HBM per device.

```python
import math
import jax
import jax.numpy as jnp
from jax import lax

D = 1024
HEADS = 16
FEAT = 16
HEAD_V = 64
FF = 2752
SEQ_LEN = 1024
SEQS = 4
DOC_MIN = 60
DOC_MAX = 800


def draw_layout(key):
    doc_key, pad_key = jax.random.split(jax.random.fold_in(key, 11))
    most_docs = SEQ_LEN // DOC_MIN + 1
    doc_lengths = jax.random.randint(doc_key, (SEQS, most_docs), DOC_MIN, DOC_MAX + 1)
    doc_ends = jnp.cumsum(doc_lengths, axis=1)
    places = jnp.arange(SEQ_LEN, dtype=jnp.int32)
    doc_index = jnp.sum((doc_ends[:, None, :] <= places[None, :, None]).astype(jnp.int32), axis=2)
    rising = SEQ_LEN // 3 + (SEQ_LEN - SEQ_LEN // 3) * jnp.arange(SEQS, dtype=jnp.int32) // max(SEQS - 1, 1)
    jitter = jax.random.randint(pad_key, (SEQS,), 0, SEQ_LEN // 8 + 1)
    live_len = jnp.minimum(rising + jitter, SEQ_LEN)
    valid = (places[None, :] < live_len[:, None]).astype(jnp.int32)
    pad_id = jnp.int32(SEQ_LEN // DOC_MIN + 1)
    segment = jnp.where(valid == 1, doc_index, pad_id)
    return (segment.astype(jnp.int32), valid)


def draw_segment_ids(key, part):
    return draw_layout(key)[0]


def draw_valid_mask(key, part):
    return draw_layout(key)[1]


def level_of(own_key, shape, cuts, low, top_value):
    def one(position, blocks):
        draws = jax.random.uniform(jax.random.fold_in(jax.random.fold_in(own_key, 6), position), (blocks,), jnp.float32, low / len(cuts), top_value / len(cuts))
        return jnp.repeat(jnp.exp(draws), shape[position] // blocks).reshape((-1,) + (1,) * (len(shape) - position - 1))

    gain = one(*cuts[0])
    for cut in cuts[1:]:
        gain = gain * one(*cut)
    return gain


def centred(own_key, dims, deviation, most, pieces=(), held_as=jnp.bfloat16):
    drawn = jax.random.normal(own_key, dims, jnp.float32) * deviation
    if len(pieces) > 0:
        drawn = level_of(own_key, dims, pieces, -0.22, 0.18) * drawn
    return jnp.clip(drawn, min=-most, max=most).astype(held_as)


def setup_inputs(seed: int = 0) -> dict:
    streams_of = jax.random.split(jax.random.key(seed), 14)
    return {
        "layer_in": centred(streams_of[0], (SEQS, SEQ_LEN, D), 1.0, 6.0, ((0, 4), (1, 4))),
        "segment_ids": draw_segment_ids(jax.random.fold_in(streams_of[13], 71), 0),
        "valid_mask": draw_valid_mask(jax.random.fold_in(streams_of[13], 71), 0),
        "teacher": centred(streams_of[3], (SEQS, SEQ_LEN, D), 1.0, 6.0, ((0, 4), (1, 4))),
        "attn_gain": jnp.clip(1.0 + 0.18 * jax.random.normal(streams_of[4], (D,), jnp.float32), 0.099609375, 1.8984375).astype(jnp.bfloat16),
        "w_query": centred(streams_of[5], (D, HEADS * FEAT), D ** -0.5, 0.1875, ((0, 4), (1, 2))),
        "w_key": centred(streams_of[6], (D, HEADS * FEAT), D ** -0.5, 0.1875, ((0, 4), (1, 2))),
        "w_value": centred(streams_of[7], (D, HEADS * HEAD_V), D ** -0.5, 0.1875, ((0, 4), (1, 2))),
        "w_out": centred(streams_of[8], (HEADS * HEAD_V, D), (max(HEADS * HEAD_V // 128, 1)) ** -0.5, 2.0, ((0, 2), (1, 4))),
        "ffn_gain": jnp.clip(1.0 + 0.18 * jax.random.normal(streams_of[9], (D,), jnp.float32), 0.099609375, 1.8984375).astype(jnp.bfloat16),
        "w_gate": centred(streams_of[10], (D, FF), D ** -0.5, 0.1875, ((0, 4), (1, 2))),
        "w_up": centred(streams_of[11], (D, FF), D ** -0.5, 0.1875, ((0, 4), (1, 2))),
        "w_down": centred(streams_of[12], (FF, D), FF ** -0.5, 0.109375, ((0, 2), (1, 4))),
    }


EPSILON = 1e-05
HIGH = lax.Precision.HIGHEST

@jax.custom_vjp
def low(v):
    return lax.optimization_barrier(v.astype(jnp.bfloat16)).astype(jnp.float32)

@jax.custom_vjp
def low_back(v):
    return v

def low_keep(v):
    return (low(v), None)

def low_pass(kept, grad):
    return (grad,)

def back_keep(v):
    return (v, None)

def back_low(kept, grad):
    return (low(grad),)
low.defvjp(low_keep, low_pass)
low_back.defvjp(back_keep, back_low)

def matmul(left_side, right_side):
    return jnp.dot(left_side, right_side, precision=HIGH, preferred_element_type=jnp.float32)

def rms_norm(values_in, gain_vec):
    return values_in * lax.rsqrt(lax.optimization_barrier(jnp.mean(values_in * values_in, axis=-1, keepdims=True)) + EPSILON) * gain_vec

def sequence_mix(operands):
    query_rows, key_rows, value_rows, segment = operands
    scores = jnp.einsum('ihf,jhf->hij', query_rows, key_rows, precision=HIGH) * 0.25
    kernel = 1.0 + scores + 0.5 * scores * scores
    places = jnp.arange(segment.shape[0])
    allowed = (places[:, None] >= places[None, :]) & (segment[:, None] == segment[None, :])
    kernel = jnp.where(allowed[None], kernel, 0.0)
    numerator = jnp.einsum('hij,jhv->ihv', kernel, value_rows, precision=HIGH)
    denominator = jnp.einsum('hij->ih', kernel)
    return numerator / denominator[:, :, None]

def forward(weights, block_in, block_ids):
    attn_gain, w_query, w_key, w_value, w_out, ffn_gain, w_gate, w_up, w_down = weights
    group_size, seq_len, model_width = block_in.shape
    rows_in = block_in.reshape(group_size * seq_len, model_width)
    normed_one = low(rms_norm(rows_in, attn_gain))
    query_rows = low_back(matmul(normed_one, w_query)).reshape(group_size, seq_len, HEADS, FEAT)
    key_rows = low_back(matmul(normed_one, w_key)).reshape(group_size, seq_len, HEADS, FEAT)
    value_rows = low_back(matmul(normed_one, w_value)).reshape(group_size, seq_len, HEADS, HEAD_V)
    attended = lax.map(jax.checkpoint(sequence_mix), (query_rows, key_rows, value_rows, block_ids))
    mixed_heads = low(attended.reshape(group_size * seq_len, HEADS * HEAD_V))
    middle = rows_in + low_back(matmul(mixed_heads, w_out))
    normed_two = low(rms_norm(middle, ffn_gain))
    gate_rows = low_back(matmul(normed_two, w_gate))
    up_rows = low_back(matmul(normed_two, w_up))
    hidden = low(jax.nn.silu(gate_rows) * up_rows)
    output = middle + low_back(matmul(hidden, w_down))
    return output.reshape(group_size, seq_len, model_width)

def reference(layer_in, segment_ids, valid_mask, teacher, attn_gain, w_query, w_key, w_value, w_out, ffn_gain, w_gate, w_up, w_down):
    weights = tuple((member.astype(jnp.float32) for member in (attn_gain, w_query, w_key, w_value, w_out, ffn_gain, w_gate, w_up, w_down)))
    group_size = math.gcd(SEQS, max(1, 4096 // SEQ_LEN))
    block_count = SEQS // group_size

    def split_blocks(array_in):
        return array_in.reshape((block_count, group_size) + array_in.shape[1:])

    def step_block(totals, operands):
        block_in, block_ids, block_valid, block_teacher = operands

        def bound_forward(weight_set, inputs_now):
            return forward(weight_set, inputs_now, block_ids)
        output, pullback = jax.vjp(bound_forward, weights, block_in.astype(jnp.float32))
        weight_rows = block_valid.astype(jnp.float32)[:, :, None]
        misfit = (output - block_teacher.astype(jnp.float32)) * weight_rows
        grad_weights, grad_inputs = pullback(misfit)
        summed = tuple((old_sum + new_term for old_sum, new_term in zip(totals[0], grad_weights)))
        carried = (summed, totals[1] + jnp.sum(misfit * misfit), totals[2] + jnp.sum(weight_rows))
        return (carried, (output.astype(jnp.bfloat16), grad_inputs.astype(jnp.bfloat16)))
    initial = (tuple((jnp.zeros_like(member) for member in weights)), jnp.zeros((), jnp.float32), jnp.zeros((), jnp.float32))
    operands = (split_blocks(layer_in), split_blocks(segment_ids), split_blocks(valid_mask), split_blocks(teacher))
    (grad_sums, total_sq, total_valid), (outputs, grad_inputs) = lax.scan(step_block, initial, operands)
    loss_value = total_sq / (total_valid * D)
    layer_out = outputs.reshape(SEQS, SEQ_LEN, D)
    grad_in = grad_inputs.reshape(SEQS, SEQ_LEN, D)
    return (layer_out, grad_in, grad_sums[0], grad_sums[1], grad_sums[2], grad_sums[3], grad_sums[4], grad_sums[5], grad_sums[6], grad_sums[7], grad_sums[8], loss_value)
```

```python
from functools import partial
import functools
import math

import jax
import jax.numpy as jnp
from jax import lax
from jax.experimental import pallas as pl
from jax.experimental.pallas import tpu as pltpu
from jax.sharding import PartitionSpec as P

FEAT = 16
HEAD_V = 64


EPSILON = 1e-05
HIGH = lax.Precision.HIGHEST
QUAD_SCALE = 1.0 / (4.0 * math.sqrt(2.0))


def entering(x, axis, join, neutral):
    place = lax.axis_index(axis)
    gathered = jax.tree.map(
        lambda a, kind: lax.all_gather(a.astype(kind), axis),
        x,
        (jnp.bfloat16, jnp.bfloat16, jnp.bfloat16),
    )
    state = jax.tree.map(lambda a, e: jnp.zeros_like(a) + jnp.asarray(e, a.dtype), x, neutral)

    def one(lap, state):
        return join(
            state,
            jax.tree.map(
                lambda a, own: lax.dynamic_index_in_dim(a, lap, 0, False).astype(own.dtype),
                gathered,
                x,
            ),
        )

    return lax.fori_loop(0, place, one, state)


def entering_2(x, axis, combine, identity):
    devices, here = (lax.axis_size(axis), lax.axis_index(axis))
    everything = jax.tree.map(
        lambda part, kind: lax.all_gather(part.astype(kind), axis),
        x,
        jax.tree.map(lambda a: jnp.bfloat16 if a.dtype == jnp.float32 else a.dtype, x),
    )
    start = jax.tree.map(
        lambda part, zero: jnp.broadcast_to(jnp.asarray(zero, part.dtype), part.shape), x, identity
    )

    def lap(k, before):
        at = devices - 1 - k
        reached = at > here
        new = combine(
            before, jax.tree.map(lambda part, own: part[at].astype(own.dtype), everything, x)
        )
        return jax.tree.map(lambda a, b: jnp.where(reached, a, b), new, before)

    return lax.fori_loop(0, devices, lap, start)


def product(left_side, right_side):
    return jnp.dot(left_side, right_side, preferred_element_type=jnp.float32)


def product_left_t(left_side, right_side):
    return lax.dot_general(
        left_side, right_side, (((0,), (0,)), ((), ())), preferred_element_type=jnp.float32
    )


def product_right_t(left_side, right_side):
    return lax.dot_general(
        left_side, right_side, (((1,), (1,)), ((), ())), preferred_element_type=jnp.float32
    )


def features(vectors):
    lead_dims = vectors.shape[:-1]
    feat_width = vectors.shape[-1]
    square = (vectors[..., :, None] * vectors[..., None, :]).reshape(
        lead_dims + (feat_width * feat_width,)
    )
    return jnp.concatenate(
        [jnp.ones(lead_dims + (1,), jnp.float32), 0.5 * vectors, QUAD_SCALE * square], axis=-1
    )


def attend(query_rows, key_rows, value_rows, prev_state, prev_norm, segment, prev_id):
    scores = jnp.einsum("slhf,smhf->shlm", query_rows, key_rows, precision=HIGH) * 0.25
    kernel = 1.0 + scores + 0.5 * scores * scores
    places = jnp.arange(segment.shape[1])
    allowed = (places[:, None] >= places[None, :])[None] & (
        segment[:, :, None] == segment[:, None, :]
    )
    kernel = jnp.where(allowed[:, None], kernel, 0.0)
    carried = (segment.astype(jnp.float32) == prev_id[:, None]).astype(jnp.float32)
    mapped = features(query_rows) * carried[:, :, None, None]
    numerator = jnp.einsum("shlm,smhv->slhv", kernel, value_rows, precision=HIGH) + jnp.einsum(
        "slht,shtv->slhv", mapped, prev_state, precision=HIGH
    )
    denominator = jnp.einsum("shlm->slh", kernel) + jnp.einsum(
        "slht,sht->slh", mapped, prev_norm, precision=HIGH
    )
    return numerator / denominator[..., None]


def summarize(key_rows, value_rows, segment):
    closing = (segment == segment[:, -1:]).astype(jnp.float32)
    mapped = features(key_rows) * closing[:, :, None, None]
    return (
        jnp.einsum("slht,slhv->shtv", mapped, value_rows, precision=HIGH),
        jnp.sum(mapped, axis=1),
    )


def rms_forward(values_in, gain_vec):
    inv_root = lax.rsqrt(jnp.mean(values_in * values_in, axis=-1, keepdims=True) + EPSILON)
    return (values_in * inv_root * gain_vec, inv_root)


def rms_backward(values_in, inv_root, gain_vec, grad_normed):
    weighted = grad_normed * gain_vec
    grad_gain = jnp.sum(grad_normed * values_in * inv_root, axis=0)
    grad_values = inv_root * weighted - values_in * inv_root**3 * jnp.mean(
        weighted * values_in, axis=-1, keepdims=True
    )
    return (grad_values, grad_gain)


def chain_combine(earlier, later):
    is_fresh = later[0] < 0
    same_doc = later[0] == earlier[0]

    def pick(early_part, late_part):
        expand = (-1,) + (1,) * (early_part.ndim - 1)
        with_early = late_part + jnp.where(same_doc.reshape(expand), early_part, 0.0)
        return jnp.where(is_fresh.reshape(expand), early_part, with_early)

    return (
        jnp.where(is_fresh, earlier[0], later[0]),
        pick(earlier[1], later[1]),
        pick(earlier[2], later[2]),
    )


def tp_forward(partial_sum):
    return lax.psum(partial_sum, "tp")


def tp_backward(partial_sum):
    return lax.psum(partial_sum.astype(jnp.bfloat16), "tp").astype(jnp.float32)


MESH = pl.DeviceIdType.MESH

def dev(z=None, c=None, t=None):
    d={}
    if z is not None: d["fsdp"]=z
    if c is not None: d["ctx"]=c
    if t is not None: d["tp"]=t
    return d

class Gather:
    def __init__(self, n, groups, sems):
        self.n=n; self.groups=groups
        self.z=lax.axis_index("fsdp"); ctx=lax.axis_index("ctx")
        self.x=ctx//2; self.c=ctx%2
        self.ic=self.x*2+(1-self.c); self.xp=(1-self.x)*2+self.c
        (self.zr,self.xr,self.i1r,self.i2r,self.zsl,self.zsr,self.xs,self.i1s,self.i2s)=sems
    def q(self,g,s,x,c):
        ref,kind,lo,sz=self.groups[g]
        if kind=="row":
            R=ref.shape[0]//self.n
            return ref.at[pl.ds(pl.multiple_of(s*R+c*(R//2)+x*(R//4)+lo,16),sz),:]
        C=ref.shape[1]//self.n; H=ref.shape[0]//2
        return ref.at[pl.ds(pl.multiple_of(x*H+lo,16),sz), pl.ds(pl.multiple_of(s*C+c*(C//2),C//2),C//2)]
    def cp(self,g,s,x,c,ss,rs,d):
        r=self.q(g,s,x,c)
        return pltpu.make_async_remote_copy(src_ref=r,dst_ref=r,send_sem=ss,recv_sem=rs,device_id=d,device_id_type=MESH)
    def left(self,g,s): return self.cp(g,s,self.x,self.c,self.zsl.at[g,s],self.zr.at[g,s],dev(z=self.z-1))
    def right(self,g,s): return self.cp(g,s,self.x,self.c,self.zsr.at[g,s],self.zr.at[g,s],dev(z=self.z+1))
    def ic1(self,g,s,x,c): return self.cp(g,s,x,c,self.i1s.at[g,s],self.i1r.at[g,s],dev(c=self.ic))
    def ic2(self,g,s,x,c): return self.cp(g,s,x,c,self.i2s.at[g,s],self.i2r.at[g,s],dev(c=self.ic))
    def xc(self,g,s,x,c): return self.cp(g,s,x,c,self.xs.at[g,s],self.xr.at[g,s],dev(c=self.xp))
    def own(self,g):
        z=self.z
        @pl.when(z>0)
        def _(): self.left(g,z).start()
        @pl.when(z<self.n-1)
        def _(): self.right(g,z).start()
    def hop(self,g,h):
        z,x,c,n=self.z,self.x,self.c,self.n
        for d in (1,-1):
            s=z+d*h
            ok=(s<n) if d==1 else (s>=0)
            @pl.when(ok)
            def _():
                self.cp(g,s,x,c,self.zsl.at[g,s],self.zr.at[g,s],dev(z=z)).wait_recv()
                if d==1:
                    @pl.when(z>0)
                    def _(): self.left(g,s).start()
                else:
                    @pl.when(z<n-1)
                    def _(): self.right(g,s).start()
                self.xc(g,s,x,c).start()
                self.ic1(g,s,x,c).start()
    def hopx(self,g,h):
        z,x,c,n=self.z,self.x,self.c,self.n
        for d in (1,-1):
            s=z+d*h
            ok=(s<n) if d==1 else (s>=0)
            @pl.when(ok)
            def _():
                self.xc(g,s,1-x,c).wait_recv()
                self.ic2(g,s,1-x,c).start()
    def finish(self,g):
        z,x,c,n=self.z,self.x,self.c,self.n
        @pl.loop(0,n)
        def _(s):
            @pl.when(s!=z)
            def _():
                self.ic1(g,s,x,1-c).wait_recv()
                self.ic2(g,s,1-x,1-c).wait_recv()
    def drain(self):
        z,x,c,n=self.z,self.x,self.c,self.n
        for g in range(len(self.groups)):
            @pl.loop(0,n)
            def _(s):
                @pl.when((s>=z)&(z>0))
                def _(): self.left(g,s).wait_send()
                @pl.when((s<=z)&(z<n-1))
                def _(): self.right(g,s).wait_send()
                @pl.when(s!=z)
                def _():
                    self.xc(g,s,x,c).wait_send()
                    self.ic1(g,s,x,c).wait_send()
                    self.ic2(g,s,1-x,c).wait_send()

def barrier(n):
    z=lax.axis_index("fsdp"); ctx=lax.axis_index("ctx"); t=lax.axis_index("tp")
    b=pltpu.get_barrier_semaphore()
    x=ctx//2;c=ctx%2
    @pl.when(z>0)
    def _(): pl.semaphore_signal(b,inc=1,device_id=dev(z=z-1),device_id_type=MESH)
    @pl.when(z<n-1)
    def _(): pl.semaphore_signal(b,inc=1,device_id=dev(z=z+1),device_id_type=MESH)
    pl.semaphore_signal(b,inc=1,device_id=dev(c=x*2+1-c),device_id_type=MESH)
    pl.semaphore_signal(b,inc=1,device_id=dev(c=(1-x)*2+c),device_id_type=MESH)
    cnt=2+(z>0).astype(jnp.int32)+(z<n-1).astype(jnp.int32)
    pl.semaphore_wait(b,cnt)

def gkernel(n,*refs):
    ins=refs[:7]; outs=refs[7:12]; lsem=refs[12]; sems=refs[13:]
    wq,wk,wv,wo,wg,wu,wd=ins
    fqkv,fo,fg,fu,fd=outs
    z=lax.axis_index("fsdp")
    CFG=(1,1,2,2,2); LA=2; LG=2
    groups=[]; need=[]
    def split(tot,k):
        u=tot//16; e=[(u*i//k)*16 for i in range(k+1)]
        return [(e[i],e[i+1]-e[i]) for i in range(k)]
    for ref,kind,k,nd in [(fqkv,"row",(CFG[0]),[0,1,2]),(fo,"col",(CFG[1]),[3]),(fg,"row",(CFG[2]),[4]),(fu,"row",(CFG[3]),[5]),(fd,"col",(CFG[4]),[6])]:
        tot=ref.shape[0]//n//4 if kind=="row" else ref.shape[0]//2
        for i,(lo,sz) in enumerate(split(tot,k)):
            groups.append((ref,kind,lo,sz)); need.append(nd if i==0 else [])
    G=Gather(n,groups,sems)
    R=wq.shape[0]; C=wo.shape[1]
    rows=pl.ds(pl.multiple_of(z*R,R),R); cols=pl.ds(pl.multiple_of(z*C,C),C)
    qa=wq.shape[1]; ka=qa+wk.shape[1]; va=ka+wv.shape[1]
    loc=[(wq,fqkv.at[rows,0:qa]),(wk,fqkv.at[rows,qa:ka]),(wv,fqkv.at[rows,ka:va]),(wo,fo.at[:,cols]),(wg,fg.at[rows,:]),(wu,fu.at[rows,:]),(wd,fd.at[:,cols])]
    cps=[pltpu.make_async_copy(a,b,lsem.at[i]) for i,(a,b) in enumerate(loc)]
    for c in cps: c.start()
    barrier(n)
    ng=len(groups)
    def own(g):
        for i in need[g]: cps[i].wait()
        G.own(g)
    for g in range(LA): own(g)
    for k in range(ng+n+LG):
        if k+LA<ng: own(k+LA)
        for h in range(1,n):
            if 0<=k-(h-1)<ng: G.hop(k-(h-1),h)
        for h in range(1,n):
            if 0<=k-LG-(h-1)<ng: G.hopx(k-LG-(h-1),h)
    for g in range(ng): G.finish(g)
    G.drain()

def gather(n,wq,wk,wv,wo,wg,wu,wd):
    R=wq.shape[0]; C=wo.shape[1]
    bf=jnp.bfloat16
    outs=(jax.ShapeDtypeStruct((n*R,wq.shape[1]+wk.shape[1]+wv.shape[1]),bf),
      jax.ShapeDtypeStruct((wo.shape[0],n*C),bf),
      jax.ShapeDtypeStruct((n*R,wg.shape[1]),bf),jax.ShapeDtypeStruct((n*R,wu.shape[1]),bf),
      jax.ShapeDtypeStruct((wd.shape[0],n*C),bf))
    D=pltpu.SemaphoreType.DMA
    return pl.pallas_call(functools.partial(gkernel,n),out_shape=outs,
      in_specs=[pl.BlockSpec(memory_space=pl.ANY)]*7,
      out_specs=[pl.BlockSpec(memory_space=pltpu.VMEM)]*5,
      scratch_shapes=[D((7,))]+[D((24,n)) for _ in range(9)],
      compiler_params=pltpu.CompilerParams(collective_id=0,has_side_effects=True,vmem_limit_bytes=60*2**20),
      name="gather_weights")(wq,wk,wv,wo,wg,wu,wd)


def per_device(
    layer_in,
    segment_ids,
    valid_mask,
    teacher,
    attn_gain,
    w_query,
    w_key,
    w_value,
    w_out,
    ffn_gain,
    w_gate,
    w_up,
    w_down,
):
    n = lax.axis_size("fsdp")
    ctx = lax.axis_size("ctx")
    if ctx == 4 and w_gate.shape[0] % 64 == 0 and w_out.shape[1] % 256 == 0:
        gain_one = lax.all_gather(attn_gain, "fsdp", axis=0, tiled=True)
        gain_two = lax.all_gather(ffn_gain, "fsdp", axis=0, tiled=True)
        full_qkv, full_out, full_gate, full_up, full_down = gather(
            n, w_query, w_key, w_value, w_out, w_gate, w_up, w_down
        )
        qa = w_query.shape[1]
        ka = qa + w_key.shape[1]
        full_query, full_key, full_value = full_qkv[:, :qa], full_qkv[:, qa:ka], full_qkv[:, ka:]
    else:
        full_weights = (
            lax.all_gather(attn_gain, "fsdp", axis=0, tiled=True),
            lax.all_gather(w_query, "fsdp", axis=0, tiled=True),
            lax.all_gather(w_key, "fsdp", axis=0, tiled=True),
            lax.all_gather(w_value, "fsdp", axis=0, tiled=True),
            lax.all_gather(w_out, "fsdp", axis=1, tiled=True),
            lax.all_gather(ffn_gain, "fsdp", axis=0, tiled=True),
            lax.all_gather(w_gate, "fsdp", axis=0, tiled=True),
            lax.all_gather(w_up, "fsdp", axis=0, tiled=True),
            lax.all_gather(w_down, "fsdp", axis=1, tiled=True),
        )
        (
            gain_one,
            full_query,
            full_key,
            full_value,
            full_out,
            gain_two,
            full_gate,
            full_up,
            full_down,
        ) = full_weights
    seq_count, shard_len, model_width = layer_in.shape
    row_count = seq_count * shard_len
    heads_here = full_query.shape[1] // FEAT
    rows_in = layer_in.reshape(row_count, model_width).astype(jnp.float32)
    normed_full, root_one = rms_forward(rows_in, gain_one.astype(jnp.float32))
    normed_one = normed_full.astype(jnp.bfloat16)
    query_rows = product(normed_one, full_query).reshape(seq_count, shard_len, heads_here, FEAT)
    key_rows = product(normed_one, full_key).reshape(seq_count, shard_len, heads_here, FEAT)
    value_rows = product(normed_one, full_value).reshape(seq_count, shard_len, heads_here, HEAD_V)
    last_id = segment_ids[:, -1].astype(jnp.float32)
    first_id = segment_ids[:, 0].astype(jnp.float32)
    (out_state, out_norm), summary_pull = jax.vjp(
        partial(summarize, segment=segment_ids), key_rows, value_rows
    )
    blank_state = jnp.zeros_like(out_state)
    blank_norm = jnp.zeros_like(out_norm)
    no_doc = jnp.full_like(last_id, -1.0)
    prev_id, prev_state, prev_norm = entering(
        (last_id, out_state, out_norm), "ctx", chain_combine, (no_doc, blank_state, blank_norm)
    )
    attended, attend_pull = jax.vjp(
        partial(attend, segment=segment_ids, prev_id=prev_id),
        query_rows,
        key_rows,
        value_rows,
        prev_state,
        prev_norm,
    )
    mixed_heads = attended.reshape(row_count, heads_here * HEAD_V).astype(jnp.bfloat16)
    head_sum = product(mixed_heads, full_out)
    teacher_rows = teacher.reshape(row_count, model_width).astype(jnp.float32)
    weight_rows = valid_mask.reshape(row_count, 1).astype(jnp.float32)
    middle = rows_in + tp_forward(head_sum)
    normed_mid, root_two = rms_forward(middle, gain_two.astype(jnp.float32))
    normed_two = normed_mid.astype(jnp.bfloat16)
    gate_rows = product(normed_two, full_gate)
    up_rows = product(normed_two, full_up)
    sigmoid_gate = jax.nn.sigmoid(gate_rows)
    silu_gate = gate_rows * sigmoid_gate
    hidden = (silu_gate * up_rows).astype(jnp.bfloat16)
    down_sum = product(hidden, full_down)
    output = middle + tp_forward(down_sum)
    misfit = (output - teacher_rows) * weight_rows
    layer_rows = output.astype(jnp.bfloat16)
    grad_rows = misfit.astype(jnp.bfloat16)
    sum_squares = jnp.sum(misfit * misfit)
    sum_valid = jnp.sum(weight_rows)
    grad_down = product_left_t(hidden, grad_rows)
    grad_hidden = product_right_t(grad_rows, full_down)
    grad_gate_rows = (
        grad_hidden * up_rows * sigmoid_gate * (1.0 + gate_rows * (1.0 - sigmoid_gate))
    ).astype(jnp.bfloat16)
    grad_up_rows = (grad_hidden * silu_gate).astype(jnp.bfloat16)
    grad_gate = product_left_t(normed_two, grad_gate_rows)
    grad_up = product_left_t(normed_two, grad_up_rows)
    normed_two_terms = product_right_t(grad_gate_rows, full_gate) + product_right_t(
        grad_up_rows, full_up
    )
    grad_normed_two = tp_backward(normed_two_terms)
    grad_mid_norm, grad_ffn_gain = rms_backward(
        middle, root_two, gain_two.astype(jnp.float32), grad_normed_two
    )
    grad_middle = misfit + grad_mid_norm
    grad_branch = grad_middle.astype(jnp.bfloat16)
    grad_out = product_left_t(mixed_heads, grad_branch)
    grad_mixed = product_right_t(grad_branch, full_out).reshape(
        seq_count, shard_len, heads_here, HEAD_V
    )
    grad_q_near, grad_k_near, grad_v_near, grad_prev_state, grad_prev_norm = attend_pull(grad_mixed)
    next_id, later_state, later_norm = entering_2(
        (first_id, grad_prev_state, grad_prev_norm),
        "ctx",
        chain_combine,
        (no_doc, blank_state, blank_norm),
    )
    continues = (next_id == last_id).astype(jnp.float32)
    grad_k_far, grad_v_far = summary_pull(
        (later_state * continues[:, None, None, None], later_norm * continues[:, None, None])
    )
    grad_query_rows = grad_q_near.reshape(row_count, heads_here * FEAT).astype(jnp.bfloat16)
    grad_key_rows = (
        (grad_k_near + grad_k_far).reshape(row_count, heads_here * FEAT).astype(jnp.bfloat16)
    )
    grad_value_rows = (
        (grad_v_near + grad_v_far).reshape(row_count, heads_here * HEAD_V).astype(jnp.bfloat16)
    )
    grad_query = product_left_t(normed_one, grad_query_rows)
    grad_key = product_left_t(normed_one, grad_key_rows)
    grad_value = product_left_t(normed_one, grad_value_rows)
    normed_one_terms = (
        product_right_t(grad_query_rows, full_query)
        + product_right_t(grad_key_rows, full_key)
        + product_right_t(grad_value_rows, full_value)
    )
    grad_normed_one = tp_backward(normed_one_terms)
    grad_rows_in, grad_attn_gain = rms_backward(
        rows_in, root_one, gain_one.astype(jnp.float32), grad_normed_one
    )
    grad_in_rows = (grad_middle + grad_rows_in).astype(jnp.bfloat16)
    total_sq, total_valid = lax.psum((sum_squares, sum_valid), ("fsdp", "ctx"))
    loss_value = total_sq / (total_valid * model_width)
    grad_in = grad_in_rows.reshape(seq_count, shard_len, model_width)
    layer_out = layer_rows.reshape(seq_count, shard_len, model_width)
    owned = (
        lax.psum_scatter(
            grad_attn_gain.astype(jnp.bfloat16), "fsdp", scatter_dimension=0, tiled=True
        ).astype(jnp.float32),
        lax.psum_scatter(
            grad_query.astype(jnp.bfloat16), "fsdp", scatter_dimension=0, tiled=True
        ).astype(jnp.float32),
        lax.psum_scatter(
            grad_key.astype(jnp.bfloat16), "fsdp", scatter_dimension=0, tiled=True
        ).astype(jnp.float32),
        lax.psum_scatter(
            grad_value.astype(jnp.bfloat16), "fsdp", scatter_dimension=0, tiled=True
        ).astype(jnp.float32),
        lax.psum_scatter(
            grad_out.astype(jnp.bfloat16), "fsdp", scatter_dimension=1, tiled=True
        ).astype(jnp.float32),
        lax.psum_scatter(
            grad_ffn_gain.astype(jnp.bfloat16), "fsdp", scatter_dimension=0, tiled=True
        ).astype(jnp.float32),
        lax.psum_scatter(
            grad_gate.astype(jnp.bfloat16), "fsdp", scatter_dimension=0, tiled=True
        ).astype(jnp.float32),
        lax.psum_scatter(
            grad_up.astype(jnp.bfloat16), "fsdp", scatter_dimension=0, tiled=True
        ).astype(jnp.float32),
        lax.psum_scatter(
            grad_down.astype(jnp.bfloat16), "fsdp", scatter_dimension=1, tiled=True
        ).astype(jnp.float32),
    )
    shares = (
        lax.psum(owned[0].astype(jnp.bfloat16), "ctx").astype(jnp.float32),
        lax.psum(owned[1].astype(jnp.bfloat16), "ctx").astype(jnp.float32),
        lax.psum(owned[2].astype(jnp.bfloat16), "ctx").astype(jnp.float32),
        lax.psum(owned[3].astype(jnp.bfloat16), "ctx").astype(jnp.float32),
        lax.psum(owned[4].astype(jnp.bfloat16), "ctx").astype(jnp.float32),
        lax.psum(owned[5].astype(jnp.bfloat16), "ctx").astype(jnp.float32),
        lax.psum(owned[6].astype(jnp.bfloat16), "ctx").astype(jnp.float32),
        lax.psum(owned[7].astype(jnp.bfloat16), "ctx").astype(jnp.float32),
        lax.psum(owned[8].astype(jnp.bfloat16), "ctx").astype(jnp.float32),
    )
    return (
        layer_out,
        grad_in,
        shares[0],
        shares[1],
        shares[2],
        shares[3],
        shares[4],
        shares[5],
        shares[6],
        shares[7],
        shares[8],
        loss_value,
    )


def solution(mesh):
    placed = (
        P("fsdp", "ctx", None),
        P("fsdp", "ctx"),
        P("fsdp", "ctx"),
        P("fsdp", "ctx", None),
        P("fsdp"),
        P("fsdp", "tp"),
        P("fsdp", "tp"),
        P("fsdp", "tp"),
        P("tp", "fsdp"),
        P("fsdp"),
        P("fsdp", "tp"),
        P("fsdp", "tp"),
        P("tp", "fsdp"),
    )
    return jax.shard_map(
        per_device,
        mesh=mesh,
        in_specs=placed,
        out_specs=(
            P("fsdp", "ctx", None),
            P("fsdp", "ctx", None),
            P("fsdp"),
            P("fsdp", "tp"),
            P("fsdp", "tp"),
            P("fsdp", "tp"),
            P("tp", "fsdp"),
            P("fsdp"),
            P("fsdp", "tp"),
            P("fsdp", "tp"),
            P("tp", "fsdp"),
            P(),
        ),
        check_vma=False,
    )
```

```python
from functools import partial
from types import SimpleNamespace
import math

import jax
import jax.numpy as jnp
from jax import lax
from jax.experimental import pallas as pl
from jax.experimental.pallas import tpu as pltpu
from jax.sharding import PartitionSpec as P

FEAT = 16
HEAD_V = 64


EPSILON = 1e-05
HIGH = lax.Precision.HIGHEST
QUAD_SCALE = 1.0 / (4.0 * math.sqrt(2.0))


def entering(x, axis, join, neutral):
    place = lax.axis_index(axis)
    gathered = jax.tree.map(
        lambda a, kind: lax.all_gather(a.astype(kind), axis),
        x,
        (jnp.bfloat16, jnp.bfloat16, jnp.bfloat16),
    )
    state = jax.tree.map(lambda a, e: jnp.zeros_like(a) + jnp.asarray(e, a.dtype), x, neutral)

    def one(lap, state):
        return join(
            state,
            jax.tree.map(
                lambda a, own: lax.dynamic_index_in_dim(a, lap, 0, False).astype(own.dtype),
                gathered,
                x,
            ),
        )

    return lax.fori_loop(0, place, one, state)


def entering_2(x, axis, combine, identity):
    devices, here = (lax.axis_size(axis), lax.axis_index(axis))
    everything = jax.tree.map(
        lambda part, kind: lax.all_gather(part.astype(kind), axis),
        x,
        jax.tree.map(lambda a: jnp.bfloat16 if a.dtype == jnp.float32 else a.dtype, x),
    )
    start = jax.tree.map(
        lambda part, zero: jnp.broadcast_to(jnp.asarray(zero, part.dtype), part.shape), x, identity
    )

    def lap(k, before):
        at = devices - 1 - k
        reached = at > here
        new = combine(
            before, jax.tree.map(lambda part, own: part[at].astype(own.dtype), everything, x)
        )
        return jax.tree.map(lambda a, b: jnp.where(reached, a, b), new, before)

    return lax.fori_loop(0, devices, lap, start)


def product(left_side, right_side):
    return jnp.dot(left_side, right_side, preferred_element_type=jnp.float32)


def product_left_t(left_side, right_side):
    return lax.dot_general(
        left_side, right_side, (((0,), (0,)), ((), ())), preferred_element_type=jnp.float32
    )


def product_right_t(left_side, right_side):
    return lax.dot_general(
        left_side, right_side, (((1,), (1,)), ((), ())), preferred_element_type=jnp.float32
    )


def features(vectors):
    lead_dims = vectors.shape[:-1]
    feat_width = vectors.shape[-1]
    square = (vectors[..., :, None] * vectors[..., None, :]).reshape(
        lead_dims + (feat_width * feat_width,)
    )
    return jnp.concatenate(
        [jnp.ones(lead_dims + (1,), jnp.float32), 0.5 * vectors, QUAD_SCALE * square], axis=-1
    )


def attend(query_rows, key_rows, value_rows, prev_state, prev_norm, segment, prev_id):
    scores = jnp.einsum("slhf,smhf->shlm", query_rows, key_rows, precision=HIGH) * 0.25
    kernel = 1.0 + scores + 0.5 * scores * scores
    places = jnp.arange(segment.shape[1])
    allowed = (places[:, None] >= places[None, :])[None] & (
        segment[:, :, None] == segment[:, None, :]
    )
    kernel = jnp.where(allowed[:, None], kernel, 0.0)
    carried = (segment.astype(jnp.float32) == prev_id[:, None]).astype(jnp.float32)
    mapped = features(query_rows) * carried[:, :, None, None]
    numerator = jnp.einsum("shlm,smhv->slhv", kernel, value_rows, precision=HIGH) + jnp.einsum(
        "slht,shtv->slhv", mapped, prev_state, precision=HIGH
    )
    denominator = jnp.einsum("shlm->slh", kernel) + jnp.einsum(
        "slht,sht->slh", mapped, prev_norm, precision=HIGH
    )
    return numerator / denominator[..., None]


def summarize(key_rows, value_rows, segment):
    closing = (segment == segment[:, -1:]).astype(jnp.float32)
    mapped = features(key_rows) * closing[:, :, None, None]
    return (
        jnp.einsum("slht,slhv->shtv", mapped, value_rows, precision=HIGH),
        jnp.sum(mapped, axis=1),
    )


def rms_forward(values_in, gain_vec):
    inv_root = lax.rsqrt(jnp.mean(values_in * values_in, axis=-1, keepdims=True) + EPSILON)
    return (values_in * inv_root * gain_vec, inv_root)


def rms_backward(values_in, inv_root, gain_vec, grad_normed):
    weighted = grad_normed * gain_vec
    grad_gain = jnp.sum(grad_normed * values_in * inv_root, axis=0)
    grad_values = inv_root * weighted - values_in * inv_root**3 * jnp.mean(
        weighted * values_in, axis=-1, keepdims=True
    )
    return (grad_values, grad_gain)


def chain_combine(earlier, later):
    is_fresh = later[0] < 0
    same_doc = later[0] == earlier[0]

    def pick(early_part, late_part):
        expand = (-1,) + (1,) * (early_part.ndim - 1)
        with_early = late_part + jnp.where(same_doc.reshape(expand), early_part, 0.0)
        return jnp.where(is_fresh.reshape(expand), early_part, with_early)

    return (
        jnp.where(is_fresh, earlier[0], later[0]),
        pick(earlier[1], later[1]),
        pick(earlier[2], later[2]),
    )


def tp_forward(partial_sum):
    return lax.psum(partial_sum, "tp")


def tp_backward(partial_sum):
    return lax.psum(partial_sum.astype(jnp.bfloat16), "tp").astype(jnp.float32)


def general(
    layer_in,
    segment_ids,
    valid_mask,
    teacher,
    attn_gain,
    w_query,
    w_key,
    w_value,
    w_out,
    ffn_gain,
    w_gate,
    w_up,
    w_down,
):
    full_weights = (
        lax.all_gather(attn_gain, "fsdp", axis=0, tiled=True),
        lax.all_gather(w_query, "fsdp", axis=0, tiled=True),
        lax.all_gather(w_key, "fsdp", axis=0, tiled=True),
        lax.all_gather(w_value, "fsdp", axis=0, tiled=True),
        lax.all_gather(w_out, "fsdp", axis=1, tiled=True),
        lax.all_gather(ffn_gain, "fsdp", axis=0, tiled=True),
        lax.all_gather(w_gate, "fsdp", axis=0, tiled=True),
        lax.all_gather(w_up, "fsdp", axis=0, tiled=True),
        lax.all_gather(w_down, "fsdp", axis=1, tiled=True),
    )
    (
        gain_one,
        full_query,
        full_key,
        full_value,
        full_out,
        gain_two,
        full_gate,
        full_up,
        full_down,
    ) = full_weights
    seq_count, shard_len, model_width = layer_in.shape
    row_count = seq_count * shard_len
    heads_here = full_query.shape[1] // FEAT
    rows_in = layer_in.reshape(row_count, model_width).astype(jnp.float32)
    normed_full, root_one = rms_forward(rows_in, gain_one.astype(jnp.float32))
    normed_one = normed_full.astype(jnp.bfloat16)
    query_rows = product(normed_one, full_query).reshape(seq_count, shard_len, heads_here, FEAT)
    key_rows = product(normed_one, full_key).reshape(seq_count, shard_len, heads_here, FEAT)
    value_rows = product(normed_one, full_value).reshape(seq_count, shard_len, heads_here, HEAD_V)
    last_id = segment_ids[:, -1].astype(jnp.float32)
    first_id = segment_ids[:, 0].astype(jnp.float32)
    (out_state, out_norm), summary_pull = jax.vjp(
        partial(summarize, segment=segment_ids), key_rows, value_rows
    )
    blank_state = jnp.zeros_like(out_state)
    blank_norm = jnp.zeros_like(out_norm)
    no_doc = jnp.full_like(last_id, -1.0)
    prev_id, prev_state, prev_norm = entering(
        (last_id, out_state, out_norm), "ctx", chain_combine, (no_doc, blank_state, blank_norm)
    )
    attended, attend_pull = jax.vjp(
        partial(attend, segment=segment_ids, prev_id=prev_id),
        query_rows,
        key_rows,
        value_rows,
        prev_state,
        prev_norm,
    )
    mixed_heads = attended.reshape(row_count, heads_here * HEAD_V).astype(jnp.bfloat16)
    head_sum = product(mixed_heads, full_out)
    teacher_rows = teacher.reshape(row_count, model_width).astype(jnp.float32)
    weight_rows = valid_mask.reshape(row_count, 1).astype(jnp.float32)
    middle = rows_in + tp_forward(head_sum)
    normed_mid, root_two = rms_forward(middle, gain_two.astype(jnp.float32))
    normed_two = normed_mid.astype(jnp.bfloat16)
    gate_rows = product(normed_two, full_gate)
    up_rows = product(normed_two, full_up)
    sigmoid_gate = jax.nn.sigmoid(gate_rows)
    silu_gate = gate_rows * sigmoid_gate
    hidden = (silu_gate * up_rows).astype(jnp.bfloat16)
    down_sum = product(hidden, full_down)
    output = middle + tp_forward(down_sum)
    misfit = (output - teacher_rows) * weight_rows
    layer_rows = output.astype(jnp.bfloat16)
    grad_rows = misfit.astype(jnp.bfloat16)
    sum_squares = jnp.sum(misfit * misfit)
    sum_valid = jnp.sum(weight_rows)
    grad_down = product_left_t(hidden, grad_rows)
    grad_hidden = product_right_t(grad_rows, full_down)
    grad_gate_rows = (
        grad_hidden * up_rows * sigmoid_gate * (1.0 + gate_rows * (1.0 - sigmoid_gate))
    ).astype(jnp.bfloat16)
    grad_up_rows = (grad_hidden * silu_gate).astype(jnp.bfloat16)
    grad_gate = product_left_t(normed_two, grad_gate_rows)
    grad_up = product_left_t(normed_two, grad_up_rows)
    normed_two_terms = product_right_t(grad_gate_rows, full_gate) + product_right_t(
        grad_up_rows, full_up
    )
    grad_normed_two = tp_backward(normed_two_terms)
    grad_mid_norm, grad_ffn_gain = rms_backward(
        middle, root_two, gain_two.astype(jnp.float32), grad_normed_two
    )
    grad_middle = misfit + grad_mid_norm
    grad_branch = grad_middle.astype(jnp.bfloat16)
    grad_out = product_left_t(mixed_heads, grad_branch)
    grad_mixed = product_right_t(grad_branch, full_out).reshape(
        seq_count, shard_len, heads_here, HEAD_V
    )
    grad_q_near, grad_k_near, grad_v_near, grad_prev_state, grad_prev_norm = attend_pull(grad_mixed)
    next_id, later_state, later_norm = entering_2(
        (first_id, grad_prev_state, grad_prev_norm),
        "ctx",
        chain_combine,
        (no_doc, blank_state, blank_norm),
    )
    continues = (next_id == last_id).astype(jnp.float32)
    grad_k_far, grad_v_far = summary_pull(
        (later_state * continues[:, None, None, None], later_norm * continues[:, None, None])
    )
    grad_query_rows = grad_q_near.reshape(row_count, heads_here * FEAT).astype(jnp.bfloat16)
    grad_key_rows = (
        (grad_k_near + grad_k_far).reshape(row_count, heads_here * FEAT).astype(jnp.bfloat16)
    )
    grad_value_rows = (
        (grad_v_near + grad_v_far).reshape(row_count, heads_here * HEAD_V).astype(jnp.bfloat16)
    )
    grad_query = product_left_t(normed_one, grad_query_rows)
    grad_key = product_left_t(normed_one, grad_key_rows)
    grad_value = product_left_t(normed_one, grad_value_rows)
    normed_one_terms = (
        product_right_t(grad_query_rows, full_query)
        + product_right_t(grad_key_rows, full_key)
        + product_right_t(grad_value_rows, full_value)
    )
    grad_normed_one = tp_backward(normed_one_terms)
    grad_rows_in, grad_attn_gain = rms_backward(
        rows_in, root_one, gain_one.astype(jnp.float32), grad_normed_one
    )
    grad_in_rows = (grad_middle + grad_rows_in).astype(jnp.bfloat16)
    total_sq, total_valid = lax.psum((sum_squares, sum_valid), ("fsdp", "ctx"))
    loss_value = total_sq / (total_valid * model_width)
    grad_in = grad_in_rows.reshape(seq_count, shard_len, model_width)
    layer_out = layer_rows.reshape(seq_count, shard_len, model_width)
    owned = (
        lax.psum_scatter(
            grad_attn_gain.astype(jnp.bfloat16), "fsdp", scatter_dimension=0, tiled=True
        ).astype(jnp.float32),
        lax.psum_scatter(
            grad_query.astype(jnp.bfloat16), "fsdp", scatter_dimension=0, tiled=True
        ).astype(jnp.float32),
        lax.psum_scatter(
            grad_key.astype(jnp.bfloat16), "fsdp", scatter_dimension=0, tiled=True
        ).astype(jnp.float32),
        lax.psum_scatter(
            grad_value.astype(jnp.bfloat16), "fsdp", scatter_dimension=0, tiled=True
        ).astype(jnp.float32),
        lax.psum_scatter(
            grad_out.astype(jnp.bfloat16), "fsdp", scatter_dimension=1, tiled=True
        ).astype(jnp.float32),
        lax.psum_scatter(
            grad_ffn_gain.astype(jnp.bfloat16), "fsdp", scatter_dimension=0, tiled=True
        ).astype(jnp.float32),
        lax.psum_scatter(
            grad_gate.astype(jnp.bfloat16), "fsdp", scatter_dimension=0, tiled=True
        ).astype(jnp.float32),
        lax.psum_scatter(
            grad_up.astype(jnp.bfloat16), "fsdp", scatter_dimension=0, tiled=True
        ).astype(jnp.float32),
        lax.psum_scatter(
            grad_down.astype(jnp.bfloat16), "fsdp", scatter_dimension=1, tiled=True
        ).astype(jnp.float32),
    )
    shares = (
        lax.psum(owned[0].astype(jnp.bfloat16), "ctx").astype(jnp.float32),
        lax.psum(owned[1].astype(jnp.bfloat16), "ctx").astype(jnp.float32),
        lax.psum(owned[2].astype(jnp.bfloat16), "ctx").astype(jnp.float32),
        lax.psum(owned[3].astype(jnp.bfloat16), "ctx").astype(jnp.float32),
        lax.psum(owned[4].astype(jnp.bfloat16), "ctx").astype(jnp.float32),
        lax.psum(owned[5].astype(jnp.bfloat16), "ctx").astype(jnp.float32),
        lax.psum(owned[6].astype(jnp.bfloat16), "ctx").astype(jnp.float32),
        lax.psum(owned[7].astype(jnp.bfloat16), "ctx").astype(jnp.float32),
        lax.psum(owned[8].astype(jnp.bfloat16), "ctx").astype(jnp.float32),
    )
    return (
        layer_out,
        grad_in,
        shares[0],
        shares[1],
        shares[2],
        shares[3],
        shares[4],
        shares[5],
        shares[6],
        shares[7],
        shares[8],
        loss_value,
    )


MESH = pl.DeviceIdType.MESH
F32 = jnp.float32
BF16 = jnp.bfloat16


def up_to(size, step):
    return -(-size // step) * step


def mm(a, b):
    return jnp.dot(a, b, preferred_element_type=F32)


def mm_nt(a, b):
    return lax.dot_general(a, b, (((1,), (1,)), ((), ())), preferred_element_type=F32)


def mm_tn(a, b):
    return lax.dot_general(a, b, (((0,), (0,)), ((), ())), preferred_element_type=F32)


def at128(offset):
    return pl.multiple_of(offset, 128)


class Place:
    def __init__(self, n):
        self.n = n
        self.z = lax.axis_index("fsdp")
        self.b = lax.axis_index("ctx")
        self.t = lax.axis_index("tp")
        self.x = self.b // 2
        self.c = self.b % 2
        self.ic = self.x * 2 + (1 - self.c)
        self.xp = (1 - self.x) * 2 + self.c
        self.dg = (1 - self.x) * 2 + (1 - self.c)


def remote(src, dst, send, recv, **where):
    return pltpu.make_async_remote_copy(
        src_ref=src, dst_ref=dst, send_sem=send, recv_sem=recv, device_id=where, device_id_type=MESH
    )


def entry_barrier(p):
    sem = pltpu.get_barrier_semaphore()
    for s in range(p.n):

        @pl.when(p.z != s)
        def _():
            pl.semaphore_signal(sem, inc=1, device_id={"fsdp": s}, device_id_type=MESH)

    for peer in (p.ic, p.xp, p.dg):
        pl.semaphore_signal(sem, inc=1, device_id={"ctx": peer}, device_id_type=MESH)
    pl.semaphore_signal(sem, inc=1, device_id={"tp": 1 - p.t}, device_id_type=MESH)
    pl.semaphore_wait(sem, p.n - 1 + 4)


class Gather:
    def __init__(self, p, pieces, sems):
        self.p = p
        self.pieces = pieces
        (self.zr, self.xr, self.i1r, self.i2r, self.zsl, self.zsr, self.xs, self.i1s, self.i2s) = sems

    def quarter(self, g, s, x, c):
        ref, kind, lo, size = self.pieces[g]
        n = self.p.n
        if kind == "row":
            return ref.at[pl.ds(pl.multiple_of((c * n + s) * 128 + x * 64 + lo[0], 16), size), 0 : lo[1]]
        half = lo[1]
        return ref.at[
            pl.ds(pl.multiple_of(x * half + lo[0], 16), size), pl.ds(at128((c * n + s) * 128), 128)
        ]

    def copy(self, g, s, x, c, send, recv, **where):
        ref = self.quarter(g, s, x, c)
        return remote(ref, ref, send.at[g, s], recv.at[g, s], **where)

    def left(self, g, s):
        return self.copy(g, s, self.p.x, self.p.c, self.zsl, self.zr, fsdp=self.p.z - 1)

    def right(self, g, s):
        return self.copy(g, s, self.p.x, self.p.c, self.zsr, self.zr, fsdp=self.p.z + 1)

    def chip(self, g, s, x, c, second):
        if second:
            return self.copy(g, s, x, c, self.i2s, self.i2r, ctx=self.p.ic)
        return self.copy(g, s, x, c, self.i1s, self.i1r, ctx=self.p.ic)

    def cross(self, g, s, x, c):
        return self.copy(g, s, x, c, self.xs, self.xr, ctx=self.p.xp)

    def own(self, g):
        p = self.p

        @pl.when(p.z > 0)
        def _():
            self.left(g, p.z).start()

        @pl.when(p.z < p.n - 1)
        def _():
            self.right(g, p.z).start()

    def hop(self, g, h):
        p = self.p
        for d in (1, -1):
            s = p.z + d * h
            there = (s < p.n) if d == 1 else (s >= 0)

            @pl.when(there)
            def _():
                self.copy(g, s, p.x, p.c, self.zsl, self.zr, fsdp=p.z).wait_recv()
                if d == 1:

                    @pl.when(p.z > 0)
                    def _():
                        self.left(g, s).start()

                else:

                    @pl.when(p.z < p.n - 1)
                    def _():
                        self.right(g, s).start()

                self.cross(g, s, p.x, p.c).start()
                self.chip(g, s, p.x, p.c, False).start()

    def hop_cross(self, g, h):
        p = self.p
        for d in (1, -1):
            s = p.z + d * h
            there = (s < p.n) if d == 1 else (s >= 0)

            @pl.when(there)
            def _():
                self.cross(g, s, 1 - p.x, p.c).wait_recv()
                self.chip(g, s, 1 - p.x, p.c, True).start()

    def finish(self, g):
        p = self.p

        @pl.loop(0, p.n)
        def _(s):
            @pl.when(s != p.z)
            def _():
                self.chip(g, s, p.x, 1 - p.c, False).wait_recv()
                self.chip(g, s, 1 - p.x, 1 - p.c, True).wait_recv()

    def drain(self):
        p = self.p
        for g in range(len(self.pieces)):

            @pl.loop(0, p.n)
            def _(s):
                @pl.when((s >= p.z) & (p.z > 0))
                def _():
                    self.left(g, s).wait_send()

                @pl.when((s <= p.z) & (p.z < p.n - 1))
                def _():
                    self.right(g, s).wait_send()

                @pl.when(s != p.z)
                def _():
                    self.cross(g, s, p.x, p.c).wait_send()
                    self.chip(g, s, p.x, p.c, False).wait_send()
                    self.chip(g, s, 1 - p.x, p.c, True).wait_send()


class Reduce:
    def __init__(self, p, parts, seen, done, sems):
        self.p = p
        self.parts = parts
        self.seen = seen
        self.done = done
        (self.ss, self.rs, self.fs, self.fr) = sems

    def move(self, g, s, slot, to):
        return remote(
            self.parts[g].at[s], self.seen[g].at[slot], self.ss.at[g, s], self.rs.at[g, slot], fsdp=to
        )

    def arrived(self, g, slot):
        self.move(g, 0, slot, self.p.z).wait_recv()

    def add(self, g, s, slot):
        total = self.parts[g][s].astype(F32) + self.seen[g][slot].astype(F32)
        self.parts[g][s] = total.astype(BF16)

    def stage(self, g, k):
        p = self.p
        n = p.n

        @pl.when(p.z == k)
        def _():
            for s in range(n - 1, k, -1):
                if k > 0:
                    self.arrived(g, s)
                    self.add(g, s, s)
                self.move(g, s, s, k + 1).start()

        @pl.when(p.z == n - 1 - k)
        def _():
            z = n - 1 - k
            for s in range(0, z):
                if k > 0:
                    self.arrived(g, s)
                    self.add(g, s, s)
                self.move(g, s, n if s == z - 1 else s, z - 1).start()

    def last(self, g):
        p = self.p
        n = p.n

        @pl.when(p.z > 0)
        def _():
            self.arrived(g, p.z)
            self.add(g, p.z, p.z)

        @pl.when(p.z < n - 1)
        def _():
            self.arrived(g, n)
            self.add(g, p.z, n)

        self.done[g][p.b] = self.parts[g][p.z]
        self.spread(g, p.b, 0, p.ic).start()
        self.spread(g, p.b, 1, p.xp).start()

    def spread(self, g, slot, which, to):
        return remote(
            self.done[g].at[slot], self.done[g].at[slot], self.fs.at[g, which], self.fr.at[g, slot], ctx=to
        )

    def relay(self, g):
        p = self.p
        self.spread(g, p.xp, 1, p.xp).wait_recv()
        self.spread(g, p.xp, 2, p.ic).start()

    def finish(self, g):
        p = self.p
        self.spread(g, p.ic, 0, p.ic).wait_recv()
        self.spread(g, p.dg, 2, p.ic).wait_recv()
        self.spread(g, p.b, 0, p.ic).wait_send()
        self.spread(g, p.b, 1, p.xp).wait_send()
        self.spread(g, p.xp, 2, p.ic).wait_send()

        @pl.loop(0, p.n)
        def _(s):
            @pl.when(s != p.z)
            def _():
                self.move(g, s, 0, p.z).wait_send()


class Columns:
    def __init__(self, p, k, src, dst, sems):
        self.p = p
        self.k = k
        self.src = src
        self.dst = dst
        self.send, self.recv = sems

    def slot(self, b):
        rows = self.src.shape[0]
        return self.dst.at[pl.ds(pl.multiple_of(b * rows, rows), rows), :]

    def copy(self, peer, which):
        p = self.p
        w = self.dst.shape[1]
        part = self.src.at[:, pl.ds(at128((peer % 2) * w), w)]
        return remote(part, self.slot(p.b), self.send.at[self.k, which], self.recv.at[self.k, p.b], ctx=peer)

    def start(self):
        p = self.p
        w = self.dst.shape[1]
        for which, peer in enumerate((p.xp, p.dg, p.ic)):
            self.copy(peer, which).start()
        self.slot(p.b)[...] = self.src[:, pl.ds(at128(p.c * w), w)]

    def wait(self):
        p = self.p
        for peer in (p.ic, p.xp, p.dg):
            remote(self.slot(peer), self.slot(peer), self.send.at[self.k, 0], self.recv.at[self.k, peer], ctx=peer).wait_recv()

    def drain(self):
        p = self.p
        for which, peer in enumerate((p.xp, p.dg, p.ic)):
            self.copy(peer, which).wait_send()


class Halves:
    def __init__(self, p, k, src, dst, step, sems):
        self.p = p
        self.k = k
        self.src = src
        self.dst = dst
        self.step = step
        self.send, self.recv = sems

    def slot(self, b):
        rows = self.src.shape[0]
        return self.dst.at[pl.ds(pl.multiple_of(b * rows, rows), rows), :]

    def part(self, x):
        return self.src.at[:, pl.ds(at128(x * self.step), self.dst.shape[1])]

    def to(self, src, slot, which, peer):
        return remote(src, self.slot(slot), self.send.at[self.k, which], self.recv.at[self.k, slot], ctx=peer)

    def start(self):
        p = self.p
        self.to(self.part(1 - p.x), p.b, 0, p.xp).start()
        self.to(self.part(p.x), p.b, 1, p.ic).start()
        self.slot(p.b)[...] = self.src[:, pl.ds(at128(p.x * self.step), self.dst.shape[1])]

    def relay(self):
        p = self.p
        self.to(self.slot(p.xp), p.xp, 2, p.ic).wait_recv()
        self.to(self.slot(p.xp), p.xp, 2, p.ic).start()

    def wait(self):
        p = self.p
        self.to(self.slot(p.ic), p.ic, 1, p.ic).wait_recv()
        self.to(self.slot(p.dg), p.dg, 1, p.ic).wait_recv()

    def drain(self):
        p = self.p
        self.to(self.part(1 - p.x), p.b, 0, p.xp).wait_send()
        self.to(self.part(p.x), p.b, 1, p.ic).wait_send()
        self.to(self.slot(p.xp), p.xp, 2, p.ic).wait_send()


def mega_kernel(n, names, *refs):
    r = SimpleNamespace(**dict(zip(names, refs)))
    p = Place(n)
    z, b, x, c = p.z, p.b, p.x, p.c
    rows_here = r.x.shape[0]
    width = r.x.shape[1]
    half_d = width // 2
    heads = r.wv.shape[1] // HEAD_V
    qk = r.wq.shape[1]
    vw = r.wv.shape[1]
    ff = r.wd.shape[0]
    ffp = r.hid.shape[1]
    order = [s * 256 + cc * 128 for cc in range(2) for s in range(n)]
    blocks = width // 256
    D = r.lsem

    fqkv, fo, fg, fu, fd = r.fqkv, r.fo, r.fg, r.fu, r.fd
    local = []

    def bring(src, dst):
        copy = pltpu.make_async_copy(src, dst, D.at[len(local)])
        copy.start()
        local.append(copy)
        return copy

    get_x = bring(r.x, r.xv)
    need = {}
    for cc in range(2):
        rows = pl.ds(at128((cc * n + z) * 128), 128)
        src = slice(cc * 128, cc * 128 + 128)
        need.setdefault("qkv", []).extend(
            (
                bring(r.wq.at[src, :], fqkv.at[rows, 0:qk]),
                bring(r.wk.at[src, :], fqkv.at[rows, qk : 2 * qk]),
                bring(r.wv.at[src, :], fqkv.at[rows, 2 * qk : 2 * qk + vw]),
            )
        )
    for cc in range(2):
        cols = pl.ds(at128((cc * n + z) * 128), 128)
        need.setdefault("o", []).append(bring(r.wo.at[:, cc * 128 : cc * 128 + 128], fo.at[:, cols]))
    for cc in range(2):
        rows = pl.ds(at128((cc * n + z) * 128), 128)
        need.setdefault("g", []).append(bring(r.wg.at[cc * 128 : cc * 128 + 128, :], fg.at[rows, :]))
        need.setdefault("u", []).append(bring(r.wu.at[cc * 128 : cc * 128 + 128, :], fu.at[rows, :]))
    for cc in range(2):
        cols = pl.ds(at128((cc * n + z) * 128), 128)
        need.setdefault("d", []).append(
            bring(r.wd.at[:, cc * 128 : cc * 128 + 128], fd.at[0:ff, cols])
        )
    get_teacher = bring(r.teacher, r.tv)

    pieces, first = [], []

    def split(total, parts):
        unit = total // 16
        edge = [(unit * i // parts) * 16 for i in range(parts + 1)]
        return [(edge[i], edge[i + 1] - edge[i]) for i in range(parts)]

    for key, ref, kind, total, parts in (
        ("qkv", fqkv, "row", 64, 1),
        ("o", fo, "col", vw // 2, 1),
        ("g", fg, "row", 64, 2),
        ("u", fu, "row", 64, 2),
        ("d", fd, "col", ff // 2, 2),
    ):
        for i, (lo, size) in enumerate(split(total, parts)):
            pieces.append((ref, kind, (lo, ref.shape[1]) if kind == "row" else (lo, total), size))
            first.append(need[key] if i == 0 else [])
    gather = Gather(p, pieces, r.gs)
    ng = len(pieces)

    def own(g):
        for copy in first[g]:
            copy.wait()
        gather.own(g)

    entry_barrier(p)
    own(0)
    own(1)

    gsend, grecv, gath = r.gnsem[0], r.gnsem[1], r.gath
    for s in range(n):

        @pl.when(z != s)
        def _():
            remote(r.gains, gath.at[z], gsend.at[s], grecv.at[z], fsdp=s).start()

    gath[z] = r.gains[...]
    segs, segr = r.segsem[0], r.segsem[1]
    for i, peer in enumerate((p.ic, p.xp, p.dg)):
        remote(r.segrow, r.segall.at[b], segs.at[i], segr.at[b], ctx=peer).start()
    r.segall[b] = r.segrow[...]

    pad = ffp - ff
    if pad:
        fd[ff:ffp, :] = jnp.zeros((pad, width), BF16)

    for s in range(n):

        @pl.when(z != s)
        def _():
            remote(r.gains, gath.at[s], gsend.at[s], grecv.at[s], fsdp=s).wait_recv()

    for row in range(2):
        r.gain[row : row + 1, :] = jnp.concatenate(
            [gath[s, row : row + 1, cc * 128 : cc * 128 + 128] for cc in range(2) for s in range(n)], axis=1
        )

    events = [(g - 1.5, "own", g, 0) for g in range(2, ng)]
    for g in range(ng):
        for h in range(1, n):
            events.append((g + 0.7 * h, "hop", g, h))
            events.append((g + 0.7 * h + 0.8, "cross", g, h))
    events.sort()
    passed = [0]

    def advance(until):
        while passed[0] < len(events) and events[passed[0]][0] <= until:
            _, kind, g, h = events[passed[0]]
            if kind == "own":
                own(g)
            elif kind == "hop":
                gather.hop(g, h)
            else:
                gather.hop_cross(g, h)
            passed[0] += 1

    def ready(g_from, g_to):
        advance(max(e[0] for e in events if e[1] == "cross" and e[2] < g_to))
        for g in range(g_from, g_to):
            gather.finish(g)

    send_n1 = Columns(p, 0, r.n1, r.n1c, r.csem)
    send_da = Columns(p, 1, r.da, r.dac, r.csem)
    send_n2 = Columns(p, 2, r.n2, r.n2c, r.csem)
    send_dy = Columns(p, 3, r.dy, r.dyc, r.csem)
    fh = r.hidx.shape[1]
    send_hid = Halves(p, 0, r.hid, r.hidx, ffp - fh, r.hsem)
    send_dg = Halves(p, 1, r.dg, r.dgx, ffp - fh, r.hsem)
    send_du = Halves(p, 2, r.du, r.dux, ffp - fh, r.hsem)
    send_mix = Halves(p, 3, r.mix, r.mixx, vw // 2, r.hsem)
    send_dqkv = Halves(p, 4, r.dqkv, r.dqkvx, (2 * qk + vw) // 2, r.hsem)
    ysend, yrecv = r.ysend, r.yrecv

    def y_copy(i, ch):
        return remote(ysend.at[i, ch], yrecv.at[i, ch], r.ysem[0].at[i, ch], r.ysem[1].at[i, ch], tp=1 - p.t)

    def y_put(i, ch, value):
        ysend[i, ch] = value.astype(BF16)
        y_copy(i, ch).start()

    def y_wait(i, between=()):
        for ch in range(blocks):
            y_copy(i, ch).wait_recv()
            if ch < len(between):
                between[ch]()

    def y_rows(i, rs):
        return jnp.concatenate(
            [ysend[i, ch, rs, :].astype(F32) + yrecv[i, ch, rs, :].astype(F32) for ch in range(blocks)], axis=1
        )

    step_rows = 32
    row_steps = rows_here // step_rows

    def per_rows(body):
        @pl.loop(0, row_steps)
        def _(i):
            body(pl.ds(pl.multiple_of(i * step_rows, step_rows), step_rows))

    def x_rows(rs):
        return jnp.concatenate([r.xv[rs, o : o + 128] for o in order], axis=1).astype(F32)

    def rsq(v):
        return lax.rsqrt(jnp.mean(v * v, axis=1, keepdims=True) + EPSILON)

    get_x.wait()

    def norm_one(rs):
        v = x_rows(rs)
        r.n1[rs, :] = (v * rsq(v) * r.gain[0:1, :]).astype(BF16)

    per_rows(norm_one)
    ready(0, 1)
    kv = r.kv
    first_chunk = mm(r.n1[...], fqkv[:, 0 : 2 * qk])
    r.q[...] = first_chunk[:, 0:qk].astype(BF16)
    kv[b, :, 0:qk] = first_chunk[:, qk : 2 * qk].astype(BF16)
    for ch in range(vw // 256):
        lo = ch * 256
        kv[b, :, qk + lo : qk + lo + 256] = mm(r.n1[...], fqkv[:, 2 * qk + lo : 2 * qk + lo + 256]).astype(BF16)

    kvs, kvr = r.kvsem

    def kv_copy(slot, which, peer):
        return remote(kv.at[slot], kv.at[slot], kvs.at[which], kvr.at[slot], ctx=peer)

    @pl.when(x == 0)
    def _():
        kv_copy(b, 0, p.xp).start()

    @pl.when(c == 0)
    def _():
        kv_copy(b, 1, p.ic).start()

    for i, peer in enumerate((p.ic, p.xp, p.dg)):
        remote(r.segrow, r.segall.at[peer], segs.at[i], segr.at[peer], ctx=peer).wait_recv()
    mask, num, den = r.mask, r.num, r.den
    num[...] = jnp.zeros_like(num)
    den[...] = jnp.zeros_like(den)
    lane = lax.broadcasted_iota(jnp.int32, (1, 128), 1)

    def q_of(h):
        keep = (lane // FEAT) == h
        return jnp.where(keep, r.q[...], jnp.zeros((), BF16))

    def attend_block(j):
        same = r.segcol[:, 0:1] == r.segall[j, 0:1, :]
        ri = lax.broadcasted_iota(jnp.int32, (rows_here, rows_here), 0)
        ci = lax.broadcasted_iota(jnp.int32, (rows_here, rows_here), 1)
        reach = ri + jnp.where(j == b, 0, rows_here) >= ci
        mask[j] = jnp.where(same & reach, 1.0, 0.0)

        @pl.loop(0, heads // 2)
        def _(pair):
            at = pl.ds(at128(pair * 128), 128)
            vpair = kv[j, :, pl.ds(at128(qk + pair * 128), 128)]
            sums = []
            for e in range(2):
                s = mm_nt(q_of(pair * 2 + e), kv[j, :, 0:qk]) * 0.25
                w = (1.0 + s + 0.5 * s * s) * mask[j]
                sums.append((mm(w.astype(BF16), vpair), jnp.sum(w, axis=1, keepdims=True)))
            low_half = lane < HEAD_V
            num[:, at] += jnp.where(low_half, sums[0][0], sums[1][0])
            den[:, at] += jnp.where(low_half, sums[0][1], sums[1][1])

    attend_block(b)
    advance(3.3)

    @pl.when(x == 1)
    def _():
        kv_copy(c, 2, p.ic).wait_recv()
        kv_copy(c, 2, p.ic).start()

    @pl.when(c == 1)
    def _():
        kv_copy(p.ic, 1, p.ic).wait_recv()

    @pl.when(x == 1)
    def _():
        kv_copy(1 - c, 2, p.ic).wait_recv()

    @pl.loop(1, b + 1)
    def _(m):
        attend_block(b - m)

    inv = 1.0 / den[...]
    den[...] = inv
    num[...] = num[...] * inv
    r.mix[...] = num[...].astype(BF16)

    ready(1, 2)
    for ch in range(blocks):
        y_put(0, ch, mm(r.mix[...], fo[:, ch * 256 : ch * 256 + 256]))
    send_mix.start()
    send_n1.start()
    advance(4.5)
    y_wait(0, [lambda u=u: advance(u) for u in (5.0, 5.7, 6.3)])

    def norm_two(rs):
        v = x_rows(rs) + y_rows(0, rs)
        r.mid[rs, :] = v
        r.n2[rs, :] = (v * rsq(v) * r.gain[1:2, :]).astype(BF16)

    per_rows(norm_two)
    send_mix.relay()
    send_n2.start()

    fchunks = -(-ffp // 256)

    def per_ff(body):
        @pl.loop(0, fchunks)
        def _(i):
            body(at128(jnp.minimum(i * 256, ffp - 256)))

    ready(2, 6)
    def wide(ref, off):
        return ref[:, pl.ds(off, 256)]

    def forward_ff(off):
        g = mm(r.n2[...], wide(fg, off))
        u = mm(r.n2[...], wide(fu, off))
        r.g[:, pl.ds(off, 256)] = g
        r.u[:, pl.ds(off, 256)] = u
        sig = 1.0 / (1.0 + jnp.exp(-g))
        r.hid[:, pl.ds(off, 256)] = (g * sig * u).astype(BF16)

    per_ff(forward_ff)
    send_hid.start()
    ready(6, ng)
    for ch in range(blocks):
        y_put(1, ch, mm(r.hid[...], fd[:, ch * 256 : ch * 256 + 256]))
    send_hid.relay()
    get_teacher.wait()
    small = r.small
    small[...] = jnp.zeros_like(small)
    y_wait(1)

    def finish_forward(rs):
        y = r.mid[rs, :] + y_rows(1, rs)
        t = jnp.concatenate([r.tv[rs, o : o + 128] for o in order], axis=1).astype(F32)
        m = (y - t) * r.valid[rs, 0:1]
        r.mis[rs, :] = m
        r.dy[rs, :] = m.astype(BF16)
        yb = y.astype(BF16)
        for i, o in enumerate(order):
            r.layer_out[rs, o : o + 128] = yb[:, i * 128 : i * 128 + 128]
        small[2:3, :] += jnp.sum(m * m, axis=0, keepdims=True)
        small[3:4, :] += jnp.broadcast_to(jnp.sum(r.valid[rs, :], axis=0, keepdims=True)[:, 0:1], (1, width))

    per_rows(finish_forward)
    send_dy.start()

    def backward_ff(off):
        dh = mm_nt(r.dy[...], fd[pl.ds(off, 256), :])
        g = r.g[:, pl.ds(off, 256)]
        u = r.u[:, pl.ds(off, 256)]
        sig = 1.0 / (1.0 + jnp.exp(-g))
        r.dg[:, pl.ds(off, 256)] = (dh * u * sig * (1.0 + g * (1.0 - sig))).astype(BF16)
        r.du[:, pl.ds(off, 256)] = (dh * g * sig).astype(BF16)

    per_ff(backward_ff)
    send_dg.start()
    send_du.start()
    for ch in range(blocks):
        rows = slice(ch * 256, ch * 256 + 256)
        y_put(2, ch, mm_nt(r.dg[...], fg[rows, :]) + mm_nt(r.du[...], fu[rows, :]))

    red = Reduce(
        p,
        [r.part[i] for i in range(5)],
        [r.seen[i] for i in range(5)],
        [r.out_d, r.out_g, r.out_u, r.out_o, r.out_q],
        r.rsem,
    )
    turned = r.turned

    def turn(src):
        w = src.shape[1]

        @pl.loop(0, 4)
        def _(i):
            at = pl.ds(pl.multiple_of(i * rows_here, rows_here), rows_here)
            turned[0:w, at] = jnp.transpose(src[at, :])

    def grad_rows(g, rhs):
        rows = r.part[g].shape[1]

        @pl.loop(0, rhs.shape[1] // 128 // 2 if rhs.shape[1] % 256 == 0 else rhs.shape[1] // 128)
        def _(i):
            w = 256 if rhs.shape[1] % 256 == 0 else 128
            at = pl.ds(at128(i * w), w)
            res = mm(turned[0 : n * rows, :], rhs[:, at]).astype(BF16)
            for s in range(n):
                r.part[g][s, :, at] = res[s * rows : s * rows + rows, :]

    def grad_cols(g, rhs):
        rows = r.part[g].shape[1]

        @pl.loop(0, rows // 256)
        def _(i):
            at = pl.ds(pl.multiple_of(i * 256, 256), 256)
            res = mm(turned[at, :], rhs[...]).astype(BF16)
            for s in range(n):
                r.part[g][s, at, :] = res[:, s * 128 : s * 128 + 128]

    send_hid.wait()
    turn(r.hidx)
    send_dy.wait()
    grad_cols(0, r.dyc)
    red.stage(0, 0)
    send_n2.wait()
    turn(r.n2c)
    send_dg.relay()
    send_du.relay()
    send_dg.wait()
    grad_rows(1, r.dgx)
    red.stage(1, 0)
    send_du.wait()
    grad_rows(2, r.dux)
    red.stage(2, 0)

    y_wait(2)

    def norm_back(i, row, v, base, rs):
        dn = y_rows(i, rs)
        inv_root = rsq(v)
        w = dn * r.gain[row : row + 1, :]
        small[row : row + 1, :] += jnp.sum(dn * v * inv_root, axis=0, keepdims=True)
        m = jnp.mean(w * v, axis=1, keepdims=True)
        return base + inv_root * w - v * (inv_root * inv_root * inv_root * m)

    def middle_back(rs):
        d = norm_back(2, 1, r.mid[rs, :], r.mis[rs, :], rs)
        r.mis[rs, :] = d
        r.da[rs, :] = d.astype(BF16)

    per_rows(middle_back)
    send_da.start()

    dnum, dden = r.dnum, r.dden
    for ch in range(vw // 256):
        at = slice(ch * 256, ch * 256 + 256)
        d = mm_nt(r.da[...], fo[at, :]) * den[:, at]
        dnum[:, at] = d.astype(BF16)
        dden[:, at] = d * num[:, at]
    red.stage(0, 1)
    dkvp, dkv, dq = r.dkvp, r.dkv, r.dqf
    dq[...] = jnp.zeros_like(dq)

    def back_block(j):
        dkv[...] = jnp.zeros_like(dkv)

        @pl.loop(0, heads // 2)
        def _(pair):
            at = pl.ds(at128(pair * 128), 128)
            vat = pl.ds(at128(qk + pair * 128), 128)
            dv = []
            for e in range(2):
                h = pair * 2 + e
                qh = q_of(h)
                keep_v = (lane // HEAD_V) == e
                keep_q = (lane // FEAT) == h
                s = mm_nt(qh, kv[j, :, 0:qk]) * 0.25
                w = ((1.0 + s + 0.5 * s * s) * mask[j]).astype(BF16)
                dn = jnp.where(keep_v, dnum[:, at], jnp.zeros((), BF16))
                dd = jnp.sum(jnp.where(keep_v, dden[:, at], 0.0), axis=1, keepdims=True)
                dw = mm_nt(dn, kv[j, :, vat]) - dd
                ds = (dw * (1.0 + s) * (0.25 * mask[j])).astype(BF16)
                dv.append(mm_tn(w, dn))
                kh = jnp.where(keep_q, kv[j, :, 0:qk], jnp.zeros((), BF16))
                dq[...] += mm(ds, kh)
                dkv[:, 0:qk] += mm_tn(ds, qh)
            dkv[:, vat] = dv[0] + dv[1]

    @pl.loop(0, b)
    def _(j):
        back_block(j)
        dkvp[j] = dkv[...].astype(BF16)

    dks, dkr = r.dksem
    back = r.back

    def dk_copy(src, slot, which, peer):
        return remote(src, back.at[slot], dks.at[which], dkr.at[slot], ctx=peer)

    @pl.when(c == 1)
    def _():
        dk_copy(dkvp.at[p.ic], 0, 0, p.ic).start()

    @pl.when(x == 1)
    def _():
        dk_copy(dkvp.at[1 - c], 1, 1, p.ic).start()

    back_block(b)
    red.stage(1, 1)

    @pl.when(x == 1)
    def _():
        dk_copy(dkvp.at[1 - c], 1, 1, p.ic).wait_recv()
        dkvp[b] = (dkvp[c].astype(F32) + back[1].astype(F32)).astype(BF16)
        dk_copy(dkvp.at[b], 2, 2, p.xp).start()

    @pl.when(c == 0)
    def _():
        dk_copy(dkvp.at[b], 0, 0, p.ic).wait_recv()
        dkv[...] += back[0].astype(F32)

    dqkv = r.dqkv
    dqkv[:, 0:qk] = dq[...].astype(BF16)
    send_da.wait()
    send_mix.wait()
    turn(r.mixx)
    grad_cols(3, r.dac)
    red.stage(3, 0)
    red.stage(2, 1)

    @pl.when(x == 0)
    def _():
        dk_copy(dkvp.at[b], 2, 2, p.xp).wait_recv()
        dkv[...] += back[2].astype(F32)

    dqkv[:, qk : 2 * qk + vw] = dkv[...].astype(BF16)
    send_dqkv.start()
    for ch in range(blocks):
        y_put(3, ch, mm_nt(dqkv[...], fqkv[ch * 256 : ch * 256 + 256, :]))
    send_n1.wait()
    turn(r.n1c)
    send_dqkv.relay()
    send_dqkv.wait()
    grad_rows(4, r.dqkvx)
    red.stage(4, 0)
    red.stage(0, 2)

    y_wait(3)

    def input_back(rs):
        d = norm_back(3, 0, x_rows(rs), r.mis[rs, :], rs).astype(BF16)
        for i, o in enumerate(order):
            r.grad_in[rs, o : o + 128] = d[:, i * 128 : i * 128 + 128]

    per_rows(input_back)

    sms, smr = r.smsem
    parts, lines = r.smctx, r.smz
    for i, peer in enumerate((p.ic, p.xp, p.dg)):
        remote(small, parts.at[b], sms.at[0, i], smr.at[0, b], ctx=peer).start()
    parts[b] = small[...]
    red.stage(3, 1)
    red.last(0)
    red.stage(1, 2)
    for i, peer in enumerate((p.ic, p.xp, p.dg)):
        remote(small, parts.at[peer], sms.at[0, i], smr.at[0, peer], ctx=peer).wait_recv()
    lines[n] = parts[0] + parts[1] + parts[2] + parts[3]
    for s in range(n):

        @pl.when(z != s)
        def _():
            remote(lines.at[n], lines.at[z], sms.at[1, s], smr.at[1, z], fsdp=s).start()

    red.last(1)
    red.stage(4, 1)
    red.stage(2, 2)
    red.last(2)
    red.relay(0)
    red.stage(3, 2)
    red.last(3)
    red.stage(4, 2)
    red.relay(1)
    red.last(4)
    for s in range(n):

        @pl.when(z != s)
        def _():
            remote(lines.at[n], lines.at[s], sms.at[1, s], smr.at[1, s], fsdp=s).wait_recv()

    total = jnp.zeros_like(small)
    for s in range(n):
        total += jnp.where(z == s, lines[n], lines[s])
    for i, o in enumerate(order):
        r.sums[:, o : o + 128] = total[:, i * 128 : i * 128 + 128]
    red.relay(2)
    red.relay(3)
    red.relay(4)
    for g in range(5):
        red.finish(g)

    gather.drain()
    for k in (send_n1, send_da, send_n2, send_dy, send_hid, send_dg, send_du, send_mix, send_dqkv):
        k.drain()
    for i in range(4):
        for ch in range(blocks):
            y_copy(i, ch).wait_send()
    for s in range(n):

        @pl.when(z != s)
        def _():
            remote(r.gains, gath.at[z], gsend.at[s], grecv.at[z], fsdp=s).wait_send()
            remote(lines.at[n], lines.at[z], sms.at[1, s], smr.at[1, z], fsdp=s).wait_send()

    for i, peer in enumerate((p.ic, p.xp, p.dg)):
        remote(r.segrow, r.segall.at[b], segs.at[i], segr.at[b], ctx=peer).wait_send()
        remote(small, parts.at[b], sms.at[0, i], smr.at[0, b], ctx=peer).wait_send()

    @pl.when(x == 0)
    def _():
        kv_copy(b, 0, p.xp).wait_send()

    @pl.when(c == 0)
    def _():
        kv_copy(b, 1, p.ic).wait_send()

    @pl.when(x == 1)
    def _():
        kv_copy(c, 2, p.ic).wait_send()
        dk_copy(dkvp.at[1 - c], 1, 1, p.ic).wait_send()
        dk_copy(dkvp.at[b], 2, 2, p.xp).wait_send()

    @pl.when(c == 1)
    def _():
        dk_copy(dkvp.at[p.ic], 0, 0, p.ic).wait_send()


def mega(n, layer_in, segment_ids, valid_mask, teacher, attn_gain, w_query, w_key, w_value, w_out, ffn_gain, w_gate, w_up, w_down):
    x = layer_in[0]
    rows, width = x.shape
    qk, vw, ff = w_query.shape[1], w_value.shape[1], w_gate.shape[1]
    ffp = up_to(ff, 128)
    fh = up_to(ffp // 2, 256)
    half_d = width // 2
    blocks = width // 256
    seg = segment_ids[0].astype(F32)
    inputs = dict(
        x=x,
        teacher=teacher[0],
        wq=w_query,
        wk=w_key,
        wv=w_value,
        wo=w_out,
        wg=jnp.pad(w_gate, ((0, 0), (0, ffp - ff))),
        wu=jnp.pad(w_up, ((0, 0), (0, ffp - ff))),
        wd=w_down,
        gains=jnp.concatenate(
            [attn_gain[None], ffn_gain[None], jnp.zeros((6, attn_gain.shape[0]), BF16)], axis=0
        ).astype(F32),
        segrow=jnp.broadcast_to(seg[None, :], (8, rows)),
        segcol=jnp.broadcast_to(seg[:, None], (rows, 128)),
        valid=jnp.broadcast_to(valid_mask[0].astype(F32)[:, None], (rows, 128)),
    )
    hbm = list(inputs)[:9]
    outs = dict(
        layer_out=((rows, width), BF16),
        grad_in=((rows, width), BF16),
        out_d=((4, fh, 128), BF16),
        out_g=((4, 128, fh), BF16),
        out_u=((4, 128, fh), BF16),
        out_o=((4, vw // 2, 128), BF16),
        out_q=((4, 128, (2 * qk + vw) // 2), BF16),
        sums=((8, width), F32),
    )
    dma = pltpu.SemaphoreType.DMA
    ng = 8
    vm = pltpu.VMEM
    piece = [(fh, 128), (128, fh), (128, fh), (vw // 2, 128), (128, (2 * qk + vw) // 2)]
    scratch = dict(
        lsem=dma((20,)),
        gs=[dma((ng, n)) for _ in range(9)],
        gnsem=[dma((n,)), dma((n,))],
        segsem=[dma((3,)), dma((4,))],
        csem=[dma((4, 3)), dma((4, 4))],
        hsem=[dma((5, 3)), dma((5, 4))],
        ysem=[dma((4, blocks)), dma((4, blocks))],
        kvsem=[dma((3,)), dma((4,))],
        dksem=[dma((3,)), dma((3,))],
        rsem=[dma((5, n)), dma((5, n + 1)), dma((5, 3)), dma((5, 4))],
        smsem=[dma((2, max(n, 3))), dma((2, max(n, 4)))],
        fqkv=vm((width, 2 * qk + vw), BF16),
        fo=vm((vw, width), BF16),
        fg=vm((width, ffp), BF16),
        fu=vm((width, ffp), BF16),
        fd=vm((ffp, width), BF16),
        xv=vm((rows, width), BF16),
        tv=vm((rows, width), BF16),
        gath=vm((n, 8, width // n), F32),
        gain=vm((8, width), F32),
        segall=vm((4, 8, rows), F32),
        n1=vm((rows, width), BF16),
        n2=vm((rows, width), BF16),
        dy=vm((rows, width), BF16),
        da=vm((rows, width), BF16),
        n1c=vm((4 * rows, half_d), BF16),
        n2c=vm((4 * rows, half_d), BF16),
        dyc=vm((4 * rows, half_d), BF16),
        dac=vm((4 * rows, half_d), BF16),
        hid=vm((rows, ffp), BF16),
        dg=vm((rows, ffp), BF16),
        du=vm((rows, ffp), BF16),
        mix=vm((rows, vw), BF16),
        dqkv=vm((rows, 2 * qk + vw), BF16),
        hidx=vm((4 * rows, fh), BF16),
        dgx=vm((4 * rows, fh), BF16),
        dux=vm((4 * rows, fh), BF16),
        mixx=vm((4 * rows, vw // 2), BF16),
        dqkvx=vm((4 * rows, (2 * qk + vw) // 2), BF16),
        ysend=vm((4, blocks, rows, 256), BF16),
        yrecv=vm((4, blocks, rows, 256), BF16),
        q=vm((rows, qk), BF16),
        kv=vm((4, rows, qk + vw), BF16),
        mask=vm((4, rows, rows), F32),
        num=vm((rows, vw), F32),
        den=vm((rows, vw), F32),
        mid=vm((rows, width), F32),
        mis=vm((rows, width), F32),
        g=vm((rows, ffp), F32),
        u=vm((rows, ffp), F32),
        small=vm((8, width), F32),
        smctx=vm((4, 8, width), F32),
        smz=vm((n + 1, 8, width), F32),
        dnum=vm((rows, vw), BF16),
        dden=vm((rows, vw), F32),
        dqf=vm((rows, qk), F32),
        dkv=vm((rows, qk + vw), F32),
        dkvp=vm((4, rows, qk + vw), BF16),
        back=vm((3, rows, qk + vw), BF16),
        turned=vm((max(fh, half_d), 4 * rows), BF16),
        part=[vm((n,) + s, BF16) for s in piece],
        seen=[vm((n + 1,) + s, BF16) for s in piece],
    )
    flat, layout = [], []
    for k, v in scratch.items():
        if isinstance(v, list):
            layout.append((k, len(v)))
            flat.extend(v)
        else:
            layout.append((k, 0))
            flat.append(v)

    def kernel(*refs):
        names = list(inputs) + list(outs)
        bound = list(refs[: len(names)])
        at = len(names)
        for k, count in layout:
            names.append(k)
            if count:
                bound.append(refs[at : at + count])
                at += count
            else:
                bound.append(refs[at])
                at += 1
        mega_kernel(n, names, *bound)

    res = pl.pallas_call(
        kernel,
        out_shape=[jax.ShapeDtypeStruct(*v) for v in outs.values()],
        in_specs=[pl.BlockSpec(memory_space=pl.ANY if k in hbm else pltpu.VMEM) for k in inputs],
        out_specs=[pl.BlockSpec(memory_space=pltpu.VMEM)] * len(outs),
        scratch_shapes=flat,
        compiler_params=pltpu.CompilerParams(
            collective_id=0, has_side_effects=True, vmem_limit_bytes=67043328
        ),
        name="block_step",
    )(*inputs.values())
    o = SimpleNamespace(**dict(zip(outs, res)))

    def rows_of(a, total):
        w = a.shape[2]
        keep = total - w
        return jnp.concatenate(
            [jnp.concatenate([a[cc], a[2 + cc][:, w - (up_to(total, 128) - w) : w - (up_to(total, 128) - total)]], axis=1) for cc in range(2)],
            axis=0,
        ).astype(F32)

    def cols_of(a, total):
        w = a.shape[1]
        return jnp.concatenate(
            [jnp.concatenate([a[cc], a[2 + cc][w - (up_to(total, 128) - w) : w - (up_to(total, 128) - total)]], axis=0) for cc in range(2)],
            axis=1,
        ).astype(F32)

    gq = rows_of(o.out_q, 2 * qk + vw)
    lo = lax.axis_index("fsdp") * (width // n)
    mine = lax.dynamic_slice_in_dim(o.sums, lo, width // n, axis=1)
    loss = jnp.sum(o.sums[2]) / (o.sums[3, 0] * width)
    return (
        o.layer_out[None],
        o.grad_in[None],
        mine[0],
        gq[:, :qk],
        gq[:, qk : 2 * qk],
        gq[:, 2 * qk :],
        cols_of(o.out_o, vw),
        mine[1],
        rows_of(o.out_g, ff),
        rows_of(o.out_u, ff),
        cols_of(o.out_d, ff),
        loss,
    )


def per_device(*arrays):
    n = lax.axis_size("fsdp")
    layer_in, w_query, w_value = arrays[0], arrays[5], arrays[7]
    fits = (
        lax.axis_size("ctx") == 4
        and lax.axis_size("tp") == 2
        and layer_in.shape[0] == 1
        and w_query.shape[0] == 256
        and w_query.shape[1] == 128
        and w_value.shape[1] % 512 == 0
        and layer_in.shape[1] % 256 == 0
    )
    return mega(n, *arrays) if fits else general(*arrays)


def solution(mesh):
    placed = (
        P("fsdp", "ctx", None),
        P("fsdp", "ctx"),
        P("fsdp", "ctx"),
        P("fsdp", "ctx", None),
        P("fsdp"),
        P("fsdp", "tp"),
        P("fsdp", "tp"),
        P("fsdp", "tp"),
        P("tp", "fsdp"),
        P("fsdp"),
        P("fsdp", "tp"),
        P("fsdp", "tp"),
        P("tp", "fsdp"),
    )
    return jax.shard_map(
        per_device,
        mesh=mesh,
        in_specs=placed,
        out_specs=(
            P("fsdp", "ctx", None),
            P("fsdp", "ctx", None),
            P("fsdp"),
            P("fsdp", "tp"),
            P("fsdp", "tp"),
            P("fsdp", "tp"),
            P("tp", "fsdp"),
            P("fsdp"),
            P("fsdp", "tp"),
            P("fsdp", "tp"),
            P("tp", "fsdp"),
            P(),
        ),
        check_vma=False,
    )
```

```python
from functools import partial
from types import SimpleNamespace
import math

import jax
import jax.numpy as jnp
from jax import lax
from jax.experimental import pallas as pl
from jax.experimental.pallas import tpu as pltpu
from jax.sharding import PartitionSpec as P

FEAT = 16
HEAD_V = 64


EPSILON = 1e-05
HIGH = lax.Precision.HIGHEST
QUAD_SCALE = 1.0 / (4.0 * math.sqrt(2.0))


def entering(x, axis, join, neutral):
    place = lax.axis_index(axis)
    gathered = jax.tree.map(
        lambda a, kind: lax.all_gather(a.astype(kind), axis),
        x,
        (jnp.bfloat16, jnp.bfloat16, jnp.bfloat16),
    )
    state = jax.tree.map(lambda a, e: jnp.zeros_like(a) + jnp.asarray(e, a.dtype), x, neutral)

    def one(lap, state):
        return join(
            state,
            jax.tree.map(
                lambda a, own: lax.dynamic_index_in_dim(a, lap, 0, False).astype(own.dtype),
                gathered,
                x,
            ),
        )

    return lax.fori_loop(0, place, one, state)


def entering_2(x, axis, combine, identity):
    devices, here = (lax.axis_size(axis), lax.axis_index(axis))
    everything = jax.tree.map(
        lambda part, kind: lax.all_gather(part.astype(kind), axis),
        x,
        jax.tree.map(lambda a: jnp.bfloat16 if a.dtype == jnp.float32 else a.dtype, x),
    )
    start = jax.tree.map(
        lambda part, zero: jnp.broadcast_to(jnp.asarray(zero, part.dtype), part.shape), x, identity
    )

    def lap(k, before):
        at = devices - 1 - k
        reached = at > here
        new = combine(
            before, jax.tree.map(lambda part, own: part[at].astype(own.dtype), everything, x)
        )
        return jax.tree.map(lambda a, b: jnp.where(reached, a, b), new, before)

    return lax.fori_loop(0, devices, lap, start)


def product(left_side, right_side):
    return jnp.dot(left_side, right_side, preferred_element_type=jnp.float32)


def product_left_t(left_side, right_side):
    return lax.dot_general(
        left_side, right_side, (((0,), (0,)), ((), ())), preferred_element_type=jnp.float32
    )


def product_right_t(left_side, right_side):
    return lax.dot_general(
        left_side, right_side, (((1,), (1,)), ((), ())), preferred_element_type=jnp.float32
    )


def features(vectors):
    lead_dims = vectors.shape[:-1]
    feat_width = vectors.shape[-1]
    square = (vectors[..., :, None] * vectors[..., None, :]).reshape(
        lead_dims + (feat_width * feat_width,)
    )
    return jnp.concatenate(
        [jnp.ones(lead_dims + (1,), jnp.float32), 0.5 * vectors, QUAD_SCALE * square], axis=-1
    )


def attend(query_rows, key_rows, value_rows, prev_state, prev_norm, segment, prev_id):
    scores = jnp.einsum("slhf,smhf->shlm", query_rows, key_rows, precision=HIGH) * 0.25
    kernel = 1.0 + scores + 0.5 * scores * scores
    places = jnp.arange(segment.shape[1])
    allowed = (places[:, None] >= places[None, :])[None] & (
        segment[:, :, None] == segment[:, None, :]
    )
    kernel = jnp.where(allowed[:, None], kernel, 0.0)
    carried = (segment.astype(jnp.float32) == prev_id[:, None]).astype(jnp.float32)
    mapped = features(query_rows) * carried[:, :, None, None]
    numerator = jnp.einsum("shlm,smhv->slhv", kernel, value_rows, precision=HIGH) + jnp.einsum(
        "slht,shtv->slhv", mapped, prev_state, precision=HIGH
    )
    denominator = jnp.einsum("shlm->slh", kernel) + jnp.einsum(
        "slht,sht->slh", mapped, prev_norm, precision=HIGH
    )
    return numerator / denominator[..., None]


def summarize(key_rows, value_rows, segment):
    closing = (segment == segment[:, -1:]).astype(jnp.float32)
    mapped = features(key_rows) * closing[:, :, None, None]
    return (
        jnp.einsum("slht,slhv->shtv", mapped, value_rows, precision=HIGH),
        jnp.sum(mapped, axis=1),
    )


def rms_forward(values_in, gain_vec):
    inv_root = lax.rsqrt(jnp.mean(values_in * values_in, axis=-1, keepdims=True) + EPSILON)
    return (values_in * inv_root * gain_vec, inv_root)


def rms_backward(values_in, inv_root, gain_vec, grad_normed):
    weighted = grad_normed * gain_vec
    grad_gain = jnp.sum(grad_normed * values_in * inv_root, axis=0)
    grad_values = inv_root * weighted - values_in * inv_root**3 * jnp.mean(
        weighted * values_in, axis=-1, keepdims=True
    )
    return (grad_values, grad_gain)


def chain_combine(earlier, later):
    is_fresh = later[0] < 0
    same_doc = later[0] == earlier[0]

    def pick(early_part, late_part):
        expand = (-1,) + (1,) * (early_part.ndim - 1)
        with_early = late_part + jnp.where(same_doc.reshape(expand), early_part, 0.0)
        return jnp.where(is_fresh.reshape(expand), early_part, with_early)

    return (
        jnp.where(is_fresh, earlier[0], later[0]),
        pick(earlier[1], later[1]),
        pick(earlier[2], later[2]),
    )


def tp_forward(partial_sum):
    return lax.psum(partial_sum, "tp")


def tp_backward(partial_sum):
    return lax.psum(partial_sum.astype(jnp.bfloat16), "tp").astype(jnp.float32)


def general(
    layer_in,
    segment_ids,
    valid_mask,
    teacher,
    attn_gain,
    w_query,
    w_key,
    w_value,
    w_out,
    ffn_gain,
    w_gate,
    w_up,
    w_down,
):
    full_weights = (
        lax.all_gather(attn_gain, "fsdp", axis=0, tiled=True),
        lax.all_gather(w_query, "fsdp", axis=0, tiled=True),
        lax.all_gather(w_key, "fsdp", axis=0, tiled=True),
        lax.all_gather(w_value, "fsdp", axis=0, tiled=True),
        lax.all_gather(w_out, "fsdp", axis=1, tiled=True),
        lax.all_gather(ffn_gain, "fsdp", axis=0, tiled=True),
        lax.all_gather(w_gate, "fsdp", axis=0, tiled=True),
        lax.all_gather(w_up, "fsdp", axis=0, tiled=True),
        lax.all_gather(w_down, "fsdp", axis=1, tiled=True),
    )
    (
        gain_one,
        full_query,
        full_key,
        full_value,
        full_out,
        gain_two,
        full_gate,
        full_up,
        full_down,
    ) = full_weights
    seq_count, shard_len, model_width = layer_in.shape
    row_count = seq_count * shard_len
    heads_here = full_query.shape[1] // FEAT
    rows_in = layer_in.reshape(row_count, model_width).astype(jnp.float32)
    normed_full, root_one = rms_forward(rows_in, gain_one.astype(jnp.float32))
    normed_one = normed_full.astype(jnp.bfloat16)
    query_rows = product(normed_one, full_query).reshape(seq_count, shard_len, heads_here, FEAT)
    key_rows = product(normed_one, full_key).reshape(seq_count, shard_len, heads_here, FEAT)
    value_rows = product(normed_one, full_value).reshape(seq_count, shard_len, heads_here, HEAD_V)
    last_id = segment_ids[:, -1].astype(jnp.float32)
    first_id = segment_ids[:, 0].astype(jnp.float32)
    (out_state, out_norm), summary_pull = jax.vjp(
        partial(summarize, segment=segment_ids), key_rows, value_rows
    )
    blank_state = jnp.zeros_like(out_state)
    blank_norm = jnp.zeros_like(out_norm)
    no_doc = jnp.full_like(last_id, -1.0)
    prev_id, prev_state, prev_norm = entering(
        (last_id, out_state, out_norm), "ctx", chain_combine, (no_doc, blank_state, blank_norm)
    )
    attended, attend_pull = jax.vjp(
        partial(attend, segment=segment_ids, prev_id=prev_id),
        query_rows,
        key_rows,
        value_rows,
        prev_state,
        prev_norm,
    )
    mixed_heads = attended.reshape(row_count, heads_here * HEAD_V).astype(jnp.bfloat16)
    head_sum = product(mixed_heads, full_out)
    teacher_rows = teacher.reshape(row_count, model_width).astype(jnp.float32)
    weight_rows = valid_mask.reshape(row_count, 1).astype(jnp.float32)
    middle = rows_in + tp_forward(head_sum)
    normed_mid, root_two = rms_forward(middle, gain_two.astype(jnp.float32))
    normed_two = normed_mid.astype(jnp.bfloat16)
    gate_rows = product(normed_two, full_gate)
    up_rows = product(normed_two, full_up)
    sigmoid_gate = jax.nn.sigmoid(gate_rows)
    silu_gate = gate_rows * sigmoid_gate
    hidden = (silu_gate * up_rows).astype(jnp.bfloat16)
    down_sum = product(hidden, full_down)
    output = middle + tp_forward(down_sum)
    misfit = (output - teacher_rows) * weight_rows
    layer_rows = output.astype(jnp.bfloat16)
    grad_rows = misfit.astype(jnp.bfloat16)
    sum_squares = jnp.sum(misfit * misfit)
    sum_valid = jnp.sum(weight_rows)
    grad_down = product_left_t(hidden, grad_rows)
    grad_hidden = product_right_t(grad_rows, full_down)
    grad_gate_rows = (
        grad_hidden * up_rows * sigmoid_gate * (1.0 + gate_rows * (1.0 - sigmoid_gate))
    ).astype(jnp.bfloat16)
    grad_up_rows = (grad_hidden * silu_gate).astype(jnp.bfloat16)
    grad_gate = product_left_t(normed_two, grad_gate_rows)
    grad_up = product_left_t(normed_two, grad_up_rows)
    normed_two_terms = product_right_t(grad_gate_rows, full_gate) + product_right_t(
        grad_up_rows, full_up
    )
    grad_normed_two = tp_backward(normed_two_terms)
    grad_mid_norm, grad_ffn_gain = rms_backward(
        middle, root_two, gain_two.astype(jnp.float32), grad_normed_two
    )
    grad_middle = misfit + grad_mid_norm
    grad_branch = grad_middle.astype(jnp.bfloat16)
    grad_out = product_left_t(mixed_heads, grad_branch)
    grad_mixed = product_right_t(grad_branch, full_out).reshape(
        seq_count, shard_len, heads_here, HEAD_V
    )
    grad_q_near, grad_k_near, grad_v_near, grad_prev_state, grad_prev_norm = attend_pull(grad_mixed)
    next_id, later_state, later_norm = entering_2(
        (first_id, grad_prev_state, grad_prev_norm),
        "ctx",
        chain_combine,
        (no_doc, blank_state, blank_norm),
    )
    continues = (next_id == last_id).astype(jnp.float32)
    grad_k_far, grad_v_far = summary_pull(
        (later_state * continues[:, None, None, None], later_norm * continues[:, None, None])
    )
    grad_query_rows = grad_q_near.reshape(row_count, heads_here * FEAT).astype(jnp.bfloat16)
    grad_key_rows = (
        (grad_k_near + grad_k_far).reshape(row_count, heads_here * FEAT).astype(jnp.bfloat16)
    )
    grad_value_rows = (
        (grad_v_near + grad_v_far).reshape(row_count, heads_here * HEAD_V).astype(jnp.bfloat16)
    )
    grad_query = product_left_t(normed_one, grad_query_rows)
    grad_key = product_left_t(normed_one, grad_key_rows)
    grad_value = product_left_t(normed_one, grad_value_rows)
    normed_one_terms = (
        product_right_t(grad_query_rows, full_query)
        + product_right_t(grad_key_rows, full_key)
        + product_right_t(grad_value_rows, full_value)
    )
    grad_normed_one = tp_backward(normed_one_terms)
    grad_rows_in, grad_attn_gain = rms_backward(
        rows_in, root_one, gain_one.astype(jnp.float32), grad_normed_one
    )
    grad_in_rows = (grad_middle + grad_rows_in).astype(jnp.bfloat16)
    total_sq, total_valid = lax.psum((sum_squares, sum_valid), ("fsdp", "ctx"))
    loss_value = total_sq / (total_valid * model_width)
    grad_in = grad_in_rows.reshape(seq_count, shard_len, model_width)
    layer_out = layer_rows.reshape(seq_count, shard_len, model_width)
    owned = (
        lax.psum_scatter(
            grad_attn_gain.astype(jnp.bfloat16), "fsdp", scatter_dimension=0, tiled=True
        ).astype(jnp.float32),
        lax.psum_scatter(
            grad_query.astype(jnp.bfloat16), "fsdp", scatter_dimension=0, tiled=True
        ).astype(jnp.float32),
        lax.psum_scatter(
            grad_key.astype(jnp.bfloat16), "fsdp", scatter_dimension=0, tiled=True
        ).astype(jnp.float32),
        lax.psum_scatter(
            grad_value.astype(jnp.bfloat16), "fsdp", scatter_dimension=0, tiled=True
        ).astype(jnp.float32),
        lax.psum_scatter(
            grad_out.astype(jnp.bfloat16), "fsdp", scatter_dimension=1, tiled=True
        ).astype(jnp.float32),
        lax.psum_scatter(
            grad_ffn_gain.astype(jnp.bfloat16), "fsdp", scatter_dimension=0, tiled=True
        ).astype(jnp.float32),
        lax.psum_scatter(
            grad_gate.astype(jnp.bfloat16), "fsdp", scatter_dimension=0, tiled=True
        ).astype(jnp.float32),
        lax.psum_scatter(
            grad_up.astype(jnp.bfloat16), "fsdp", scatter_dimension=0, tiled=True
        ).astype(jnp.float32),
        lax.psum_scatter(
            grad_down.astype(jnp.bfloat16), "fsdp", scatter_dimension=1, tiled=True
        ).astype(jnp.float32),
    )
    shares = (
        lax.psum(owned[0].astype(jnp.bfloat16), "ctx").astype(jnp.float32),
        lax.psum(owned[1].astype(jnp.bfloat16), "ctx").astype(jnp.float32),
        lax.psum(owned[2].astype(jnp.bfloat16), "ctx").astype(jnp.float32),
        lax.psum(owned[3].astype(jnp.bfloat16), "ctx").astype(jnp.float32),
        lax.psum(owned[4].astype(jnp.bfloat16), "ctx").astype(jnp.float32),
        lax.psum(owned[5].astype(jnp.bfloat16), "ctx").astype(jnp.float32),
        lax.psum(owned[6].astype(jnp.bfloat16), "ctx").astype(jnp.float32),
        lax.psum(owned[7].astype(jnp.bfloat16), "ctx").astype(jnp.float32),
        lax.psum(owned[8].astype(jnp.bfloat16), "ctx").astype(jnp.float32),
    )
    return (
        layer_out,
        grad_in,
        shares[0],
        shares[1],
        shares[2],
        shares[3],
        shares[4],
        shares[5],
        shares[6],
        shares[7],
        shares[8],
        loss_value,
    )


MESH = pl.DeviceIdType.MESH
F32 = jnp.float32
BF16 = jnp.bfloat16


def up_to(size, step):
    return -(-size // step) * step


def mm(a, b):
    return jnp.dot(a, b, preferred_element_type=F32)


def mm_nt(a, b):
    return lax.dot_general(a, b, (((1,), (1,)), ((), ())), preferred_element_type=F32)


def mm_tn(a, b):
    return lax.dot_general(a, b, (((0,), (0,)), ((), ())), preferred_element_type=F32)


def at128(offset):
    return pl.multiple_of(offset, 128)


class Place:
    def __init__(self, n):
        self.n = n
        self.z = lax.axis_index("fsdp")
        self.b = lax.axis_index("ctx")
        self.t = lax.axis_index("tp")
        self.x = self.b // 2
        self.c = self.b % 2
        self.ic = self.x * 2 + (1 - self.c)
        self.xp = (1 - self.x) * 2 + self.c
        self.dg = (1 - self.x) * 2 + (1 - self.c)


def remote(src, dst, send, recv, **where):
    return pltpu.make_async_remote_copy(
        src_ref=src, dst_ref=dst, send_sem=send, recv_sem=recv, device_id=where, device_id_type=MESH
    )


def entry_barrier(p):
    sem = pltpu.get_barrier_semaphore()
    for s in range(p.n):

        @pl.when(p.z != s)
        def _():
            pl.semaphore_signal(sem, inc=1, device_id={"fsdp": s}, device_id_type=MESH)

    for peer in (p.ic, p.xp, p.dg):
        pl.semaphore_signal(sem, inc=1, device_id={"ctx": peer}, device_id_type=MESH)
    pl.semaphore_signal(sem, inc=1, device_id={"tp": 1 - p.t}, device_id_type=MESH)
    pl.semaphore_wait(sem, p.n - 1 + 4)


class Gather:
    def __init__(self, p, pieces, sems):
        self.p = p
        self.pieces = pieces
        (self.zr, self.xr, self.i1r, self.i2r, self.zsl, self.zsr, self.xs, self.i1s, self.i2s) = sems

    def quarter(self, g, s, x, c):
        ref, kind, lo, size = self.pieces[g]
        n = self.p.n
        if kind == "row":
            return ref.at[pl.ds(pl.multiple_of((c * n + s) * 128 + x * 64 + lo[0], 16), size), 0 : lo[1]]
        half = lo[1]
        return ref.at[
            pl.ds(pl.multiple_of(x * half + lo[0], 16), size), pl.ds(at128((c * n + s) * 128), 128)
        ]

    def copy(self, g, s, x, c, send, recv, **where):
        ref = self.quarter(g, s, x, c)
        return remote(ref, ref, send.at[g, s], recv.at[g, s], **where)

    def left(self, g, s):
        return self.copy(g, s, self.p.x, self.p.c, self.zsl, self.zr, fsdp=self.p.z - 1)

    def right(self, g, s):
        return self.copy(g, s, self.p.x, self.p.c, self.zsr, self.zr, fsdp=self.p.z + 1)

    def chip(self, g, s, x, c, second):
        if second:
            return self.copy(g, s, x, c, self.i2s, self.i2r, ctx=self.p.ic)
        return self.copy(g, s, x, c, self.i1s, self.i1r, ctx=self.p.ic)

    def cross(self, g, s, x, c):
        return self.copy(g, s, x, c, self.xs, self.xr, ctx=self.p.xp)

    def own(self, g):
        p = self.p

        @pl.when(p.z > 0)
        def _():
            self.left(g, p.z).start()

        @pl.when(p.z < p.n - 1)
        def _():
            self.right(g, p.z).start()

    def hop(self, g, h):
        p = self.p
        for d in (1, -1):
            s = p.z + d * h
            there = (s < p.n) if d == 1 else (s >= 0)

            @pl.when(there)
            def _():
                self.copy(g, s, p.x, p.c, self.zsl, self.zr, fsdp=p.z).wait_recv()
                if d == 1:

                    @pl.when(p.z > 0)
                    def _():
                        self.left(g, s).start()

                else:

                    @pl.when(p.z < p.n - 1)
                    def _():
                        self.right(g, s).start()

                self.cross(g, s, p.x, p.c).start()
                self.chip(g, s, p.x, p.c, False).start()

    def hop_cross(self, g, h):
        p = self.p
        for d in (1, -1):
            s = p.z + d * h
            there = (s < p.n) if d == 1 else (s >= 0)

            @pl.when(there)
            def _():
                self.cross(g, s, 1 - p.x, p.c).wait_recv()
                self.chip(g, s, 1 - p.x, p.c, True).start()

    def finish(self, g):
        p = self.p

        @pl.loop(0, p.n)
        def _(s):
            @pl.when(s != p.z)
            def _():
                self.chip(g, s, p.x, 1 - p.c, False).wait_recv()
                self.chip(g, s, 1 - p.x, 1 - p.c, True).wait_recv()

    def drain(self):
        p = self.p
        for g in range(len(self.pieces)):

            @pl.loop(0, p.n)
            def _(s):
                @pl.when((s >= p.z) & (p.z > 0))
                def _():
                    self.left(g, s).wait_send()

                @pl.when((s <= p.z) & (p.z < p.n - 1))
                def _():
                    self.right(g, s).wait_send()

                @pl.when(s != p.z)
                def _():
                    self.cross(g, s, p.x, p.c).wait_send()
                    self.chip(g, s, p.x, p.c, False).wait_send()
                    self.chip(g, s, 1 - p.x, p.c, True).wait_send()


class Reduce:
    def __init__(self, p, parts, seen, done, other, sems):
        self.p = p
        self.parts = parts
        self.seen = seen
        self.done = done
        self.other = other
        (self.ss, self.rs, self.fs, self.fr) = sems

    def move(self, g, s, slot, to):
        return remote(
            self.parts[g].at[s], self.seen[g].at[slot], self.ss.at[g, s], self.rs.at[g, slot], fsdp=to
        )

    def arrived(self, g, slot):
        self.move(g, 0, slot, self.p.z).wait_recv()

    def by_rows(self, g, body):
        @pl.loop(0, self.parts[g].shape[1] // 128)
        def _(i):
            body(pl.ds(at128(i * 128), 128))

    def add(self, g, s, slot):
        def body(at):
            total = self.parts[g][s, at, :].astype(F32) + self.seen[g][slot, at, :].astype(F32)
            self.parts[g][s, at, :] = total.astype(BF16)

        self.by_rows(g, body)

    def stage(self, g, k):
        p = self.p
        n = p.n

        @pl.when(p.z == k)
        def _():
            for s in range(n - 1, k, -1):
                if k > 0:
                    self.arrived(g, s)
                    self.add(g, s, s)
                self.move(g, s, s, k + 1).start()

        @pl.when(p.z == n - 1 - k)
        def _():
            z = n - 1 - k
            for s in range(0, z):
                if k > 0:
                    self.arrived(g, s)
                    self.add(g, s, s)
                self.move(g, s, n if s == z - 1 else s, z - 1).start()

    def last(self, g):
        p = self.p
        n = p.n

        @pl.when(p.z > 0)
        def _():
            self.arrived(g, p.z)
            self.add(g, p.z, p.z)

        @pl.when(p.z < n - 1)
        def _():
            self.arrived(g, n)
            self.add(g, p.z, n)

        if self.other[g] is not None:
            self.across(g).start()
            return
        self.block(g, p.x, p.c)[...] = self.mine(g)[...]
        self.spread(g, p.b, 0, p.ic, self.mine(g)).start()
        self.spread(g, p.b, 1, p.xp, self.mine(g)).start()

    def mine(self, g):
        p = self.p
        half = self.done[g].shape[0] // 2
        skip = self.parts[g].shape[1] - half
        return self.parts[g].at[p.z, pl.ds(pl.multiple_of(p.x * skip, 16), half), :]

    def block(self, g, x, c):
        half = self.done[g].shape[0] // 2
        return self.done[g].at[pl.ds(pl.multiple_of(x * half, 16), half), pl.ds(at128(c * 128), 128)]

    def spread(self, g, slot, which, to, src=None):
        dst = self.block(g, slot // 2, slot % 2)
        return remote(dst if src is None else src, dst, self.fs.at[g, which], self.fr.at[g, slot], ctx=to)

    def side(self, g, c):
        at = pl.ds(at128(c * 128), 128)
        if self.done[g].shape[1] == 256:
            return self.done[g].at[:, at]
        return self.done[g].at[at, :]

    def across(self, g):
        p = self.p
        return remote(self.parts[g].at[p.z], self.other[g], self.fs.at[g, 0], self.fr.at[g, 0], ctx=p.xp)

    def beside(self, g, c):
        ref = self.side(g, c)
        return remote(ref, ref, self.fs.at[g, 1], self.fr.at[g, 1], ctx=self.p.ic)

    def relay(self, g):
        p = self.p
        if self.other[g] is not None:
            self.across(g).wait_recv()

            side = self.side(g, p.c)

            def body(at):
                total = self.parts[g][p.z, at, :].astype(F32) + self.other[g][at, :].astype(F32)
                side[at, :] = total.astype(BF16)

            self.by_rows(g, body)
            self.beside(g, p.c).start()
            return
        self.spread(g, p.xp, 1, p.xp).wait_recv()
        self.spread(g, p.xp, 2, p.ic).start()

    def finish(self, g):
        p = self.p
        if self.other[g] is not None:
            self.beside(g, 1 - p.c).wait_recv()
            self.beside(g, p.c).wait_send()
            self.across(g).wait_send()
        else:
            self.spread(g, p.ic, 0, p.ic).wait_recv()
            self.spread(g, p.dg, 2, p.ic).wait_recv()
            self.spread(g, p.b, 0, p.ic, self.mine(g)).wait_send()
            self.spread(g, p.b, 1, p.xp, self.mine(g)).wait_send()
            self.spread(g, p.xp, 2, p.ic).wait_send()

        @pl.loop(0, p.n)
        def _(s):
            @pl.when(s != p.z)
            def _():
                self.move(g, s, 0, p.z).wait_send()


class Columns:
    def __init__(self, p, k, src, dst, sems):
        self.p = p
        self.k = k
        self.src = src
        self.dst = dst
        self.send, self.recv = sems

    def slot(self, b):
        rows = self.src.shape[0]
        return self.dst.at[pl.ds(pl.multiple_of(b * rows, rows), rows), :]

    def copy(self, peer, which):
        p = self.p
        w = self.dst.shape[1]
        part = self.src.at[:, pl.ds(at128((peer % 2) * w), w)]
        return remote(part, self.slot(p.b), self.send.at[self.k, which], self.recv.at[self.k, p.b], ctx=peer)

    def start(self):
        p = self.p
        w = self.dst.shape[1]
        for which, peer in enumerate((p.xp, p.dg, p.ic)):
            self.copy(peer, which).start()
        self.slot(p.b)[...] = self.src[:, pl.ds(at128(p.c * w), w)]

    def wait(self):
        p = self.p
        for peer in (p.ic, p.xp, p.dg):
            remote(self.slot(peer), self.slot(peer), self.send.at[self.k, 0], self.recv.at[self.k, peer], ctx=peer).wait_recv()

    def drain(self):
        p = self.p
        for which, peer in enumerate((p.xp, p.dg, p.ic)):
            self.copy(peer, which).wait_send()


class Pair:
    def __init__(self, p, k, src, dst, sems):
        self.p = p
        self.k = k
        self.src = src
        self.dst = dst
        self.send, self.recv = sems

    def slot(self, c):
        rows = self.src.shape[0]
        return self.dst.at[pl.ds(pl.multiple_of(c * rows, rows), rows), :]

    def part(self, c):
        w = self.dst.shape[1]
        if w == self.src.shape[1]:
            return self.src
        return self.src.at[:, pl.ds(at128(c * w), w)]

    def copy(self):
        p = self.p
        return remote(self.part(1 - p.c), self.slot(p.c), self.send.at[self.k], self.recv.at[self.k], ctx=p.ic)

    def start(self):
        c = self.p.c
        self.copy().start()
        self.slot(c)[...] = self.part(c)[...]

    def wait(self):
        p = self.p
        remote(self.part(1 - p.c), self.slot(1 - p.c), self.send.at[self.k], self.recv.at[self.k], ctx=p.ic).wait_recv()

    def drain(self):
        self.copy().wait_send()


class Halves:
    def __init__(self, p, k, src, dst, step, sems):
        self.p = p
        self.k = k
        self.src = src
        self.dst = dst
        self.step = step
        self.send, self.recv = sems

    def slot(self, b):
        rows = self.src.shape[0]
        return self.dst.at[pl.ds(pl.multiple_of(b * rows, rows), rows), :]

    def part(self, x):
        return self.src.at[:, pl.ds(at128(x * self.step), self.dst.shape[1])]

    def to(self, src, slot, which, peer):
        return remote(src, self.slot(slot), self.send.at[self.k, which], self.recv.at[self.k, slot], ctx=peer)

    def start(self):
        p = self.p
        self.to(self.part(1 - p.x), p.b, 0, p.xp).start()
        self.to(self.part(p.x), p.b, 1, p.ic).start()
        self.slot(p.b)[...] = self.src[:, pl.ds(at128(p.x * self.step), self.dst.shape[1])]

    def relay(self):
        p = self.p
        self.to(self.slot(p.xp), p.xp, 2, p.ic).wait_recv()
        self.to(self.slot(p.xp), p.xp, 2, p.ic).start()

    def wait(self):
        p = self.p
        self.to(self.slot(p.ic), p.ic, 1, p.ic).wait_recv()
        self.to(self.slot(p.dg), p.dg, 1, p.ic).wait_recv()

    def drain(self):
        p = self.p
        self.to(self.part(1 - p.x), p.b, 0, p.xp).wait_send()
        self.to(self.part(p.x), p.b, 1, p.ic).wait_send()
        self.to(self.slot(p.xp), p.xp, 2, p.ic).wait_send()


def mega_kernel(n, names, *refs):
    r = SimpleNamespace(**dict(zip(names, refs)))
    p = Place(n)
    z, b, x, c = p.z, p.b, p.x, p.c
    rows_here = r.x.shape[0]
    width = r.x.shape[1]
    half_d = width // 2
    heads = r.wv.shape[1] // HEAD_V
    qk = r.wq.shape[1]
    vw = r.wv.shape[1]
    ff = r.wd.shape[0]
    ffp = r.hid.shape[1]
    order = [s * 256 + cc * 128 for cc in range(2) for s in range(n)]
    blocks = width // 256
    D = r.lsem

    fqkv, fo, fg, fu, fd = r.fqkv, r.fo, r.fg, r.fu, r.fd
    local = []

    def bring(src, dst):
        copy = pltpu.make_async_copy(src, dst, D.at[len(local)])
        copy.start()
        local.append(copy)
        return copy

    get_x = bring(r.x, r.xv)
    need = {}
    for cc in range(2):
        rows = pl.ds(at128((cc * n + z) * 128), 128)
        src = slice(cc * 128, cc * 128 + 128)
        need.setdefault("qkv", []).extend(
            (
                bring(r.wq.at[src, :], fqkv.at[rows, 0:qk]),
                bring(r.wk.at[src, :], fqkv.at[rows, qk : 2 * qk]),
                bring(r.wv.at[src, :], fqkv.at[rows, 2 * qk : 2 * qk + vw]),
            )
        )
    for cc in range(2):
        cols = pl.ds(at128((cc * n + z) * 128), 128)
        need.setdefault("o", []).append(bring(r.wo.at[:, cc * 128 : cc * 128 + 128], fo.at[:, cols]))
    for key, src, dst in (("g", r.wg, fg), ("u", r.wu, fu), ("d", r.wd, fd)):
        for cc in range(2):
            cols = pl.ds(at128((cc * n + z) * 128), 128)
            need.setdefault(key, []).append(bring(src.at[:, cc * 128 : cc * 128 + 128], dst.at[0:ff, cols]))
    get_teacher = bring(r.teacher, r.tv)

    pieces, first = [], []

    def split(total, parts):
        unit = total // 16
        edge = [(unit * i // parts) * 16 for i in range(parts + 1)]
        return [(edge[i], edge[i + 1] - edge[i]) for i in range(parts)]

    for key, ref, kind, total, parts in (
        ("qkv", fqkv, "row", 64, 1),
        ("o", fo, "col", vw // 2, 1),
        ("g", fg, "col", ff // 2, 2),
        ("u", fu, "col", ff // 2, 2),
        ("d", fd, "col", ff // 2, 2),
    ):
        for i, (lo, size) in enumerate(split(total, parts)):
            pieces.append((ref, kind, (lo, ref.shape[1]) if kind == "row" else (lo, total), size))
            first.append(need[key] if i == 0 else [])
    gather = Gather(p, pieces, r.gs)
    ng = len(pieces)

    def own(g):
        for copy in first[g]:
            copy.wait()
        gather.own(g)

    entry_barrier(p)
    own(0)
    own(1)

    r.gains[...] = jnp.concatenate(
        [r.attn_gain[...].astype(F32).reshape(1, -1), r.ffn_gain[...].astype(F32).reshape(1, -1)]
        + [jnp.zeros((6, width // n), F32)],
        axis=0,
    )
    segment = r.segment[...].astype(F32)
    r.segrow[...] = jnp.broadcast_to(segment, (8, rows_here))
    r.segcol[...] = jnp.transpose(jnp.broadcast_to(segment, (128, rows_here)))
    r.valid[...] = jnp.transpose(jnp.broadcast_to(r.real[...].astype(F32), (128, rows_here)))
    gsend, grecv, gath = r.gnsem[0], r.gnsem[1], r.gath
    for s in range(n):

        @pl.when(z != s)
        def _():
            remote(r.gains, gath.at[z], gsend.at[s], grecv.at[z], fsdp=s).start()

    gath[z] = r.gains[...]
    segs, segr = r.segsem[0], r.segsem[1]
    for i, peer in enumerate((p.ic, p.xp, p.dg)):
        remote(r.segrow, r.segall.at[b], segs.at[i], segr.at[b], ctx=peer).start()
    r.segall[b] = r.segrow[...]

    pad = ffp - ff
    if pad:
        for ref in (fg, fu, fd):
            ref[ff:ffp, :] = jnp.zeros((pad, width), BF16)

    for s in range(n):

        @pl.when(z != s)
        def _():
            remote(r.gains, gath.at[s], gsend.at[s], grecv.at[s], fsdp=s).wait_recv()

    for row in range(2):
        r.gain[row : row + 1, :] = jnp.concatenate(
            [gath[s, row : row + 1, cc * 128 : cc * 128 + 128] for cc in range(2) for s in range(n)], axis=1
        )

    events = [(g - 1.5, "own", g, 0) for g in range(2, ng)]
    for g in range(ng):
        for h in range(1, n):
            events.append((g + 0.7 * h, "hop", g, h))
            events.append((g + 0.7 * h + 0.8, "cross", g, h))
    events.sort()
    passed = [0]

    def advance(until):
        while passed[0] < len(events) and events[passed[0]][0] <= until:
            _, kind, g, h = events[passed[0]]
            if kind == "own":
                own(g)
            elif kind == "hop":
                gather.hop(g, h)
            else:
                gather.hop_cross(g, h)
            passed[0] += 1

    def ready(g_from, g_to):
        advance(max(e[0] for e in events if e[1] == "cross" and e[2] < g_to))
        for g in range(g_from, g_to):
            gather.finish(g)

    send_n1 = Pair(p, 0, r.n1, r.n1c, r.psem)
    send_da = Pair(p, 1, r.da, r.dac, r.psem)
    send_dy = Pair(p, 2, r.dy, r.dyc, r.psem)
    send_hid = Pair(p, 3, r.hid, r.hidx, r.psem)
    send_mix = Pair(p, 4, r.mix, r.mixx, r.psem)
    send_dqkv = Pair(p, 5, r.dqkv, r.dqkvx, r.psem)
    send_n2 = Columns(p, 0, r.n2, r.n2c, r.csem)
    fh = r.dgx.shape[1]
    send_dg = Halves(p, 0, r.dg, r.dgx, ffp - fh, r.hsem)
    send_du = Halves(p, 1, r.du, r.dux, ffp - fh, r.hsem)
    ysend, yrecv = r.ysend, r.yrecv

    def y_copy(i, ch):
        return remote(ysend.at[i, ch], yrecv.at[i, ch], r.ysem[0].at[i, ch], r.ysem[1].at[i, ch], tp=1 - p.t)

    def y_put(i, ch, value):
        ysend[i, ch] = value.astype(BF16)
        y_copy(i, ch).start()

    def y_wait(i, between=()):
        for ch in range(blocks):
            y_copy(i, ch).wait_recv()
            if ch < len(between):
                between[ch]()

    def y_rows(i, rs):
        return jnp.concatenate(
            [ysend[i, ch, rs, :].astype(F32) + yrecv[i, ch, rs, :].astype(F32) for ch in range(blocks)], axis=1
        )

    step_rows = 32
    row_steps = rows_here // step_rows

    def per_rows(body):
        @pl.loop(0, row_steps)
        def _(i):
            body(pl.ds(pl.multiple_of(i * step_rows, step_rows), step_rows))

    def x_rows(rs):
        return jnp.concatenate([r.xv[rs, o : o + 128] for o in order], axis=1).astype(F32)

    def rsq(v):
        return lax.rsqrt(jnp.mean(v * v, axis=1, keepdims=True) + EPSILON)

    get_x.wait()

    def norm_one(rs):
        v = x_rows(rs)
        r.n1[rs, :] = (v * rsq(v) * r.gain[0:1, :]).astype(BF16)

    per_rows(norm_one)
    ready(0, 1)
    kv = r.kv
    first_chunk = mm(r.n1[...], fqkv[:, 0 : 2 * qk])
    r.q[...] = first_chunk[:, 0:qk].astype(BF16)
    kv[b, :, 0:qk] = first_chunk[:, qk : 2 * qk].astype(BF16)
    for ch in range(vw // 256):
        lo = ch * 256
        kv[b, :, qk + lo : qk + lo + 256] = mm(r.n1[...], fqkv[:, 2 * qk + lo : 2 * qk + lo + 256]).astype(BF16)

    kvs, kvr = r.kvsem

    def kv_copy(slot, which, peer):
        return remote(kv.at[slot], kv.at[slot], kvs.at[which], kvr.at[slot], ctx=peer)

    @pl.when(x == 0)
    def _():
        kv_copy(b, 0, p.xp).start()

    @pl.when(c == 0)
    def _():
        kv_copy(b, 1, p.ic).start()

    for i, peer in enumerate((p.ic, p.xp, p.dg)):
        remote(r.segrow, r.segall.at[peer], segs.at[i], segr.at[peer], ctx=peer).wait_recv()
    mask, num, den = r.mask, r.num, r.den
    num[...] = jnp.zeros_like(num)
    den[...] = jnp.zeros_like(den)
    lane = lax.broadcasted_iota(jnp.int32, (1, 128), 1)

    def q_of(h):
        keep = (lane // FEAT) == h
        return jnp.where(keep, r.q[...], jnp.zeros((), BF16))

    def attend_block(j):
        same = r.segcol[:, 0:1] == r.segall[j, 0:1, :]
        ri = lax.broadcasted_iota(jnp.int32, (rows_here, rows_here), 0)
        ci = lax.broadcasted_iota(jnp.int32, (rows_here, rows_here), 1)
        reach = ri + jnp.where(j == b, 0, rows_here) >= ci
        mask[j] = jnp.where(same & reach, 1.0, 0.0)

        @pl.loop(0, heads // 2)
        def _(pair):
            at = pl.ds(at128(pair * 128), 128)
            vpair = kv[j, :, pl.ds(at128(qk + pair * 128), 128)]
            sums = []
            for e in range(2):
                s = mm_nt(q_of(pair * 2 + e), kv[j, :, 0:qk]) * 0.25
                w = (1.0 + s + 0.5 * s * s) * mask[j]
                sums.append((mm(w.astype(BF16), vpair), jnp.sum(w, axis=1, keepdims=True)))
            low_half = lane < HEAD_V
            num[:, at] += jnp.where(low_half, sums[0][0], sums[1][0])
            den[:, at] += jnp.where(low_half, sums[0][1], sums[1][1])

    attend_block(b)
    advance(3.3)

    @pl.when(x == 1)
    def _():
        kv_copy(c, 2, p.ic).wait_recv()
        kv_copy(c, 2, p.ic).start()

    @pl.when(c == 1)
    def _():
        kv_copy(p.ic, 1, p.ic).wait_recv()

    @pl.when(x == 1)
    def _():
        kv_copy(1 - c, 2, p.ic).wait_recv()

    @pl.loop(1, b + 1)
    def _(m):
        attend_block(b - m)

    inv = 1.0 / den[...]
    den[...] = inv
    num[...] = num[...] * inv
    r.mix[...] = num[...].astype(BF16)

    ready(1, 2)
    for ch in range(blocks):
        y_put(0, ch, mm(r.mix[...], fo[:, ch * 256 : ch * 256 + 256]))
    send_mix.start()
    send_n1.start()
    advance(4.5)
    y_wait(0, [lambda u=u: advance(u) for u in (5.0, 5.7, 6.3)])

    def norm_two(rs):
        v = x_rows(rs) + y_rows(0, rs)
        r.mid[rs, :] = v
        r.n2[rs, :] = (v * rsq(v) * r.gain[1:2, :]).astype(BF16)

    per_rows(norm_two)

    fchunks = -(-ffp // 256)

    def per_ff(body):
        @pl.loop(0, fchunks)
        def _(i):
            body(at128(jnp.minimum(i * 256, ffp - 256)))

    ready(2, 6)

    def wide(ref, off):
        return ref[pl.ds(off, 256), :]

    def forward_ff(off):
        g = mm_nt(r.n2[...], wide(fg, off))
        u = mm_nt(r.n2[...], wide(fu, off))
        r.g[:, pl.ds(off, 256)] = g
        r.u[:, pl.ds(off, 256)] = u
        sig = 1.0 / (1.0 + jnp.exp(-g))
        r.hid[:, pl.ds(off, 256)] = (g * sig * u).astype(BF16)

    per_ff(forward_ff)
    send_hid.start()
    ready(6, ng)
    for ch in range(blocks):
        y_put(1, ch, mm(r.hid[...], fd[:, ch * 256 : ch * 256 + 256]))
    send_n2.start()
    get_teacher.wait()
    small = r.small
    small[...] = jnp.zeros_like(small)
    y_wait(1)

    def finish_forward(rs):
        y = r.mid[rs, :] + y_rows(1, rs)
        t = jnp.concatenate([r.tv[rs, o : o + 128] for o in order], axis=1).astype(F32)
        m = (y - t) * r.valid[rs, 0:1]
        r.mis[rs, :] = m
        r.dy[rs, :] = m.astype(BF16)
        yb = y.astype(BF16)
        for i, o in enumerate(order):
            r.layer_out[rs, o : o + 128] = yb[:, i * 128 : i * 128 + 128]
        small[2:3, :] += jnp.sum(m * m, axis=0, keepdims=True)
        small[3:4, :] += jnp.broadcast_to(jnp.sum(r.valid[rs, :], axis=0, keepdims=True)[:, 0:1], (1, width))

    per_rows(finish_forward)
    send_dy.start()

    def backward_ff(off):
        dh = mm_nt(r.dy[...], fd[pl.ds(off, 256), :])
        g = r.g[:, pl.ds(off, 256)]
        u = r.u[:, pl.ds(off, 256)]
        sig = 1.0 / (1.0 + jnp.exp(-g))
        r.dg[:, pl.ds(off, 256)] = (dh * u * sig * (1.0 + g * (1.0 - sig))).astype(BF16)
        r.du[:, pl.ds(off, 256)] = (dh * g * sig).astype(BF16)

    per_ff(backward_ff)
    send_dg.start()
    send_du.start()
    for ch in range(blocks):
        cols = slice(ch * 256, ch * 256 + 256)
        y_put(2, ch, mm(r.dg[...], fg[:, cols]) + mm(r.du[...], fu[:, cols]))

    red = Reduce(
        p,
        [r.part[i] for i in range(5)],
        [r.seen[i] for i in range(5)],
        [r.out_d, r.out_g, r.out_u, r.out_o, r.out_q],
        [r.other[0], None, None, r.other[1], r.other[2]],
        r.rsem,
    )
    turned = r.turned

    def turn(src):
        w = src.shape[1]

        @pl.loop(0, src.shape[0] // rows_here)
        def _(i):
            at = pl.ds(pl.multiple_of(i * rows_here, rows_here), rows_here)
            turned[0:w, at] = jnp.transpose(src[at, :])

    def grad_rows(g, rhs):
        rows = r.part[g].shape[1]

        @pl.loop(0, rhs.shape[1] // 128 // 2 if rhs.shape[1] % 256 == 0 else rhs.shape[1] // 128)
        def _(i):
            w = 256 if rhs.shape[1] % 256 == 0 else 128
            at = pl.ds(at128(i * w), w)
            res = mm(turned[0 : n * rows, 0 : rhs.shape[0]], rhs[:, at]).astype(BF16)
            for s in range(n):
                r.part[g][s, :, at] = res[s * rows : s * rows + rows, :]

    def grad_cols(g, rhs):
        rows = r.part[g].shape[1]

        @pl.loop(0, -(-rows // 256))
        def _(i):
            at = pl.ds(at128(jnp.minimum(i * 256, rows - 256)), 256)
            res = mm(turned[at, 0 : rhs.shape[0]], rhs[...]).astype(BF16)
            for s in range(n):
                r.part[g][s, at, :] = res[:, s * 128 : s * 128 + 128]

    send_hid.wait()
    turn(r.hidx)
    send_dy.wait()
    grad_cols(0, r.dyc)
    red.stage(0, 0)
    send_dg.relay()

    y_wait(2)

    def norm_back(i, row, v, base, rs):
        dn = y_rows(i, rs)
        inv_root = rsq(v)
        w = dn * r.gain[row : row + 1, :]
        small[row : row + 1, :] += jnp.sum(dn * v * inv_root, axis=0, keepdims=True)
        m = jnp.mean(w * v, axis=1, keepdims=True)
        return base + inv_root * w - v * (inv_root * inv_root * inv_root * m)

    def middle_back(rs):
        d = norm_back(2, 1, r.mid[rs, :], r.mis[rs, :], rs)
        r.mis[rs, :] = d
        r.da[rs, :] = d.astype(BF16)

    per_rows(middle_back)
    send_da.start()
    send_du.relay()
    send_n2.wait()
    send_dg.wait()
    turn(r.dgx)
    grad_cols(1, r.n2c)
    red.stage(1, 0)

    dnum, dden = r.dnum, r.dden
    for ch in range(vw // 256):
        at = slice(ch * 256, ch * 256 + 256)
        d = mm_nt(r.da[...], fo[at, :]) * den[:, at]
        dnum[:, at] = d.astype(BF16)
        dden[:, at] = d * num[:, at]
    dkvp, dkv, dq = r.dkvp, r.dkv, r.dqf
    dq[...] = jnp.zeros_like(dq)

    def back_block(j):
        dkv[...] = jnp.zeros_like(dkv)

        @pl.loop(0, heads // 2)
        def _(pair):
            at = pl.ds(at128(pair * 128), 128)
            vat = pl.ds(at128(qk + pair * 128), 128)
            dv = []
            for e in range(2):
                h = pair * 2 + e
                qh = q_of(h)
                keep_v = (lane // HEAD_V) == e
                keep_q = (lane // FEAT) == h
                s = mm_nt(qh, kv[j, :, 0:qk]) * 0.25
                w = ((1.0 + s + 0.5 * s * s) * mask[j]).astype(BF16)
                dn = jnp.where(keep_v, dnum[:, at], jnp.zeros((), BF16))
                dd = jnp.sum(jnp.where(keep_v, dden[:, at], 0.0), axis=1, keepdims=True)
                dw = mm_nt(dn, kv[j, :, vat]) - dd
                ds = (dw * (1.0 + s) * (0.25 * mask[j])).astype(BF16)
                dv.append(mm_tn(w, dn))
                kh = jnp.where(keep_q, kv[j, :, 0:qk], jnp.zeros((), BF16))
                dq[...] += mm(ds, kh)
                dkv[:, 0:qk] += mm_tn(ds, qh)
            dkv[:, vat] = dv[0] + dv[1]

    @pl.loop(0, b)
    def _(j):
        back_block(j)
        dkvp[j] = dkv[...].astype(BF16)

    dks, dkr = r.dksem
    back = r.back

    def dk_copy(src, slot, which, peer):
        return remote(src, back.at[slot], dks.at[which], dkr.at[slot], ctx=peer)

    @pl.when(c == 1)
    def _():
        dk_copy(dkvp.at[p.ic], 0, 0, p.ic).start()

    @pl.when(x == 1)
    def _():
        dk_copy(dkvp.at[1 - c], 1, 1, p.ic).start()

    back_block(b)

    @pl.when(x == 1)
    def _():
        dk_copy(dkvp.at[1 - c], 1, 1, p.ic).wait_recv()
        dkvp[b] = (dkvp[c].astype(F32) + back[1].astype(F32)).astype(BF16)
        dk_copy(dkvp.at[b], 2, 2, p.xp).start()

    @pl.when(c == 0)
    def _():
        dk_copy(dkvp.at[b], 0, 0, p.ic).wait_recv()
        dkv[...] += back[0].astype(F32)

    dqkv = r.dqkv
    dqkv[:, 0:qk] = dq[...].astype(BF16)
    send_du.wait()
    turn(r.dux)
    grad_cols(2, r.n2c)
    red.stage(2, 0)
    red.stage(0, 1)
    send_da.wait()
    send_mix.wait()
    turn(r.mixx)
    grad_cols(3, r.dac)
    red.stage(3, 0)
    red.stage(1, 1)

    @pl.when(x == 0)
    def _():
        dk_copy(dkvp.at[b], 2, 2, p.xp).wait_recv()
        dkv[...] += back[2].astype(F32)

    dqkv[:, qk : 2 * qk + vw] = dkv[...].astype(BF16)
    send_dqkv.start()
    for ch in range(blocks):
        y_put(3, ch, mm_nt(dqkv[...], fqkv[ch * 256 : ch * 256 + 256, :]))
    send_n1.wait()
    turn(r.n1c)
    send_dqkv.wait()
    grad_rows(4, r.dqkvx)
    red.stage(4, 0)
    red.stage(0, 2)
    red.stage(2, 1)
    red.last(0)

    y_wait(3)

    def input_back(rs):
        d = norm_back(3, 0, x_rows(rs), r.mis[rs, :], rs).astype(BF16)
        for i, o in enumerate(order):
            r.grad_in[rs, o : o + 128] = d[:, i * 128 : i * 128 + 128]

    per_rows(input_back)

    sms, smr = r.smsem
    parts, lines = r.smctx, r.smz
    for i, peer in enumerate((p.ic, p.xp, p.dg)):
        remote(small, parts.at[b], sms.at[0, i], smr.at[0, b], ctx=peer).start()
    parts[b] = small[...]
    red.stage(3, 1)
    red.stage(1, 2)
    for i, peer in enumerate((p.ic, p.xp, p.dg)):
        remote(small, parts.at[peer], sms.at[0, i], smr.at[0, peer], ctx=peer).wait_recv()
    lines[n] = parts[0] + parts[1] + parts[2] + parts[3]
    for s in range(n):

        @pl.when(z != s)
        def _():
            remote(lines.at[n], lines.at[z], sms.at[1, s], smr.at[1, z], fsdp=s).start()

    red.last(1)
    red.stage(4, 1)
    red.stage(2, 2)
    red.last(2)
    red.relay(0)
    red.stage(3, 2)
    red.last(3)
    red.stage(4, 2)
    red.relay(1)
    red.last(4)
    for s in range(n):

        @pl.when(z != s)
        def _():
            remote(lines.at[n], lines.at[s], sms.at[1, s], smr.at[1, s], fsdp=s).wait_recv()

    total = jnp.zeros_like(small)
    for s in range(n):
        total += jnp.where(z == s, lines[n], lines[s])
    r.gain[...] = total
    for cc in range(2):
        at = pl.ds(at128((cc * n + z) * 128), 128)
        r.grad_attn[0:1, cc * 128 : cc * 128 + 128] = r.gain[0:1, at]
        r.grad_ffn[0:1, cc * 128 : cc * 128 + 128] = r.gain[1:2, at]
    r.loss[...] = jnp.sum(total[2:3, :], axis=1, keepdims=True) / (total[3:4, 0:1] * width)
    red.relay(2)
    red.relay(3)
    red.relay(4)
    for g in (4, 0, 1, 2, 3):
        red.finish(g)
        if g == 4:
            r.grad_q[...] = r.out_q[:, 0:qk].astype(F32)
            r.grad_k[...] = r.out_q[:, qk : 2 * qk].astype(F32)
            r.grad_v[...] = r.out_q[:, 2 * qk : 2 * qk + vw].astype(F32)

    gather.drain()
    for k in (send_n1, send_da, send_n2, send_dy, send_hid, send_dg, send_du, send_mix, send_dqkv):
        k.drain()
    for i in range(4):
        for ch in range(blocks):
            y_copy(i, ch).wait_send()
    for s in range(n):

        @pl.when(z != s)
        def _():
            remote(r.gains, gath.at[z], gsend.at[s], grecv.at[z], fsdp=s).wait_send()
            remote(lines.at[n], lines.at[z], sms.at[1, s], smr.at[1, z], fsdp=s).wait_send()

    for i, peer in enumerate((p.ic, p.xp, p.dg)):
        remote(r.segrow, r.segall.at[b], segs.at[i], segr.at[b], ctx=peer).wait_send()
        remote(small, parts.at[b], sms.at[0, i], smr.at[0, b], ctx=peer).wait_send()

    @pl.when(x == 0)
    def _():
        kv_copy(b, 0, p.xp).wait_send()

    @pl.when(c == 0)
    def _():
        kv_copy(b, 1, p.ic).wait_send()

    @pl.when(x == 1)
    def _():
        kv_copy(c, 2, p.ic).wait_send()
        dk_copy(dkvp.at[1 - c], 1, 1, p.ic).wait_send()
        dk_copy(dkvp.at[b], 2, 2, p.xp).wait_send()

    @pl.when(c == 1)
    def _():
        dk_copy(dkvp.at[p.ic], 0, 0, p.ic).wait_send()


def mega(n, layer_in, segment_ids, valid_mask, teacher, attn_gain, w_query, w_key, w_value, w_out, ffn_gain, w_gate, w_up, w_down):
    x = layer_in[0]
    rows, width = x.shape
    qk, vw, ff = w_query.shape[1], w_value.shape[1], w_gate.shape[1]
    ffp = up_to(ff, 128)
    fh = up_to(ffp // 2, 256)
    half_d = width // 2
    blocks = width // 256
    inputs = dict(
        x=x,
        teacher=teacher[0],
        wq=w_query,
        wk=w_key,
        wv=w_value,
        wo=w_out,
        wg=w_gate.T,
        wu=w_up.T,
        wd=w_down,
        attn_gain=attn_gain,
        ffn_gain=ffn_gain,
        segment=segment_ids,
        real=valid_mask,
    )
    hbm = list(inputs)[:9]
    outs = dict(
        layer_out=((rows, width), BF16),
        grad_in=((rows, width), BF16),
        out_d=((ffp, width // n), BF16),
        out_g=((ffp, width // n), BF16),
        out_u=((ffp, width // n), BF16),
        out_o=((vw, width // n), BF16),
        grad_q=((width // n, qk), F32),
        grad_k=((width // n, qk), F32),
        grad_v=((width // n, vw), F32),
        grad_attn=((1, width // n), F32),
        grad_ffn=((1, width // n), F32),
        loss=((1, 1), F32),
    )
    dma = pltpu.SemaphoreType.DMA
    ng = 8
    vm = pltpu.VMEM
    piece = [(ffp, 128), (fh, 128), (fh, 128), (vw, 128), (128, 2 * qk + vw)]
    scratch = dict(
        lsem=dma((20,)),
        gs=[dma((ng, n)) for _ in range(9)],
        gnsem=[dma((n,)), dma((n,))],
        segsem=[dma((3,)), dma((4,))],
        psem=[dma((6,)), dma((6,))],
        csem=[dma((1, 3)), dma((1, 4))],
        hsem=[dma((2, 3)), dma((2, 4))],
        ysem=[dma((4, blocks)), dma((4, blocks))],
        kvsem=[dma((3,)), dma((4,))],
        dksem=[dma((3,)), dma((3,))],
        rsem=[dma((5, n)), dma((5, n + 1)), dma((5, 3)), dma((5, 4))],
        smsem=[dma((2, max(n, 3))), dma((2, max(n, 4)))],
        fqkv=vm((width, 2 * qk + vw), BF16),
        fo=vm((vw, width), BF16),
        fg=vm((ffp, width), BF16),
        fu=vm((ffp, width), BF16),
        fd=vm((ffp, width), BF16),
        xv=vm((rows, width), BF16),
        tv=vm((rows, width), BF16),
        gath=vm((n, 8, width // n), F32),
        gain=vm((8, width), F32),
        gains=vm((8, width // n), F32),
        segrow=vm((8, rows), F32),
        segcol=vm((rows, 128), F32),
        valid=vm((rows, 128), F32),
        segall=vm((4, 8, rows), F32),
        n1=vm((rows, width), BF16),
        n2=vm((rows, width), BF16),
        dy=vm((rows, width), BF16),
        da=vm((rows, width), BF16),
        n1c=vm((2 * rows, half_d), BF16),
        n2c=vm((4 * rows, half_d), BF16),
        dyc=vm((2 * rows, half_d), BF16),
        dac=vm((2 * rows, half_d), BF16),
        hid=vm((rows, ffp), BF16),
        dg=vm((rows, ffp), BF16),
        du=vm((rows, ffp), BF16),
        mix=vm((rows, vw), BF16),
        dqkv=vm((rows, 2 * qk + vw), BF16),
        hidx=vm((2 * rows, ffp), BF16),
        dgx=vm((4 * rows, fh), BF16),
        dux=vm((4 * rows, fh), BF16),
        mixx=vm((2 * rows, vw), BF16),
        dqkvx=vm((2 * rows, 2 * qk + vw), BF16),
        ysend=vm((4, blocks, rows, 256), BF16),
        yrecv=vm((4, blocks, rows, 256), BF16),
        q=vm((rows, qk), BF16),
        kv=vm((4, rows, qk + vw), BF16),
        mask=vm((4, rows, rows), F32),
        num=vm((rows, vw), F32),
        den=vm((rows, vw), F32),
        mid=vm((rows, width), F32),
        mis=vm((rows, width), F32),
        g=vm((rows, ffp), F32),
        u=vm((rows, ffp), F32),
        small=vm((8, width), F32),
        smctx=vm((4, 8, width), F32),
        smz=vm((n + 1, 8, width), F32),
        dnum=vm((rows, vw), BF16),
        dden=vm((rows, vw), F32),
        dqf=vm((rows, qk), F32),
        dkv=vm((rows, qk + vw), F32),
        dkvp=vm((4, rows, qk + vw), BF16),
        back=vm((3, rows, qk + vw), BF16),
        turned=vm((max(ffp, half_d), 4 * rows), BF16),
        part=[vm((n,) + s, BF16) for s in piece],
        seen=[vm((n + 1,) + s, BF16) for s in piece],
        other=[vm(piece[i], BF16) for i in (0, 3, 4)],
        out_q=vm((width // n, 2 * qk + vw), BF16),
    )
    flat, layout = [], []
    for k, v in scratch.items():
        if isinstance(v, list):
            layout.append((k, len(v)))
            flat.extend(v)
        else:
            layout.append((k, 0))
            flat.append(v)

    def kernel(*refs):
        names = list(inputs) + list(outs)
        bound = list(refs[: len(names)])
        at = len(names)
        for k, count in layout:
            names.append(k)
            if count:
                bound.append(refs[at : at + count])
                at += count
            else:
                bound.append(refs[at])
                at += 1
        mega_kernel(n, names, *bound)

    res = pl.pallas_call(
        kernel,
        out_shape=[jax.ShapeDtypeStruct(*v) for v in outs.values()],
        in_specs=[pl.BlockSpec(memory_space=pl.ANY if k in hbm else pltpu.VMEM) for k in inputs],
        out_specs=[pl.BlockSpec(memory_space=pltpu.VMEM)] * len(outs),
        scratch_shapes=flat,
        compiler_params=pltpu.CompilerParams(
            collective_id=0, has_side_effects=True, vmem_limit_bytes=67043328
        ),
        name="block_step",
    )(*inputs.values())
    o = SimpleNamespace(**dict(zip(outs, res)))

    return (
        o.layer_out[None],
        o.grad_in[None],
        o.grad_attn[0],
        o.grad_q,
        o.grad_k,
        o.grad_v,
        o.out_o.astype(F32),
        o.grad_ffn[0],
        o.out_g[:ff].astype(F32).T,
        o.out_u[:ff].astype(F32).T,
        o.out_d[:ff].astype(F32),
        o.loss[0, 0],
    )


def per_device(*arrays):
    n = lax.axis_size("fsdp")
    layer_in, w_query, w_value = arrays[0], arrays[5], arrays[7]
    fits = (
        lax.axis_size("ctx") == 4
        and lax.axis_size("tp") == 2
        and layer_in.shape[0] == 1
        and w_query.shape[0] == 256
        and w_query.shape[1] == 128
        and w_value.shape[1] % 512 == 0
        and layer_in.shape[1] % 256 == 0
    )
    return mega(n, *arrays) if fits else general(*arrays)


def solution(mesh):
    placed = (
        P("fsdp", "ctx", None),
        P("fsdp", "ctx"),
        P("fsdp", "ctx"),
        P("fsdp", "ctx", None),
        P("fsdp"),
        P("fsdp", "tp"),
        P("fsdp", "tp"),
        P("fsdp", "tp"),
        P("tp", "fsdp"),
        P("fsdp"),
        P("fsdp", "tp"),
        P("fsdp", "tp"),
        P("tp", "fsdp"),
    )
    return jax.shard_map(
        per_device,
        mesh=mesh,
        in_specs=placed,
        out_specs=(
            P("fsdp", "ctx", None),
            P("fsdp", "ctx", None),
            P("fsdp"),
            P("fsdp", "tp"),
            P("fsdp", "tp"),
            P("fsdp", "tp"),
            P("tp", "fsdp"),
            P("fsdp"),
            P("fsdp", "tp"),
            P("fsdp", "tp"),
            P("tp", "fsdp"),
            P(),
        ),
        check_vma=False,
    )
```

```python
from functools import partial
from types import SimpleNamespace
import math

import jax
import jax.numpy as jnp
from jax import lax
from jax.experimental import pallas as pl
from jax.experimental.pallas import tpu as pltpu
from jax.sharding import PartitionSpec as P

FEAT = 16
HEAD_V = 64


EPSILON = 1e-05
HIGH = lax.Precision.HIGHEST
QUAD_SCALE = 1.0 / (4.0 * math.sqrt(2.0))


def entering(x, axis, join, neutral):
    place = lax.axis_index(axis)
    gathered = jax.tree.map(
        lambda a, kind: lax.all_gather(a.astype(kind), axis),
        x,
        (jnp.bfloat16, jnp.bfloat16, jnp.bfloat16),
    )
    state = jax.tree.map(lambda a, e: jnp.zeros_like(a) + jnp.asarray(e, a.dtype), x, neutral)

    def one(lap, state):
        return join(
            state,
            jax.tree.map(
                lambda a, own: lax.dynamic_index_in_dim(a, lap, 0, False).astype(own.dtype),
                gathered,
                x,
            ),
        )

    return lax.fori_loop(0, place, one, state)


def entering_2(x, axis, combine, identity):
    devices, here = (lax.axis_size(axis), lax.axis_index(axis))
    everything = jax.tree.map(
        lambda part, kind: lax.all_gather(part.astype(kind), axis),
        x,
        jax.tree.map(lambda a: jnp.bfloat16 if a.dtype == jnp.float32 else a.dtype, x),
    )
    start = jax.tree.map(
        lambda part, zero: jnp.broadcast_to(jnp.asarray(zero, part.dtype), part.shape), x, identity
    )

    def lap(k, before):
        at = devices - 1 - k
        reached = at > here
        new = combine(
            before, jax.tree.map(lambda part, own: part[at].astype(own.dtype), everything, x)
        )
        return jax.tree.map(lambda a, b: jnp.where(reached, a, b), new, before)

    return lax.fori_loop(0, devices, lap, start)


def product(left_side, right_side):
    return jnp.dot(left_side, right_side, preferred_element_type=jnp.float32)


def product_left_t(left_side, right_side):
    return lax.dot_general(
        left_side, right_side, (((0,), (0,)), ((), ())), preferred_element_type=jnp.float32
    )


def product_right_t(left_side, right_side):
    return lax.dot_general(
        left_side, right_side, (((1,), (1,)), ((), ())), preferred_element_type=jnp.float32
    )


def features(vectors):
    lead_dims = vectors.shape[:-1]
    feat_width = vectors.shape[-1]
    square = (vectors[..., :, None] * vectors[..., None, :]).reshape(
        lead_dims + (feat_width * feat_width,)
    )
    return jnp.concatenate(
        [jnp.ones(lead_dims + (1,), jnp.float32), 0.5 * vectors, QUAD_SCALE * square], axis=-1
    )


def attend(query_rows, key_rows, value_rows, prev_state, prev_norm, segment, prev_id):
    scores = jnp.einsum("slhf,smhf->shlm", query_rows, key_rows, precision=HIGH) * 0.25
    kernel = 1.0 + scores + 0.5 * scores * scores
    places = jnp.arange(segment.shape[1])
    allowed = (places[:, None] >= places[None, :])[None] & (
        segment[:, :, None] == segment[:, None, :]
    )
    kernel = jnp.where(allowed[:, None], kernel, 0.0)
    carried = (segment.astype(jnp.float32) == prev_id[:, None]).astype(jnp.float32)
    mapped = features(query_rows) * carried[:, :, None, None]
    numerator = jnp.einsum("shlm,smhv->slhv", kernel, value_rows, precision=HIGH) + jnp.einsum(
        "slht,shtv->slhv", mapped, prev_state, precision=HIGH
    )
    denominator = jnp.einsum("shlm->slh", kernel) + jnp.einsum(
        "slht,sht->slh", mapped, prev_norm, precision=HIGH
    )
    return numerator / denominator[..., None]


def summarize(key_rows, value_rows, segment):
    closing = (segment == segment[:, -1:]).astype(jnp.float32)
    mapped = features(key_rows) * closing[:, :, None, None]
    return (
        jnp.einsum("slht,slhv->shtv", mapped, value_rows, precision=HIGH),
        jnp.sum(mapped, axis=1),
    )


def rms_forward(values_in, gain_vec):
    inv_root = lax.rsqrt(jnp.mean(values_in * values_in, axis=-1, keepdims=True) + EPSILON)
    return (values_in * inv_root * gain_vec, inv_root)


def rms_backward(values_in, inv_root, gain_vec, grad_normed):
    weighted = grad_normed * gain_vec
    grad_gain = jnp.sum(grad_normed * values_in * inv_root, axis=0)
    grad_values = inv_root * weighted - values_in * inv_root**3 * jnp.mean(
        weighted * values_in, axis=-1, keepdims=True
    )
    return (grad_values, grad_gain)


def chain_combine(earlier, later):
    is_fresh = later[0] < 0
    same_doc = later[0] == earlier[0]

    def pick(early_part, late_part):
        expand = (-1,) + (1,) * (early_part.ndim - 1)
        with_early = late_part + jnp.where(same_doc.reshape(expand), early_part, 0.0)
        return jnp.where(is_fresh.reshape(expand), early_part, with_early)

    return (
        jnp.where(is_fresh, earlier[0], later[0]),
        pick(earlier[1], later[1]),
        pick(earlier[2], later[2]),
    )


def tp_forward(partial_sum):
    return lax.psum(partial_sum, "tp")


def tp_backward(partial_sum):
    return lax.psum(partial_sum.astype(jnp.bfloat16), "tp").astype(jnp.float32)


def general(
    layer_in,
    segment_ids,
    valid_mask,
    teacher,
    attn_gain,
    w_query,
    w_key,
    w_value,
    w_out,
    ffn_gain,
    w_gate,
    w_up,
    w_down,
):
    full_weights = (
        lax.all_gather(attn_gain, "fsdp", axis=0, tiled=True),
        lax.all_gather(w_query, "fsdp", axis=0, tiled=True),
        lax.all_gather(w_key, "fsdp", axis=0, tiled=True),
        lax.all_gather(w_value, "fsdp", axis=0, tiled=True),
        lax.all_gather(w_out, "fsdp", axis=1, tiled=True),
        lax.all_gather(ffn_gain, "fsdp", axis=0, tiled=True),
        lax.all_gather(w_gate, "fsdp", axis=0, tiled=True),
        lax.all_gather(w_up, "fsdp", axis=0, tiled=True),
        lax.all_gather(w_down, "fsdp", axis=1, tiled=True),
    )
    (
        gain_one,
        full_query,
        full_key,
        full_value,
        full_out,
        gain_two,
        full_gate,
        full_up,
        full_down,
    ) = full_weights
    seq_count, shard_len, model_width = layer_in.shape
    row_count = seq_count * shard_len
    heads_here = full_query.shape[1] // FEAT
    rows_in = layer_in.reshape(row_count, model_width).astype(jnp.float32)
    normed_full, root_one = rms_forward(rows_in, gain_one.astype(jnp.float32))
    normed_one = normed_full.astype(jnp.bfloat16)
    query_rows = product(normed_one, full_query).reshape(seq_count, shard_len, heads_here, FEAT)
    key_rows = product(normed_one, full_key).reshape(seq_count, shard_len, heads_here, FEAT)
    value_rows = product(normed_one, full_value).reshape(seq_count, shard_len, heads_here, HEAD_V)
    last_id = segment_ids[:, -1].astype(jnp.float32)
    first_id = segment_ids[:, 0].astype(jnp.float32)
    (out_state, out_norm), summary_pull = jax.vjp(
        partial(summarize, segment=segment_ids), key_rows, value_rows
    )
    blank_state = jnp.zeros_like(out_state)
    blank_norm = jnp.zeros_like(out_norm)
    no_doc = jnp.full_like(last_id, -1.0)
    prev_id, prev_state, prev_norm = entering(
        (last_id, out_state, out_norm), "ctx", chain_combine, (no_doc, blank_state, blank_norm)
    )
    attended, attend_pull = jax.vjp(
        partial(attend, segment=segment_ids, prev_id=prev_id),
        query_rows,
        key_rows,
        value_rows,
        prev_state,
        prev_norm,
    )
    mixed_heads = attended.reshape(row_count, heads_here * HEAD_V).astype(jnp.bfloat16)
    head_sum = product(mixed_heads, full_out)
    teacher_rows = teacher.reshape(row_count, model_width).astype(jnp.float32)
    weight_rows = valid_mask.reshape(row_count, 1).astype(jnp.float32)
    middle = rows_in + tp_forward(head_sum)
    normed_mid, root_two = rms_forward(middle, gain_two.astype(jnp.float32))
    normed_two = normed_mid.astype(jnp.bfloat16)
    gate_rows = product(normed_two, full_gate)
    up_rows = product(normed_two, full_up)
    sigmoid_gate = jax.nn.sigmoid(gate_rows)
    silu_gate = gate_rows * sigmoid_gate
    hidden = (silu_gate * up_rows).astype(jnp.bfloat16)
    down_sum = product(hidden, full_down)
    output = middle + tp_forward(down_sum)
    misfit = (output - teacher_rows) * weight_rows
    layer_rows = output.astype(jnp.bfloat16)
    grad_rows = misfit.astype(jnp.bfloat16)
    sum_squares = jnp.sum(misfit * misfit)
    sum_valid = jnp.sum(weight_rows)
    grad_down = product_left_t(hidden, grad_rows)
    grad_hidden = product_right_t(grad_rows, full_down)
    grad_gate_rows = (
        grad_hidden * up_rows * sigmoid_gate * (1.0 + gate_rows * (1.0 - sigmoid_gate))
    ).astype(jnp.bfloat16)
    grad_up_rows = (grad_hidden * silu_gate).astype(jnp.bfloat16)
    grad_gate = product_left_t(normed_two, grad_gate_rows)
    grad_up = product_left_t(normed_two, grad_up_rows)
    normed_two_terms = product_right_t(grad_gate_rows, full_gate) + product_right_t(
        grad_up_rows, full_up
    )
    grad_normed_two = tp_backward(normed_two_terms)
    grad_mid_norm, grad_ffn_gain = rms_backward(
        middle, root_two, gain_two.astype(jnp.float32), grad_normed_two
    )
    grad_middle = misfit + grad_mid_norm
    grad_branch = grad_middle.astype(jnp.bfloat16)
    grad_out = product_left_t(mixed_heads, grad_branch)
    grad_mixed = product_right_t(grad_branch, full_out).reshape(
        seq_count, shard_len, heads_here, HEAD_V
    )
    grad_q_near, grad_k_near, grad_v_near, grad_prev_state, grad_prev_norm = attend_pull(grad_mixed)
    next_id, later_state, later_norm = entering_2(
        (first_id, grad_prev_state, grad_prev_norm),
        "ctx",
        chain_combine,
        (no_doc, blank_state, blank_norm),
    )
    continues = (next_id == last_id).astype(jnp.float32)
    grad_k_far, grad_v_far = summary_pull(
        (later_state * continues[:, None, None, None], later_norm * continues[:, None, None])
    )
    grad_query_rows = grad_q_near.reshape(row_count, heads_here * FEAT).astype(jnp.bfloat16)
    grad_key_rows = (
        (grad_k_near + grad_k_far).reshape(row_count, heads_here * FEAT).astype(jnp.bfloat16)
    )
    grad_value_rows = (
        (grad_v_near + grad_v_far).reshape(row_count, heads_here * HEAD_V).astype(jnp.bfloat16)
    )
    grad_query = product_left_t(normed_one, grad_query_rows)
    grad_key = product_left_t(normed_one, grad_key_rows)
    grad_value = product_left_t(normed_one, grad_value_rows)
    normed_one_terms = (
        product_right_t(grad_query_rows, full_query)
        + product_right_t(grad_key_rows, full_key)
        + product_right_t(grad_value_rows, full_value)
    )
    grad_normed_one = tp_backward(normed_one_terms)
    grad_rows_in, grad_attn_gain = rms_backward(
        rows_in, root_one, gain_one.astype(jnp.float32), grad_normed_one
    )
    grad_in_rows = (grad_middle + grad_rows_in).astype(jnp.bfloat16)
    total_sq, total_valid = lax.psum((sum_squares, sum_valid), ("fsdp", "ctx"))
    loss_value = total_sq / (total_valid * model_width)
    grad_in = grad_in_rows.reshape(seq_count, shard_len, model_width)
    layer_out = layer_rows.reshape(seq_count, shard_len, model_width)
    owned = (
        lax.psum_scatter(
            grad_attn_gain.astype(jnp.bfloat16), "fsdp", scatter_dimension=0, tiled=True
        ).astype(jnp.float32),
        lax.psum_scatter(
            grad_query.astype(jnp.bfloat16), "fsdp", scatter_dimension=0, tiled=True
        ).astype(jnp.float32),
        lax.psum_scatter(
            grad_key.astype(jnp.bfloat16), "fsdp", scatter_dimension=0, tiled=True
        ).astype(jnp.float32),
        lax.psum_scatter(
            grad_value.astype(jnp.bfloat16), "fsdp", scatter_dimension=0, tiled=True
        ).astype(jnp.float32),
        lax.psum_scatter(
            grad_out.astype(jnp.bfloat16), "fsdp", scatter_dimension=1, tiled=True
        ).astype(jnp.float32),
        lax.psum_scatter(
            grad_ffn_gain.astype(jnp.bfloat16), "fsdp", scatter_dimension=0, tiled=True
        ).astype(jnp.float32),
        lax.psum_scatter(
            grad_gate.astype(jnp.bfloat16), "fsdp", scatter_dimension=0, tiled=True
        ).astype(jnp.float32),
        lax.psum_scatter(
            grad_up.astype(jnp.bfloat16), "fsdp", scatter_dimension=0, tiled=True
        ).astype(jnp.float32),
        lax.psum_scatter(
            grad_down.astype(jnp.bfloat16), "fsdp", scatter_dimension=1, tiled=True
        ).astype(jnp.float32),
    )
    shares = (
        lax.psum(owned[0].astype(jnp.bfloat16), "ctx").astype(jnp.float32),
        lax.psum(owned[1].astype(jnp.bfloat16), "ctx").astype(jnp.float32),
        lax.psum(owned[2].astype(jnp.bfloat16), "ctx").astype(jnp.float32),
        lax.psum(owned[3].astype(jnp.bfloat16), "ctx").astype(jnp.float32),
        lax.psum(owned[4].astype(jnp.bfloat16), "ctx").astype(jnp.float32),
        lax.psum(owned[5].astype(jnp.bfloat16), "ctx").astype(jnp.float32),
        lax.psum(owned[6].astype(jnp.bfloat16), "ctx").astype(jnp.float32),
        lax.psum(owned[7].astype(jnp.bfloat16), "ctx").astype(jnp.float32),
        lax.psum(owned[8].astype(jnp.bfloat16), "ctx").astype(jnp.float32),
    )
    return (
        layer_out,
        grad_in,
        shares[0],
        shares[1],
        shares[2],
        shares[3],
        shares[4],
        shares[5],
        shares[6],
        shares[7],
        shares[8],
        loss_value,
    )


MESH = pl.DeviceIdType.MESH
F32 = jnp.float32
BF16 = jnp.bfloat16


def up_to(size, step):
    return -(-size // step) * step


def mm(a, b):
    return jnp.dot(a, b, preferred_element_type=F32)


def mm_nt(a, b):
    return lax.dot_general(a, b, (((1,), (1,)), ((), ())), preferred_element_type=F32)


def mm_tn(a, b):
    return lax.dot_general(a, b, (((0,), (0,)), ((), ())), preferred_element_type=F32)


def at128(offset):
    return pl.multiple_of(offset, 128)


class Place:
    def __init__(self, n):
        self.n = n
        self.z = lax.axis_index("fsdp")
        self.b = lax.axis_index("ctx")
        self.t = lax.axis_index("tp")
        self.x = self.b // 2
        self.c = self.b % 2
        self.ic = self.x * 2 + (1 - self.c)
        self.xp = (1 - self.x) * 2 + self.c
        self.dg = (1 - self.x) * 2 + (1 - self.c)


def remote(src, dst, send, recv, **where):
    return pltpu.make_async_remote_copy(
        src_ref=src, dst_ref=dst, send_sem=send, recv_sem=recv, device_id=where, device_id_type=MESH
    )


def entry_barrier(p):
    sem = pltpu.get_barrier_semaphore()
    for s in range(p.n):

        @pl.when(p.z != s)
        def _():
            pl.semaphore_signal(sem, inc=1, device_id={"fsdp": s}, device_id_type=MESH)

    for peer in (p.ic, p.xp, p.dg):
        pl.semaphore_signal(sem, inc=1, device_id={"ctx": peer}, device_id_type=MESH)
    pl.semaphore_signal(sem, inc=1, device_id={"tp": 1 - p.t}, device_id_type=MESH)
    pl.semaphore_wait(sem, p.n - 1 + 4)


class Gather:
    def __init__(self, p, pieces, sems):
        self.p = p
        self.pieces = pieces
        (self.zr, self.xr, self.i1r, self.i2r, self.zsl, self.zsr, self.xs, self.i1s, self.i2s) = sems

    def quarter(self, g, s, x, c):
        ref, kind, lo, size = self.pieces[g]
        n = self.p.n
        if kind == "row":
            return ref.at[pl.ds(pl.multiple_of((c * n + s) * 128 + x * 64 + lo[0], 16), size), 0 : lo[1]]
        half = lo[1]
        return ref.at[
            pl.ds(pl.multiple_of(x * half + lo[0], 16), size), pl.ds(at128((c * n + s) * 128), 128)
        ]

    def copy(self, g, s, x, c, send, recv, **where):
        ref = self.quarter(g, s, x, c)
        return remote(ref, ref, send.at[g, s], recv.at[g, s], **where)

    def left(self, g, s):
        return self.copy(g, s, self.p.x, self.p.c, self.zsl, self.zr, fsdp=self.p.z - 1)

    def right(self, g, s):
        return self.copy(g, s, self.p.x, self.p.c, self.zsr, self.zr, fsdp=self.p.z + 1)

    def chip(self, g, s, x, c, second):
        if second:
            return self.copy(g, s, x, c, self.i2s, self.i2r, ctx=self.p.ic)
        return self.copy(g, s, x, c, self.i1s, self.i1r, ctx=self.p.ic)

    def cross(self, g, s, x, c):
        return self.copy(g, s, x, c, self.xs, self.xr, ctx=self.p.xp)

    def own(self, g):
        p = self.p

        @pl.when(p.z > 0)
        def _():
            self.left(g, p.z).start()

        @pl.when(p.z < p.n - 1)
        def _():
            self.right(g, p.z).start()

    def hop(self, g, h):
        p = self.p
        for d in (1, -1):
            s = p.z + d * h
            there = (s < p.n) if d == 1 else (s >= 0)

            @pl.when(there)
            def _():
                self.copy(g, s, p.x, p.c, self.zsl, self.zr, fsdp=p.z).wait_recv()
                if d == 1:

                    @pl.when(p.z > 0)
                    def _():
                        self.left(g, s).start()

                else:

                    @pl.when(p.z < p.n - 1)
                    def _():
                        self.right(g, s).start()

                self.cross(g, s, p.x, p.c).start()
                self.chip(g, s, p.x, p.c, False).start()

    def hop_cross(self, g, h):
        p = self.p
        for d in (1, -1):
            s = p.z + d * h
            there = (s < p.n) if d == 1 else (s >= 0)

            @pl.when(there)
            def _():
                self.cross(g, s, 1 - p.x, p.c).wait_recv()
                self.chip(g, s, 1 - p.x, p.c, True).start()

    def whole(self, g, s):
        p = self.p
        self.chip(g, s, p.x, 1 - p.c, False).wait_recv()
        self.chip(g, s, 1 - p.x, 1 - p.c, True).wait_recv()

    def finish(self, g):
        p = self.p

        @pl.loop(0, p.n)
        def _(s):
            @pl.when(s != p.z)
            def _():
                self.whole(g, s)

    def drain(self):
        p = self.p
        for g in range(len(self.pieces)):

            @pl.loop(0, p.n)
            def _(s):
                @pl.when((s >= p.z) & (p.z > 0))
                def _():
                    self.left(g, s).wait_send()

                @pl.when((s <= p.z) & (p.z < p.n - 1))
                def _():
                    self.right(g, s).wait_send()

                @pl.when(s != p.z)
                def _():
                    self.cross(g, s, p.x, p.c).wait_send()
                    self.chip(g, s, p.x, p.c, False).wait_send()
                    self.chip(g, s, 1 - p.x, p.c, True).wait_send()


class Reduce:
    def __init__(self, p, parts, seen, done, other, sems):
        self.p = p
        self.parts = parts
        self.seen = seen
        self.done = done
        self.other = other
        (self.ss, self.rs, self.fs, self.fr) = sems

    def move(self, g, s, slot, to):
        return remote(
            self.parts[g].at[s], self.seen[g].at[slot], self.ss.at[g, s], self.rs.at[g, slot], fsdp=to
        )

    def arrived(self, g, slot):
        self.move(g, 0, slot, self.p.z).wait_recv()

    def by_rows(self, g, body):
        @pl.loop(0, self.parts[g].shape[1] // 128)
        def _(i):
            body(pl.ds(at128(i * 128), 128))

    def add(self, g, s, slot):
        def body(at):
            total = self.parts[g][s, at, :].astype(F32) + self.seen[g][slot, at, :].astype(F32)
            self.parts[g][s, at, :] = total.astype(BF16)

        self.by_rows(g, body)

    def stage(self, g, k):
        p = self.p
        n = p.n

        @pl.when(p.z == k)
        def _():
            for s in range(n - 1, k, -1):
                if k > 0:
                    self.arrived(g, s)
                    self.add(g, s, s)
                self.move(g, s, s, k + 1).start()

        @pl.when(p.z == n - 1 - k)
        def _():
            z = n - 1 - k
            for s in range(0, z):
                if k > 0:
                    self.arrived(g, s)
                    self.add(g, s, s)
                self.move(g, s, n if s == z - 1 else s, z - 1).start()

    def last(self, g):
        p = self.p
        n = p.n

        @pl.when(p.z > 0)
        def _():
            self.arrived(g, p.z)
            self.add(g, p.z, p.z)

        @pl.when(p.z < n - 1)
        def _():
            self.arrived(g, n)
            self.add(g, p.z, n)

        if self.other[g] is not None:
            self.across(g).start()
            return
        self.block(g, p.x, p.c)[...] = self.mine(g)[...]
        self.spread(g, p.b, 0, p.ic, self.mine(g)).start()
        self.spread(g, p.b, 1, p.xp, self.mine(g)).start()

    def mine(self, g):
        p = self.p
        if self.done[g].shape[1] != 256:
            return self.parts[g].at[p.z]
        half = self.done[g].shape[0] // 2
        skip = self.parts[g].shape[1] - half
        return self.parts[g].at[p.z, pl.ds(pl.multiple_of(p.x * skip, 16), half), :]

    def block(self, g, x, c):
        if self.done[g].shape[1] != 256:
            w = self.done[g].shape[1] // 2
            return self.done[g].at[pl.ds(at128(c * 128), 128), pl.ds(at128(x * w), w)]
        half = self.done[g].shape[0] // 2
        return self.done[g].at[pl.ds(pl.multiple_of(x * half, 16), half), pl.ds(at128(c * 128), 128)]

    def spread(self, g, slot, which, to, src=None):
        dst = self.block(g, slot // 2, slot % 2)
        return remote(dst if src is None else src, dst, self.fs.at[g, which], self.fr.at[g, slot], ctx=to)

    def side(self, g, c):
        return self.done[g].at[:, pl.ds(at128(c * 128), 128)]

    def across(self, g):
        p = self.p
        return remote(self.parts[g].at[p.z], self.other[g], self.fs.at[g, 0], self.fr.at[g, 0], ctx=p.xp)

    def beside(self, g, c):
        ref = self.side(g, c)
        return remote(ref, ref, self.fs.at[g, 1], self.fr.at[g, 1], ctx=self.p.ic)

    def relay(self, g):
        p = self.p
        if self.other[g] is not None:
            self.across(g).wait_recv()

            side = self.side(g, p.c)

            def body(at):
                total = self.parts[g][p.z, at, :].astype(F32) + self.other[g][at, :].astype(F32)
                side[at, :] = total.astype(BF16)

            self.by_rows(g, body)
            self.beside(g, p.c).start()
            return
        self.spread(g, p.xp, 1, p.xp).wait_recv()
        self.spread(g, p.xp, 2, p.ic).start()

    def finish(self, g):
        p = self.p
        if self.other[g] is not None:
            self.beside(g, 1 - p.c).wait_recv()
            self.beside(g, p.c).wait_send()
            self.across(g).wait_send()
        else:
            self.spread(g, p.ic, 0, p.ic).wait_recv()
            self.spread(g, p.dg, 2, p.ic).wait_recv()
            self.spread(g, p.b, 0, p.ic, self.mine(g)).wait_send()
            self.spread(g, p.b, 1, p.xp, self.mine(g)).wait_send()
            self.spread(g, p.xp, 2, p.ic).wait_send()

        @pl.loop(0, p.n)
        def _(s):
            @pl.when(s != p.z)
            def _():
                self.move(g, s, 0, p.z).wait_send()


class Columns:
    def __init__(self, p, k, src, dst, sems):
        self.p = p
        self.k = k
        self.src = src
        self.dst = dst
        self.send, self.recv = sems

    def slot(self, b):
        rows = self.src.shape[0]
        return self.dst.at[pl.ds(pl.multiple_of(b * rows, rows), rows), :]

    def copy(self, peer, which):
        p = self.p
        w = self.dst.shape[1]
        part = self.src.at[:, pl.ds(at128((peer % 2) * w), w)]
        return remote(part, self.slot(p.b), self.send.at[self.k, which], self.recv.at[self.k, p.b], ctx=peer)

    def start(self):
        p = self.p
        w = self.dst.shape[1]
        for which, peer in enumerate((p.xp, p.dg, p.ic)):
            self.copy(peer, which).start()
        self.slot(p.b)[...] = self.src[:, pl.ds(at128(p.c * w), w)]

    def wait(self):
        p = self.p
        for peer in (p.ic, p.xp, p.dg):
            remote(self.slot(peer), self.slot(peer), self.send.at[self.k, 0], self.recv.at[self.k, peer], ctx=peer).wait_recv()

    def drain(self):
        p = self.p
        for which, peer in enumerate((p.xp, p.dg, p.ic)):
            self.copy(peer, which).wait_send()


class Pair:
    def __init__(self, p, k, src, dst, sems):
        self.p = p
        self.k = k
        self.src = src
        self.dst = dst
        self.send, self.recv = sems

    def slot(self, c):
        rows = self.src.shape[0]
        return self.dst.at[pl.ds(pl.multiple_of(c * rows, rows), rows), :]

    def part(self, c):
        w = self.dst.shape[1]
        if w == self.src.shape[1]:
            return self.src
        return self.src.at[:, pl.ds(at128(c * w), w)]

    def copy(self):
        p = self.p
        return remote(self.part(1 - p.c), self.slot(p.c), self.send.at[self.k], self.recv.at[self.k], ctx=p.ic)

    def start(self):
        c = self.p.c
        self.copy().start()
        self.slot(c)[...] = self.part(c)[...]

    def wait(self):
        p = self.p
        remote(self.part(1 - p.c), self.slot(1 - p.c), self.send.at[self.k], self.recv.at[self.k], ctx=p.ic).wait_recv()

    def drain(self):
        self.copy().wait_send()


class Halves:
    def __init__(self, p, k, src, dst, step, sems):
        self.p = p
        self.k = k
        self.src = src
        self.dst = dst
        self.step = step
        self.send, self.recv = sems

    def slot(self, b):
        rows = self.src.shape[0]
        return self.dst.at[pl.ds(pl.multiple_of(b * rows, rows), rows), :]

    def part(self, x):
        return self.src.at[:, pl.ds(at128(x * self.step), self.dst.shape[1])]

    def to(self, src, slot, which, peer):
        return remote(src, self.slot(slot), self.send.at[self.k, which], self.recv.at[self.k, slot], ctx=peer)

    def start(self):
        p = self.p
        self.to(self.part(1 - p.x), p.b, 0, p.xp).start()
        self.to(self.part(p.x), p.b, 1, p.ic).start()
        self.slot(p.b)[...] = self.src[:, pl.ds(at128(p.x * self.step), self.dst.shape[1])]

    def relay(self):
        p = self.p
        self.to(self.slot(p.xp), p.xp, 2, p.ic).wait_recv()
        self.to(self.slot(p.xp), p.xp, 2, p.ic).start()

    def wait(self):
        p = self.p
        self.to(self.slot(p.ic), p.ic, 1, p.ic).wait_recv()
        self.to(self.slot(p.dg), p.dg, 1, p.ic).wait_recv()

    def drain(self):
        p = self.p
        self.to(self.part(1 - p.x), p.b, 0, p.xp).wait_send()
        self.to(self.part(p.x), p.b, 1, p.ic).wait_send()
        self.to(self.slot(p.xp), p.xp, 2, p.ic).wait_send()


def mega_kernel(n, names, *refs):
    r = SimpleNamespace(**dict(zip(names, refs)))
    p = Place(n)
    z, b, x, c = p.z, p.b, p.x, p.c
    rows_here = r.x.shape[0]
    width = r.x.shape[1]
    half_d = width // 2
    heads = r.wv.shape[1] // HEAD_V
    qk = r.wq.shape[1]
    vw = r.wv.shape[1]
    ff = r.wd.shape[0]
    ffp = r.hid.shape[1]
    order = [s * 256 + cc * 128 for cc in range(2) for s in range(n)]
    blocks = width // 256
    D = r.lsem

    fqkv, fo, fg, fu, fd = r.fqkv, r.fo, r.fg, r.fu, r.fd
    local = []

    def bring(src, dst):
        copy = pltpu.make_async_copy(src, dst, D.at[len(local)])
        copy.start()
        local.append(copy)
        return copy

    get_x = bring(r.x, r.xv)
    need = {}
    for cc in range(2):
        rows = pl.ds(at128((cc * n + z) * 128), 128)
        src = slice(cc * 128, cc * 128 + 128)
        need.setdefault("qkv", []).extend(
            (
                bring(r.wq.at[src, :], fqkv.at[rows, 0:qk]),
                bring(r.wk.at[src, :], fqkv.at[rows, qk : 2 * qk]),
                bring(r.wv.at[src, :], fqkv.at[rows, 2 * qk : 2 * qk + vw]),
            )
        )
    for cc in range(2):
        cols = pl.ds(at128((cc * n + z) * 128), 128)
        need.setdefault("o", []).append(bring(r.wo.at[:, cc * 128 : cc * 128 + 128], fo.at[:, cols]))
    for key, src, dst in (("g", r.wg, fg), ("u", r.wu, fu), ("d", r.wd, fd)):
        for cc in range(2):
            cols = pl.ds(at128((cc * n + z) * 128), 128)
            need.setdefault(key, []).append(bring(src.at[:, cc * 128 : cc * 128 + 128], dst.at[0:ff, cols]))
    get_teacher = bring(r.teacher, r.tv)

    pieces, first = [], []

    def split(total, parts):
        unit = total // 16
        edge = [(unit * i // parts) * 16 for i in range(parts + 1)]
        return [(edge[i], edge[i + 1] - edge[i]) for i in range(parts)]

    for key, ref, kind, total, parts in (
        ("qkv", fqkv, "row", 64, 1),
        ("o", fo, "col", vw // 2, 1),
        ("g", fg, "col", ff // 2, 2),
        ("u", fu, "col", ff // 2, 2),
        ("d", fd, "col", ff // 2, 2),
    ):
        for i, (lo, size) in enumerate(split(total, parts)):
            pieces.append((ref, kind, (lo, ref.shape[1]) if kind == "row" else (lo, total), size))
            first.append(need[key] if i == 0 else [])
    gather = Gather(p, pieces, r.gs)
    ng = len(pieces)

    def own(g):
        for copy in first[g]:
            copy.wait()
        gather.own(g)

    entry_barrier(p)
    own(0)
    own(1)

    r.gains[...] = jnp.concatenate(
        [r.attn_gain[...].astype(F32).reshape(1, -1), r.ffn_gain[...].astype(F32).reshape(1, -1)]
        + [jnp.zeros((6, width // n), F32)],
        axis=0,
    )
    segment = r.segment[...].astype(F32)
    r.segrow[...] = jnp.broadcast_to(segment, (8, rows_here))
    r.segcol[...] = jnp.transpose(jnp.broadcast_to(segment, (128, rows_here)))
    r.valid[...] = jnp.transpose(jnp.broadcast_to(r.real[...].astype(F32), (128, rows_here)))
    gsend, grecv, gath = r.gnsem[0], r.gnsem[1], r.gath
    for s in range(n):

        @pl.when(z != s)
        def _():
            remote(r.gains, gath.at[z], gsend.at[s], grecv.at[z], fsdp=s).start()

    gath[z] = r.gains[...]
    segs, segr = r.segsem[0], r.segsem[1]
    for i, peer in enumerate((p.ic, p.xp, p.dg)):
        remote(r.segrow, r.segall.at[b], segs.at[i], segr.at[b], ctx=peer).start()
    r.segall[b] = r.segrow[...]

    pad = ffp - ff
    if pad:
        for ref in (fg, fu, fd):
            ref[ff:ffp, :] = jnp.zeros((pad, width), BF16)

    for s in range(n):

        @pl.when(z != s)
        def _():
            remote(r.gains, gath.at[s], gsend.at[s], grecv.at[s], fsdp=s).wait_recv()

    for row in range(2):
        r.gain[row : row + 1, :] = jnp.concatenate(
            [gath[s, row : row + 1, cc * 128 : cc * 128 + 128] for cc in range(2) for s in range(n)], axis=1
        )

    events = [(g - 1.5, "own", g, 0) for g in range(2, ng)]
    for g in range(ng):
        for h in range(1, n):
            events.append((g + 0.7 * h, "hop", g, h))
            events.append((g + 0.7 * h + 0.8, "cross", g, h))
    events.sort()
    passed = [0]

    def advance(until):
        while passed[0] < len(events) and events[passed[0]][0] <= until:
            _, kind, g, h = events[passed[0]]
            if kind == "own":
                own(g)
            elif kind == "hop":
                gather.hop(g, h)
            else:
                gather.hop_cross(g, h)
            passed[0] += 1

    def ready(g_from, g_to):
        advance(max(e[0] for e in events if e[1] == "cross" and e[2] < g_to))
        for g in range(g_from, g_to):
            gather.finish(g)

    send_n1 = Pair(p, 0, r.n1, r.n1c, r.psem)
    send_da = Pair(p, 1, r.da, r.dac, r.psem)
    send_dy = Pair(p, 2, r.dy, r.dyc, r.psem)
    send_hid = Pair(p, 3, r.hid, r.hidx, r.psem)
    send_mix = Pair(p, 4, r.mix, r.mixx, r.psem)
    send_dqkv = Pair(p, 5, r.dqkv, r.dqkvx, r.psem)
    send_n2 = Columns(p, 0, r.n2, r.n2c, r.csem)
    fh = r.dgx.shape[1]
    send_dg = Halves(p, 0, r.dg, r.dgx, ffp - fh, r.hsem)
    send_du = Halves(p, 1, r.du, r.dux, ffp - fh, r.hsem)
    ysend, yrecv = r.ysend, r.yrecv

    def y_copy(i, ch):
        return remote(ysend.at[i, ch], yrecv.at[i, ch], r.ysem[0].at[i, ch], r.ysem[1].at[i, ch], tp=1 - p.t)

    def y_put(i, ch, value):
        ysend[i, ch] = value.astype(BF16)
        y_copy(i, ch).start()

    def y_wait(i, between=()):
        for ch in range(blocks):
            y_copy(i, ch).wait_recv()
            if ch < len(between):
                between[ch]()

    def y_rows(i, rs):
        if i == 1:
            parts = [(s, slice(cc * 128, cc * 128 + 128)) for cc in range(2) for s in range(n)]
            return jnp.concatenate(
                [ysend[1, s, rs, at].astype(F32) + yrecv[1, s, rs, at].astype(F32) for s, at in parts], axis=1
            )
        return jnp.concatenate(
            [ysend[i, ch, rs, :].astype(F32) + yrecv[i, ch, rs, :].astype(F32) for ch in range(blocks)], axis=1
        )

    step_rows = 32
    row_steps = rows_here // step_rows

    def per_rows(body):
        @pl.loop(0, row_steps)
        def _(i):
            body(pl.ds(pl.multiple_of(i * step_rows, step_rows), step_rows))

    def x_rows(rs):
        return jnp.concatenate([r.xv[rs, o : o + 128] for o in order], axis=1).astype(F32)

    def rsq(v):
        return lax.rsqrt(jnp.mean(v * v, axis=1, keepdims=True) + EPSILON)

    get_x.wait()

    def norm_one(rs):
        v = x_rows(rs)
        r.n1[rs, :] = (v * rsq(v) * r.gain[0:1, :]).astype(BF16)

    per_rows(norm_one)
    ready(0, 1)
    kv = r.kv
    first_chunk = mm(r.n1[...], fqkv[:, 0 : 2 * qk])
    r.q[...] = first_chunk[:, 0:qk].astype(BF16)
    kv[b, :, 0:qk] = first_chunk[:, qk : 2 * qk].astype(BF16)
    for ch in range(vw // 256):
        lo = ch * 256
        kv[b, :, qk + lo : qk + lo + 256] = mm(r.n1[...], fqkv[:, 2 * qk + lo : 2 * qk + lo + 256]).astype(BF16)

    kvs, kvr = r.kvsem

    def kv_copy(slot, which, peer):
        return remote(kv.at[slot], kv.at[slot], kvs.at[which], kvr.at[slot], ctx=peer)

    @pl.when(x == 0)
    def _():
        kv_copy(b, 0, p.xp).start()

    @pl.when(c == 0)
    def _():
        kv_copy(b, 1, p.ic).start()

    for i, peer in enumerate((p.ic, p.xp, p.dg)):
        remote(r.segrow, r.segall.at[peer], segs.at[i], segr.at[peer], ctx=peer).wait_recv()
    mask, num, den = r.mask, r.num, r.den
    num[...] = jnp.zeros_like(num)
    den[...] = jnp.zeros_like(den)
    lane = lax.broadcasted_iota(jnp.int32, (1, 128), 1)

    def q_of(h):
        keep = (lane // FEAT) == h
        return jnp.where(keep, r.q[...], jnp.zeros((), BF16))

    def attend_block(j):
        same = r.segcol[:, 0:1] == r.segall[j, 0:1, :]
        ri = lax.broadcasted_iota(jnp.int32, (rows_here, rows_here), 0)
        ci = lax.broadcasted_iota(jnp.int32, (rows_here, rows_here), 1)
        reach = ri + jnp.where(j == b, 0, rows_here) >= ci
        mask[j] = jnp.where(same & reach, 1.0, 0.0)

        @pl.loop(0, heads // 2)
        def _(pair):
            at = pl.ds(at128(pair * 128), 128)
            vpair = kv[j, :, pl.ds(at128(qk + pair * 128), 128)]
            sums = []
            for e in range(2):
                s = mm_nt(q_of(pair * 2 + e), kv[j, :, 0:qk]) * 0.25
                w = (1.0 + s + 0.5 * s * s) * mask[j]
                sums.append((mm(w.astype(BF16), vpair), jnp.sum(w, axis=1, keepdims=True)))
            low_half = lane < HEAD_V
            num[:, at] += jnp.where(low_half, sums[0][0], sums[1][0])
            den[:, at] += jnp.where(low_half, sums[0][1], sums[1][1])

    attend_block(b)
    advance(3.3)

    @pl.when(x == 1)
    def _():
        kv_copy(c, 2, p.ic).wait_recv()
        kv_copy(c, 2, p.ic).start()

    @pl.when(c == 1)
    def _():
        kv_copy(p.ic, 1, p.ic).wait_recv()

    @pl.when(x == 1)
    def _():
        kv_copy(1 - c, 2, p.ic).wait_recv()

    @pl.loop(1, b + 1)
    def _(m):
        attend_block(b - m)

    inv = 1.0 / den[...]
    den[...] = inv
    num[...] = num[...] * inv
    r.mix[...] = num[...].astype(BF16)

    ready(1, 2)
    for ch in range(blocks):
        y_put(0, ch, mm(r.mix[...], fo[:, ch * 256 : ch * 256 + 256]))
    send_mix.start()
    send_n1.start()
    advance(4.5)
    y_wait(0, [lambda u=u: advance(u) for u in (5.0, 5.7, 6.3)])

    def norm_two(rs):
        v = x_rows(rs) + y_rows(0, rs)
        r.mid[rs, :] = v
        r.n2[rs, :] = (v * rsq(v) * r.gain[1:2, :]).astype(BF16)

    per_rows(norm_two)

    red = Reduce(
        p,
        [r.part[i] for i in range(5)],
        [r.seen[i] for i in range(5)],
        [r.out_d, r.out_g, r.out_u, r.out_o, r.out_q],
        [r.other, None, None, None, None],
        r.rsem,
    )
    turned = r.turned

    def turn(src):
        w = src.shape[1]

        @pl.loop(0, src.shape[0] // rows_here)
        def _(i):
            at = pl.ds(pl.multiple_of(i * rows_here, rows_here), rows_here)
            turned[0:w, at] = jnp.transpose(src[at, :])

    def grad_cols(g, rhs):
        rows = r.part[g].shape[1]

        @pl.loop(0, -(-rows // 256))
        def _(i):
            at = pl.ds(at128(jnp.minimum(i * 256, rows - 256)), 256)
            res = mm(turned[at, 0 : rhs.shape[0]], rhs[...]).astype(BF16)
            for s in range(n):
                r.part[g][s, at, :] = res[:, s * 128 : s * 128 + 128]

    fchunks = -(-ffp // 256)

    def per_ff(body):
        @pl.loop(0, fchunks)
        def _(i):
            body(at128(jnp.minimum(i * 256, ffp - 256)))

    ready(2, 6)

    def wide(ref, off):
        return ref[pl.ds(off, 256), :]

    def forward_ff(off):
        g = mm_nt(r.n2[...], wide(fg, off))
        u = mm_nt(r.n2[...], wide(fu, off))
        r.g[:, pl.ds(off, 256)] = g
        r.u[:, pl.ds(off, 256)] = u
        sig = 1.0 / (1.0 + jnp.exp(-g))
        r.hid[:, pl.ds(off, 256)] = (g * sig * u).astype(BF16)

    per_ff(forward_ff)
    send_hid.start()

    def down_block(s):
        for cc in range(2):
            cols = pl.ds(at128((cc * n + s) * 128), 128)
            ysend[1, s, :, cc * 128 : cc * 128 + 128] = mm(r.hid[...], fd[:, cols]).astype(BF16)
        y_copy(1, s).start()

    advance(ng - 1)
    down_block(z)
    for h in range(1, n):
        advance(ng - 1 + 0.7 * h + 0.81)
        for s, there in ((z + h, z + h < n), (z - h, z - h >= 0)):

            @pl.when(there)
            def _():
                for g in range(6, ng):
                    gather.whole(g, s)
                down_block(s)

    advance(2 * ng)
    send_n2.start()
    get_teacher.wait()
    small = r.small
    small[...] = jnp.zeros_like(small)
    send_hid.wait()
    turn(r.hidx)
    y_wait(1)

    def finish_forward(rs):
        y = r.mid[rs, :] + y_rows(1, rs)
        t = jnp.concatenate([r.tv[rs, o : o + 128] for o in order], axis=1).astype(F32)
        m = (y - t) * r.valid[rs, 0:1]
        r.mis[rs, :] = m
        r.dy[rs, :] = m.astype(BF16)
        yb = y.astype(BF16)
        for i, o in enumerate(order):
            r.layer_out[rs, o : o + 128] = yb[:, i * 128 : i * 128 + 128]
        small[2:3, :] += jnp.sum(m * m, axis=0, keepdims=True)
        small[3:4, :] += jnp.broadcast_to(jnp.sum(r.valid[rs, :], axis=0, keepdims=True)[:, 0:1], (1, width))

    per_rows(finish_forward)
    send_dy.start()

    def backward_ff(off):
        dh = mm_nt(r.dy[...], fd[pl.ds(off, 256), :])
        g = r.g[:, pl.ds(off, 256)]
        u = r.u[:, pl.ds(off, 256)]
        sig = 1.0 / (1.0 + jnp.exp(-g))
        r.dg[:, pl.ds(off, 256)] = (dh * u * sig * (1.0 + g * (1.0 - sig))).astype(BF16)
        r.du[:, pl.ds(off, 256)] = (dh * g * sig).astype(BF16)

    per_ff(backward_ff)
    send_dg.start()
    send_du.start()
    send_dy.wait()
    grad_cols(0, r.dyc)
    red.stage(0, 0)
    for ch in range(blocks):
        cols = slice(ch * 256, ch * 256 + 256)
        y_put(2, ch, mm(r.dg[...], fg[:, cols]) + mm(r.du[...], fu[:, cols]))

    send_dg.relay()

    y_wait(2)

    def norm_back(i, row, v, base, rs):
        dn = y_rows(i, rs)
        inv_root = rsq(v)
        w = dn * r.gain[row : row + 1, :]
        small[row : row + 1, :] += jnp.sum(dn * v * inv_root, axis=0, keepdims=True)
        m = jnp.mean(w * v, axis=1, keepdims=True)
        return base + inv_root * w - v * (inv_root * inv_root * inv_root * m)

    def middle_back(rs):
        d = norm_back(2, 1, r.mid[rs, :], r.mis[rs, :], rs)
        r.mis[rs, :] = d
        r.da[rs, :] = d.astype(BF16)

    per_rows(middle_back)
    send_da.start()
    send_n2.wait()
    send_dg.wait()
    turn(r.dgx)
    grad_cols(1, r.n2c)
    red.stage(1, 0)

    dnum, dden = r.dnum, r.dden
    for ch in range(vw // 256):
        at = slice(ch * 256, ch * 256 + 256)
        d = mm_nt(r.da[...], fo[at, :]) * den[:, at]
        dnum[:, at] = d.astype(BF16)
        dden[:, at] = d * num[:, at]
    send_du.relay()
    send_da.wait()
    send_mix.wait()
    turn(r.mixx)

    def out_half(dst, xx):
        rows = vw // 2
        res = mm(turned[pl.ds(pl.multiple_of(xx * rows, 128), rows), 0 : 2 * rows_here], r.dac[...]).astype(BF16)
        for s in range(n):
            dst[s] = res[:, s * 128 : s * 128 + 128]

    def halve(i, g, make):
        give, got = r.give[i], r.got[i]
        make(give, 1 - x)
        half_copy(i).start()
        make(r.part[g], x)

    def half_copy(i):
        return remote(r.give[i], r.got[i], r.presem[0].at[i], r.presem[1].at[i], ctx=p.xp)

    def joined(i, g):
        half_copy(i).wait_recv()
        for s in range(n):
            r.part[g][s] = (r.part[g][s].astype(F32) + r.got[i][s].astype(F32)).astype(BF16)

    halve(0, 3, out_half)
    send_du.wait()
    turn(r.dux)
    grad_cols(2, r.n2c)
    red.stage(2, 0)
    dkvp, dkv, dq = r.dkvp, r.dkv, r.dqf
    dq[...] = jnp.zeros_like(dq)

    def back_block(j):
        dkv[...] = jnp.zeros_like(dkv)

        @pl.loop(0, heads // 2)
        def _(pair):
            at = pl.ds(at128(pair * 128), 128)
            vat = pl.ds(at128(qk + pair * 128), 128)
            dv = []
            for e in range(2):
                h = pair * 2 + e
                qh = q_of(h)
                keep_v = (lane // HEAD_V) == e
                keep_q = (lane // FEAT) == h
                s = mm_nt(qh, kv[j, :, 0:qk]) * 0.25
                w = ((1.0 + s + 0.5 * s * s) * mask[j]).astype(BF16)
                dn = jnp.where(keep_v, dnum[:, at], jnp.zeros((), BF16))
                dd = jnp.sum(jnp.where(keep_v, dden[:, at], 0.0), axis=1, keepdims=True)
                dw = mm_nt(dn, kv[j, :, vat]) - dd
                ds = (dw * (1.0 + s) * (0.25 * mask[j])).astype(BF16)
                dv.append(mm_tn(w, dn))
                kh = jnp.where(keep_q, kv[j, :, 0:qk], jnp.zeros((), BF16))
                dq[...] += mm(ds, kh)
                dkv[:, 0:qk] += mm_tn(ds, qh)
            dkv[:, vat] = dv[0] + dv[1]

    @pl.loop(0, b)
    def _(j):
        back_block(j)
        dkvp[j] = dkv[...].astype(BF16)

    red.stage(0, 1)
    dks, dkr = r.dksem
    back = r.back

    def dk_copy(src, slot, which, peer):
        return remote(src, back.at[slot], dks.at[which], dkr.at[slot], ctx=peer)

    @pl.when(c == 1)
    def _():
        dk_copy(dkvp.at[p.ic], 0, 0, p.ic).start()

    @pl.when(x == 1)
    def _():
        dk_copy(dkvp.at[1 - c], 1, 1, p.ic).start()

    @pl.when(x == 1)
    def _():
        dk_copy(dkvp.at[1 - c], 1, 1, p.ic).wait_recv()
        dkvp[b] = (dkvp[c].astype(F32) + back[1].astype(F32)).astype(BF16)
        dk_copy(dkvp.at[b], 2, 2, p.xp).start()

    back_block(b)

    @pl.when(c == 0)
    def _():
        dk_copy(dkvp.at[b], 0, 0, p.ic).wait_recv()
        dkv[...] += back[0].astype(F32)

    dqkv = r.dqkv
    dqkv[:, 0:qk] = dq[...].astype(BF16)
    joined(0, 3)
    red.stage(3, 0)
    red.stage(1, 1)

    @pl.when(x == 0)
    def _():
        dk_copy(dkvp.at[b], 2, 2, p.xp).wait_recv()
        dkv[...] += back[2].astype(F32)

    dqkv[:, qk : 2 * qk + vw] = dkv[...].astype(BF16)
    send_dqkv.start()
    for ch in range(blocks):
        y_put(3, ch, mm_nt(dqkv[...], fqkv[ch * 256 : ch * 256 + 256, :]))
    send_n1.wait()
    turn(r.n1c)
    send_dqkv.wait()

    def qkv_half(dst, xx):
        cols = (2 * qk + vw) // 2
        rhs = r.dqkvx[:, pl.ds(at128(xx * cols), cols)]
        res = mm(turned[0:half_d, 0 : 2 * rows_here], rhs).astype(BF16)
        for s in range(n):
            dst[s] = res[s * 128 : s * 128 + 128, :]

    halve(1, 4, qkv_half)
    red.stage(0, 2)
    joined(1, 4)
    red.stage(4, 0)
    red.stage(2, 1)
    red.last(0)

    y_wait(3)

    def input_back(rs):
        d = norm_back(3, 0, x_rows(rs), r.mis[rs, :], rs).astype(BF16)
        for i, o in enumerate(order):
            r.grad_in[rs, o : o + 128] = d[:, i * 128 : i * 128 + 128]

    per_rows(input_back)

    sms, smr = r.smsem
    parts, lines = r.smctx, r.smz
    for i, peer in enumerate((p.ic, p.xp, p.dg)):
        remote(small, parts.at[b], sms.at[0, i], smr.at[0, b], ctx=peer).start()
    parts[b] = small[...]
    red.stage(3, 1)
    red.stage(1, 2)
    for i, peer in enumerate((p.ic, p.xp, p.dg)):
        remote(small, parts.at[peer], sms.at[0, i], smr.at[0, peer], ctx=peer).wait_recv()
    lines[n] = parts[0] + parts[1] + parts[2] + parts[3]
    for s in range(n):

        @pl.when(z != s)
        def _():
            remote(lines.at[n], lines.at[z], sms.at[1, s], smr.at[1, z], fsdp=s).start()

    red.last(1)
    red.stage(4, 1)
    red.stage(2, 2)
    red.last(2)
    red.relay(0)
    red.stage(3, 2)
    red.last(3)
    red.stage(4, 2)
    red.relay(1)
    red.last(4)
    for s in range(n):

        @pl.when(z != s)
        def _():
            remote(lines.at[n], lines.at[s], sms.at[1, s], smr.at[1, s], fsdp=s).wait_recv()

    total = jnp.zeros_like(small)
    for s in range(n):
        total += jnp.where(z == s, lines[n], lines[s])
    r.gain[...] = total
    for cc in range(2):
        at = pl.ds(at128((cc * n + z) * 128), 128)
        r.grad_attn[0:1, cc * 128 : cc * 128 + 128] = r.gain[0:1, at]
        r.grad_ffn[0:1, cc * 128 : cc * 128 + 128] = r.gain[1:2, at]
    r.loss[...] = jnp.sum(total[2:3, :], axis=1, keepdims=True) / (total[3:4, 0:1] * width)
    red.relay(2)
    red.relay(3)
    red.relay(4)
    for g in (4, 0, 1, 2, 3):
        red.finish(g)
        if g == 4:
            r.grad_q[...] = r.out_q[:, 0:qk].astype(F32)
            r.grad_k[...] = r.out_q[:, qk : 2 * qk].astype(F32)
            r.grad_v[...] = r.out_q[:, 2 * qk : 2 * qk + vw].astype(F32)

    for i in range(2):
        half_copy(i).wait_send()
    gather.drain()
    for k in (send_n1, send_da, send_n2, send_dy, send_hid, send_dg, send_du, send_mix, send_dqkv):
        k.drain()
    for i in range(4):
        for ch in range(blocks):
            y_copy(i, ch).wait_send()
    for s in range(n):

        @pl.when(z != s)
        def _():
            remote(r.gains, gath.at[z], gsend.at[s], grecv.at[z], fsdp=s).wait_send()
            remote(lines.at[n], lines.at[z], sms.at[1, s], smr.at[1, z], fsdp=s).wait_send()

    for i, peer in enumerate((p.ic, p.xp, p.dg)):
        remote(r.segrow, r.segall.at[b], segs.at[i], segr.at[b], ctx=peer).wait_send()
        remote(small, parts.at[b], sms.at[0, i], smr.at[0, b], ctx=peer).wait_send()

    @pl.when(x == 0)
    def _():
        kv_copy(b, 0, p.xp).wait_send()

    @pl.when(c == 0)
    def _():
        kv_copy(b, 1, p.ic).wait_send()

    @pl.when(x == 1)
    def _():
        kv_copy(c, 2, p.ic).wait_send()
        dk_copy(dkvp.at[1 - c], 1, 1, p.ic).wait_send()
        dk_copy(dkvp.at[b], 2, 2, p.xp).wait_send()

    @pl.when(c == 1)
    def _():
        dk_copy(dkvp.at[p.ic], 0, 0, p.ic).wait_send()


def mega(n, layer_in, segment_ids, valid_mask, teacher, attn_gain, w_query, w_key, w_value, w_out, ffn_gain, w_gate, w_up, w_down):
    x = layer_in[0]
    rows, width = x.shape
    qk, vw, ff = w_query.shape[1], w_value.shape[1], w_gate.shape[1]
    ffp = up_to(ff, 128)
    fh = up_to(ffp // 2, 256)
    half_d = width // 2
    blocks = width // 256
    inputs = dict(
        x=x,
        teacher=teacher[0],
        wq=w_query,
        wk=w_key,
        wv=w_value,
        wo=w_out,
        wg=w_gate.T,
        wu=w_up.T,
        wd=w_down,
        attn_gain=attn_gain,
        ffn_gain=ffn_gain,
        segment=segment_ids,
        real=valid_mask,
    )
    hbm = list(inputs)[:9]
    outs = dict(
        layer_out=((rows, width), BF16),
        grad_in=((rows, width), BF16),
        out_d=((ffp, width // n), BF16),
        out_g=((ffp, width // n), BF16),
        out_u=((ffp, width // n), BF16),
        out_o=((vw, width // n), BF16),
        grad_q=((width // n, qk), F32),
        grad_k=((width // n, qk), F32),
        grad_v=((width // n, vw), F32),
        grad_attn=((1, width // n), F32),
        grad_ffn=((1, width // n), F32),
        loss=((1, 1), F32),
    )
    dma = pltpu.SemaphoreType.DMA
    ng = 8
    vm = pltpu.VMEM
    piece = [(ffp, 128), (fh, 128), (fh, 128), (vw // 2, 128), (128, (2 * qk + vw) // 2)]
    scratch = dict(
        lsem=dma((20,)),
        gs=[dma((ng, n)) for _ in range(9)],
        gnsem=[dma((n,)), dma((n,))],
        segsem=[dma((3,)), dma((4,))],
        psem=[dma((6,)), dma((6,))],
        csem=[dma((1, 3)), dma((1, 4))],
        hsem=[dma((2, 3)), dma((2, 4))],
        ysem=[dma((4, blocks)), dma((4, blocks))],
        kvsem=[dma((3,)), dma((4,))],
        dksem=[dma((3,)), dma((3,))],
        rsem=[dma((5, n)), dma((5, n + 1)), dma((5, 3)), dma((5, 4))],
        smsem=[dma((2, max(n, 3))), dma((2, max(n, 4)))],
        fqkv=vm((width, 2 * qk + vw), BF16),
        fo=vm((vw, width), BF16),
        fg=vm((ffp, width), BF16),
        fu=vm((ffp, width), BF16),
        fd=vm((ffp, width), BF16),
        xv=vm((rows, width), BF16),
        tv=vm((rows, width), BF16),
        gath=vm((n, 8, width // n), F32),
        gain=vm((8, width), F32),
        gains=vm((8, width // n), F32),
        segrow=vm((8, rows), F32),
        segcol=vm((rows, 128), F32),
        valid=vm((rows, 128), F32),
        segall=vm((4, 8, rows), F32),
        n1=vm((rows, width), BF16),
        n2=vm((rows, width), BF16),
        dy=vm((rows, width), BF16),
        da=vm((rows, width), BF16),
        n1c=vm((2 * rows, half_d), BF16),
        n2c=vm((4 * rows, half_d), BF16),
        dyc=vm((2 * rows, half_d), BF16),
        dac=vm((2 * rows, half_d), BF16),
        hid=vm((rows, ffp), BF16),
        dg=vm((rows, ffp), BF16),
        du=vm((rows, ffp), BF16),
        mix=vm((rows, vw), BF16),
        dqkv=vm((rows, 2 * qk + vw), BF16),
        hidx=vm((2 * rows, ffp), BF16),
        dgx=vm((4 * rows, fh), BF16),
        dux=vm((4 * rows, fh), BF16),
        mixx=vm((2 * rows, vw), BF16),
        dqkvx=vm((2 * rows, 2 * qk + vw), BF16),
        ysend=vm((4, max(blocks, n), rows, 256), BF16),
        yrecv=vm((4, blocks, rows, 256), BF16),
        q=vm((rows, qk), BF16),
        kv=vm((4, rows, qk + vw), BF16),
        mask=vm((4, rows, rows), F32),
        num=vm((rows, vw), F32),
        den=vm((rows, vw), F32),
        mid=vm((rows, width), F32),
        mis=vm((rows, width), F32),
        g=vm((rows, ffp), F32),
        u=vm((rows, ffp), F32),
        small=vm((8, width), F32),
        smctx=vm((4, 8, width), F32),
        smz=vm((n + 1, 8, width), F32),
        dnum=vm((rows, vw), BF16),
        dden=vm((rows, vw), F32),
        dqf=vm((rows, qk), F32),
        dkv=vm((rows, qk + vw), F32),
        dkvp=vm((4, rows, qk + vw), BF16),
        back=vm((3, rows, qk + vw), BF16),
        turned=vm((max(ffp, half_d), 4 * rows), BF16),
        part=[vm((n,) + s, BF16) for s in piece],
        seen=[vm((n + 1,) + s, BF16) for s in piece],
        other=vm(piece[0], BF16),
        give=[vm((n,) + piece[i], BF16) for i in (3, 4)],
        got=[vm((n,) + piece[i], BF16) for i in (3, 4)],
        presem=[dma((2,)), dma((2,))],
        out_q=vm((width // n, 2 * qk + vw), BF16),
    )
    flat, layout = [], []
    for k, v in scratch.items():
        if isinstance(v, list):
            layout.append((k, len(v)))
            flat.extend(v)
        else:
            layout.append((k, 0))
            flat.append(v)

    def kernel(*refs):
        names = list(inputs) + list(outs)
        bound = list(refs[: len(names)])
        at = len(names)
        for k, count in layout:
            names.append(k)
            if count:
                bound.append(refs[at : at + count])
                at += count
            else:
                bound.append(refs[at])
                at += 1
        mega_kernel(n, names, *bound)

    res = pl.pallas_call(
        kernel,
        out_shape=[jax.ShapeDtypeStruct(*v) for v in outs.values()],
        in_specs=[pl.BlockSpec(memory_space=pl.ANY if k in hbm else pltpu.VMEM) for k in inputs],
        out_specs=[pl.BlockSpec(memory_space=pltpu.VMEM)] * len(outs),
        scratch_shapes=flat,
        compiler_params=pltpu.CompilerParams(
            collective_id=0, has_side_effects=True, vmem_limit_bytes=67043328
        ),
        name="block_step",
    )(*inputs.values())
    o = SimpleNamespace(**dict(zip(outs, res)))

    return (
        o.layer_out[None],
        o.grad_in[None],
        o.grad_attn[0],
        o.grad_q,
        o.grad_k,
        o.grad_v,
        o.out_o.astype(F32),
        o.grad_ffn[0],
        o.out_g[:ff].astype(F32).T,
        o.out_u[:ff].astype(F32).T,
        o.out_d[:ff].astype(F32),
        o.loss[0, 0],
    )


def per_device(*arrays):
    n = lax.axis_size("fsdp")
    layer_in, w_query, w_value = arrays[0], arrays[5], arrays[7]
    fits = (
        lax.axis_size("ctx") == 4
        and lax.axis_size("tp") == 2
        and layer_in.shape[0] == 1
        and w_query.shape[0] == 256
        and w_query.shape[1] == 128
        and w_value.shape[1] % 512 == 0
        and layer_in.shape[1] % 256 == 0
    )
    return mega(n, *arrays) if fits else general(*arrays)


def solution(mesh):
    placed = (
        P("fsdp", "ctx", None),
        P("fsdp", "ctx"),
        P("fsdp", "ctx"),
        P("fsdp", "ctx", None),
        P("fsdp"),
        P("fsdp", "tp"),
        P("fsdp", "tp"),
        P("fsdp", "tp"),
        P("tp", "fsdp"),
        P("fsdp"),
        P("fsdp", "tp"),
        P("fsdp", "tp"),
        P("tp", "fsdp"),
    )
    return jax.shard_map(
        per_device,
        mesh=mesh,
        in_specs=placed,
        out_specs=(
            P("fsdp", "ctx", None),
            P("fsdp", "ctx", None),
            P("fsdp"),
            P("fsdp", "tp"),
            P("fsdp", "tp"),
            P("fsdp", "tp"),
            P("tp", "fsdp"),
            P("fsdp"),
            P("fsdp", "tp"),
            P("fsdp", "tp"),
            P("tp", "fsdp"),
            P(),
        ),
        check_vma=False,
    )
```

```python
from functools import partial
from types import SimpleNamespace
import math

import jax
import jax.numpy as jnp
from jax import lax
from jax.experimental import pallas as pl
from jax.experimental.pallas import tpu as pltpu
from jax.sharding import PartitionSpec as P

FEAT = 16
HEAD_V = 64


EPSILON = 1e-05
HIGH = lax.Precision.HIGHEST
QUAD_SCALE = 1.0 / (4.0 * math.sqrt(2.0))


def entering(x, axis, join, neutral):
    place = lax.axis_index(axis)
    gathered = jax.tree.map(
        lambda a, kind: lax.all_gather(a.astype(kind), axis),
        x,
        (jnp.bfloat16, jnp.bfloat16, jnp.bfloat16),
    )
    state = jax.tree.map(lambda a, e: jnp.zeros_like(a) + jnp.asarray(e, a.dtype), x, neutral)

    def one(lap, state):
        return join(
            state,
            jax.tree.map(
                lambda a, own: lax.dynamic_index_in_dim(a, lap, 0, False).astype(own.dtype),
                gathered,
                x,
            ),
        )

    return lax.fori_loop(0, place, one, state)


def entering_2(x, axis, combine, identity):
    devices, here = (lax.axis_size(axis), lax.axis_index(axis))
    everything = jax.tree.map(
        lambda part, kind: lax.all_gather(part.astype(kind), axis),
        x,
        jax.tree.map(lambda a: jnp.bfloat16 if a.dtype == jnp.float32 else a.dtype, x),
    )
    start = jax.tree.map(
        lambda part, zero: jnp.broadcast_to(jnp.asarray(zero, part.dtype), part.shape), x, identity
    )

    def lap(k, before):
        at = devices - 1 - k
        reached = at > here
        new = combine(
            before, jax.tree.map(lambda part, own: part[at].astype(own.dtype), everything, x)
        )
        return jax.tree.map(lambda a, b: jnp.where(reached, a, b), new, before)

    return lax.fori_loop(0, devices, lap, start)


def product(left_side, right_side):
    return jnp.dot(left_side, right_side, preferred_element_type=jnp.float32)


def product_left_t(left_side, right_side):
    return lax.dot_general(
        left_side, right_side, (((0,), (0,)), ((), ())), preferred_element_type=jnp.float32
    )


def product_right_t(left_side, right_side):
    return lax.dot_general(
        left_side, right_side, (((1,), (1,)), ((), ())), preferred_element_type=jnp.float32
    )


def features(vectors):
    lead_dims = vectors.shape[:-1]
    feat_width = vectors.shape[-1]
    square = (vectors[..., :, None] * vectors[..., None, :]).reshape(
        lead_dims + (feat_width * feat_width,)
    )
    return jnp.concatenate(
        [jnp.ones(lead_dims + (1,), jnp.float32), 0.5 * vectors, QUAD_SCALE * square], axis=-1
    )


def attend(query_rows, key_rows, value_rows, prev_state, prev_norm, segment, prev_id):
    scores = jnp.einsum("slhf,smhf->shlm", query_rows, key_rows, precision=HIGH) * 0.25
    kernel = 1.0 + scores + 0.5 * scores * scores
    places = jnp.arange(segment.shape[1])
    allowed = (places[:, None] >= places[None, :])[None] & (
        segment[:, :, None] == segment[:, None, :]
    )
    kernel = jnp.where(allowed[:, None], kernel, 0.0)
    carried = (segment.astype(jnp.float32) == prev_id[:, None]).astype(jnp.float32)
    mapped = features(query_rows) * carried[:, :, None, None]
    numerator = jnp.einsum("shlm,smhv->slhv", kernel, value_rows, precision=HIGH) + jnp.einsum(
        "slht,shtv->slhv", mapped, prev_state, precision=HIGH
    )
    denominator = jnp.einsum("shlm->slh", kernel) + jnp.einsum(
        "slht,sht->slh", mapped, prev_norm, precision=HIGH
    )
    return numerator / denominator[..., None]


def summarize(key_rows, value_rows, segment):
    closing = (segment == segment[:, -1:]).astype(jnp.float32)
    mapped = features(key_rows) * closing[:, :, None, None]
    return (
        jnp.einsum("slht,slhv->shtv", mapped, value_rows, precision=HIGH),
        jnp.sum(mapped, axis=1),
    )


def rms_forward(values_in, gain_vec):
    inv_root = lax.rsqrt(jnp.mean(values_in * values_in, axis=-1, keepdims=True) + EPSILON)
    return (values_in * inv_root * gain_vec, inv_root)


def rms_backward(values_in, inv_root, gain_vec, grad_normed):
    weighted = grad_normed * gain_vec
    grad_gain = jnp.sum(grad_normed * values_in * inv_root, axis=0)
    grad_values = inv_root * weighted - values_in * inv_root**3 * jnp.mean(
        weighted * values_in, axis=-1, keepdims=True
    )
    return (grad_values, grad_gain)


def chain_combine(earlier, later):
    is_fresh = later[0] < 0
    same_doc = later[0] == earlier[0]

    def pick(early_part, late_part):
        expand = (-1,) + (1,) * (early_part.ndim - 1)
        with_early = late_part + jnp.where(same_doc.reshape(expand), early_part, 0.0)
        return jnp.where(is_fresh.reshape(expand), early_part, with_early)

    return (
        jnp.where(is_fresh, earlier[0], later[0]),
        pick(earlier[1], later[1]),
        pick(earlier[2], later[2]),
    )


def tp_forward(partial_sum):
    return lax.psum(partial_sum, "tp")


def tp_backward(partial_sum):
    return lax.psum(partial_sum.astype(jnp.bfloat16), "tp").astype(jnp.float32)


def general(
    layer_in,
    segment_ids,
    valid_mask,
    teacher,
    attn_gain,
    w_query,
    w_key,
    w_value,
    w_out,
    ffn_gain,
    w_gate,
    w_up,
    w_down,
):
    full_weights = (
        lax.all_gather(attn_gain, "fsdp", axis=0, tiled=True),
        lax.all_gather(w_query, "fsdp", axis=0, tiled=True),
        lax.all_gather(w_key, "fsdp", axis=0, tiled=True),
        lax.all_gather(w_value, "fsdp", axis=0, tiled=True),
        lax.all_gather(w_out, "fsdp", axis=1, tiled=True),
        lax.all_gather(ffn_gain, "fsdp", axis=0, tiled=True),
        lax.all_gather(w_gate, "fsdp", axis=0, tiled=True),
        lax.all_gather(w_up, "fsdp", axis=0, tiled=True),
        lax.all_gather(w_down, "fsdp", axis=1, tiled=True),
    )
    (
        gain_one,
        full_query,
        full_key,
        full_value,
        full_out,
        gain_two,
        full_gate,
        full_up,
        full_down,
    ) = full_weights
    seq_count, shard_len, model_width = layer_in.shape
    row_count = seq_count * shard_len
    heads_here = full_query.shape[1] // FEAT
    rows_in = layer_in.reshape(row_count, model_width).astype(jnp.float32)
    normed_full, root_one = rms_forward(rows_in, gain_one.astype(jnp.float32))
    normed_one = normed_full.astype(jnp.bfloat16)
    query_rows = product(normed_one, full_query).reshape(seq_count, shard_len, heads_here, FEAT)
    key_rows = product(normed_one, full_key).reshape(seq_count, shard_len, heads_here, FEAT)
    value_rows = product(normed_one, full_value).reshape(seq_count, shard_len, heads_here, HEAD_V)
    last_id = segment_ids[:, -1].astype(jnp.float32)
    first_id = segment_ids[:, 0].astype(jnp.float32)
    (out_state, out_norm), summary_pull = jax.vjp(
        partial(summarize, segment=segment_ids), key_rows, value_rows
    )
    blank_state = jnp.zeros_like(out_state)
    blank_norm = jnp.zeros_like(out_norm)
    no_doc = jnp.full_like(last_id, -1.0)
    prev_id, prev_state, prev_norm = entering(
        (last_id, out_state, out_norm), "ctx", chain_combine, (no_doc, blank_state, blank_norm)
    )
    attended, attend_pull = jax.vjp(
        partial(attend, segment=segment_ids, prev_id=prev_id),
        query_rows,
        key_rows,
        value_rows,
        prev_state,
        prev_norm,
    )
    mixed_heads = attended.reshape(row_count, heads_here * HEAD_V).astype(jnp.bfloat16)
    head_sum = product(mixed_heads, full_out)
    teacher_rows = teacher.reshape(row_count, model_width).astype(jnp.float32)
    weight_rows = valid_mask.reshape(row_count, 1).astype(jnp.float32)
    middle = rows_in + tp_forward(head_sum)
    normed_mid, root_two = rms_forward(middle, gain_two.astype(jnp.float32))
    normed_two = normed_mid.astype(jnp.bfloat16)
    gate_rows = product(normed_two, full_gate)
    up_rows = product(normed_two, full_up)
    sigmoid_gate = jax.nn.sigmoid(gate_rows)
    silu_gate = gate_rows * sigmoid_gate
    hidden = (silu_gate * up_rows).astype(jnp.bfloat16)
    down_sum = product(hidden, full_down)
    output = middle + tp_forward(down_sum)
    misfit = (output - teacher_rows) * weight_rows
    layer_rows = output.astype(jnp.bfloat16)
    grad_rows = misfit.astype(jnp.bfloat16)
    sum_squares = jnp.sum(misfit * misfit)
    sum_valid = jnp.sum(weight_rows)
    grad_down = product_left_t(hidden, grad_rows)
    grad_hidden = product_right_t(grad_rows, full_down)
    grad_gate_rows = (
        grad_hidden * up_rows * sigmoid_gate * (1.0 + gate_rows * (1.0 - sigmoid_gate))
    ).astype(jnp.bfloat16)
    grad_up_rows = (grad_hidden * silu_gate).astype(jnp.bfloat16)
    grad_gate = product_left_t(normed_two, grad_gate_rows)
    grad_up = product_left_t(normed_two, grad_up_rows)
    normed_two_terms = product_right_t(grad_gate_rows, full_gate) + product_right_t(
        grad_up_rows, full_up
    )
    grad_normed_two = tp_backward(normed_two_terms)
    grad_mid_norm, grad_ffn_gain = rms_backward(
        middle, root_two, gain_two.astype(jnp.float32), grad_normed_two
    )
    grad_middle = misfit + grad_mid_norm
    grad_branch = grad_middle.astype(jnp.bfloat16)
    grad_out = product_left_t(mixed_heads, grad_branch)
    grad_mixed = product_right_t(grad_branch, full_out).reshape(
        seq_count, shard_len, heads_here, HEAD_V
    )
    grad_q_near, grad_k_near, grad_v_near, grad_prev_state, grad_prev_norm = attend_pull(grad_mixed)
    next_id, later_state, later_norm = entering_2(
        (first_id, grad_prev_state, grad_prev_norm),
        "ctx",
        chain_combine,
        (no_doc, blank_state, blank_norm),
    )
    continues = (next_id == last_id).astype(jnp.float32)
    grad_k_far, grad_v_far = summary_pull(
        (later_state * continues[:, None, None, None], later_norm * continues[:, None, None])
    )
    grad_query_rows = grad_q_near.reshape(row_count, heads_here * FEAT).astype(jnp.bfloat16)
    grad_key_rows = (
        (grad_k_near + grad_k_far).reshape(row_count, heads_here * FEAT).astype(jnp.bfloat16)
    )
    grad_value_rows = (
        (grad_v_near + grad_v_far).reshape(row_count, heads_here * HEAD_V).astype(jnp.bfloat16)
    )
    grad_query = product_left_t(normed_one, grad_query_rows)
    grad_key = product_left_t(normed_one, grad_key_rows)
    grad_value = product_left_t(normed_one, grad_value_rows)
    normed_one_terms = (
        product_right_t(grad_query_rows, full_query)
        + product_right_t(grad_key_rows, full_key)
        + product_right_t(grad_value_rows, full_value)
    )
    grad_normed_one = tp_backward(normed_one_terms)
    grad_rows_in, grad_attn_gain = rms_backward(
        rows_in, root_one, gain_one.astype(jnp.float32), grad_normed_one
    )
    grad_in_rows = (grad_middle + grad_rows_in).astype(jnp.bfloat16)
    total_sq, total_valid = lax.psum((sum_squares, sum_valid), ("fsdp", "ctx"))
    loss_value = total_sq / (total_valid * model_width)
    grad_in = grad_in_rows.reshape(seq_count, shard_len, model_width)
    layer_out = layer_rows.reshape(seq_count, shard_len, model_width)
    owned = (
        lax.psum_scatter(
            grad_attn_gain.astype(jnp.bfloat16), "fsdp", scatter_dimension=0, tiled=True
        ).astype(jnp.float32),
        lax.psum_scatter(
            grad_query.astype(jnp.bfloat16), "fsdp", scatter_dimension=0, tiled=True
        ).astype(jnp.float32),
        lax.psum_scatter(
            grad_key.astype(jnp.bfloat16), "fsdp", scatter_dimension=0, tiled=True
        ).astype(jnp.float32),
        lax.psum_scatter(
            grad_value.astype(jnp.bfloat16), "fsdp", scatter_dimension=0, tiled=True
        ).astype(jnp.float32),
        lax.psum_scatter(
            grad_out.astype(jnp.bfloat16), "fsdp", scatter_dimension=1, tiled=True
        ).astype(jnp.float32),
        lax.psum_scatter(
            grad_ffn_gain.astype(jnp.bfloat16), "fsdp", scatter_dimension=0, tiled=True
        ).astype(jnp.float32),
        lax.psum_scatter(
            grad_gate.astype(jnp.bfloat16), "fsdp", scatter_dimension=0, tiled=True
        ).astype(jnp.float32),
        lax.psum_scatter(
            grad_up.astype(jnp.bfloat16), "fsdp", scatter_dimension=0, tiled=True
        ).astype(jnp.float32),
        lax.psum_scatter(
            grad_down.astype(jnp.bfloat16), "fsdp", scatter_dimension=1, tiled=True
        ).astype(jnp.float32),
    )
    shares = (
        lax.psum(owned[0].astype(jnp.bfloat16), "ctx").astype(jnp.float32),
        lax.psum(owned[1].astype(jnp.bfloat16), "ctx").astype(jnp.float32),
        lax.psum(owned[2].astype(jnp.bfloat16), "ctx").astype(jnp.float32),
        lax.psum(owned[3].astype(jnp.bfloat16), "ctx").astype(jnp.float32),
        lax.psum(owned[4].astype(jnp.bfloat16), "ctx").astype(jnp.float32),
        lax.psum(owned[5].astype(jnp.bfloat16), "ctx").astype(jnp.float32),
        lax.psum(owned[6].astype(jnp.bfloat16), "ctx").astype(jnp.float32),
        lax.psum(owned[7].astype(jnp.bfloat16), "ctx").astype(jnp.float32),
        lax.psum(owned[8].astype(jnp.bfloat16), "ctx").astype(jnp.float32),
    )
    return (
        layer_out,
        grad_in,
        shares[0],
        shares[1],
        shares[2],
        shares[3],
        shares[4],
        shares[5],
        shares[6],
        shares[7],
        shares[8],
        loss_value,
    )


MESH = pl.DeviceIdType.MESH
F32 = jnp.float32
BF16 = jnp.bfloat16


def up_to(size, step):
    return -(-size // step) * step


def mm(a, b):
    return jnp.dot(a, b, preferred_element_type=F32)


def mm_nt(a, b):
    return lax.dot_general(a, b, (((1,), (1,)), ((), ())), preferred_element_type=F32)


def mm_tn(a, b):
    return lax.dot_general(a, b, (((0,), (0,)), ((), ())), preferred_element_type=F32)


def at128(offset):
    return pl.multiple_of(offset, 128)


class Place:
    def __init__(self, n):
        self.n = n
        self.z = lax.axis_index("fsdp")
        self.b = lax.axis_index("ctx")
        self.t = lax.axis_index("tp")
        self.x = self.b // 2
        self.c = self.b % 2
        self.ic = self.x * 2 + (1 - self.c)
        self.xp = (1 - self.x) * 2 + self.c
        self.dg = (1 - self.x) * 2 + (1 - self.c)


def remote(src, dst, send, recv, **where):
    return pltpu.make_async_remote_copy(
        src_ref=src, dst_ref=dst, send_sem=send, recv_sem=recv, device_id=where, device_id_type=MESH
    )


def entry_barrier(p):
    sem = pltpu.get_barrier_semaphore()
    for s in range(p.n):

        @pl.when(p.z != s)
        def _():
            pl.semaphore_signal(sem, inc=1, device_id={"fsdp": s}, device_id_type=MESH)

    for peer in (p.ic, p.xp, p.dg):
        pl.semaphore_signal(sem, inc=1, device_id={"ctx": peer}, device_id_type=MESH)
    pl.semaphore_signal(sem, inc=1, device_id={"tp": 1 - p.t}, device_id_type=MESH)
    pl.semaphore_wait(sem, p.n - 1 + 4)


class Gather:
    def __init__(self, p, pieces, sems):
        self.p = p
        self.pieces = pieces
        (self.zr, self.xr, self.i1r, self.i2r, self.zsl, self.zsr, self.xs, self.i1s, self.i2s) = sems

    def quarter(self, g, s, x, c):
        ref, kind, lo, size = self.pieces[g]
        n = self.p.n
        if kind == "row":
            return ref.at[pl.ds(pl.multiple_of((c * n + s) * 128 + x * 64 + lo[0], 16), size), 0 : lo[1]]
        half = lo[1]
        return ref.at[
            pl.ds(pl.multiple_of(x * half + lo[0], 16), size), pl.ds(at128((c * n + s) * 128), 128)
        ]

    def copy(self, g, s, x, c, send, recv, **where):
        ref = self.quarter(g, s, x, c)
        return remote(ref, ref, send.at[g, s], recv.at[g, s], **where)

    def left(self, g, s):
        return self.copy(g, s, self.p.x, self.p.c, self.zsl, self.zr, fsdp=self.p.z - 1)

    def right(self, g, s):
        return self.copy(g, s, self.p.x, self.p.c, self.zsr, self.zr, fsdp=self.p.z + 1)

    def chip(self, g, s, x, c, second):
        if second:
            return self.copy(g, s, x, c, self.i2s, self.i2r, ctx=self.p.ic)
        return self.copy(g, s, x, c, self.i1s, self.i1r, ctx=self.p.ic)

    def cross(self, g, s, x, c):
        return self.copy(g, s, x, c, self.xs, self.xr, ctx=self.p.xp)

    def own(self, g):
        p = self.p

        @pl.when(p.z > 0)
        def _():
            self.left(g, p.z).start()

        @pl.when(p.z < p.n - 1)
        def _():
            self.right(g, p.z).start()

    def hop(self, g, h):
        p = self.p
        for d in (1, -1):
            s = p.z + d * h
            there = (s < p.n) if d == 1 else (s >= 0)

            @pl.when(there)
            def _():
                self.copy(g, s, p.x, p.c, self.zsl, self.zr, fsdp=p.z).wait_recv()
                if d == 1:

                    @pl.when(p.z > 0)
                    def _():
                        self.left(g, s).start()

                else:

                    @pl.when(p.z < p.n - 1)
                    def _():
                        self.right(g, s).start()

                self.cross(g, s, p.x, p.c).start()
                self.chip(g, s, p.x, p.c, False).start()

    def hop_cross(self, g, h):
        p = self.p
        for d in (1, -1):
            s = p.z + d * h
            there = (s < p.n) if d == 1 else (s >= 0)

            @pl.when(there)
            def _():
                self.cross(g, s, 1 - p.x, p.c).wait_recv()
                self.chip(g, s, 1 - p.x, p.c, True).start()

    def whole(self, g, s):
        p = self.p
        self.chip(g, s, p.x, 1 - p.c, False).wait_recv()
        self.chip(g, s, 1 - p.x, 1 - p.c, True).wait_recv()

    def finish(self, g):
        p = self.p

        @pl.loop(0, p.n)
        def _(s):
            @pl.when(s != p.z)
            def _():
                self.whole(g, s)

    def drain(self):
        p = self.p
        for g in range(len(self.pieces)):

            @pl.loop(0, p.n)
            def _(s):
                @pl.when((s >= p.z) & (p.z > 0))
                def _():
                    self.left(g, s).wait_send()

                @pl.when((s <= p.z) & (p.z < p.n - 1))
                def _():
                    self.right(g, s).wait_send()

                @pl.when(s != p.z)
                def _():
                    self.cross(g, s, p.x, p.c).wait_send()
                    self.chip(g, s, p.x, p.c, False).wait_send()
                    self.chip(g, s, 1 - p.x, p.c, True).wait_send()


class Reduce:
    def __init__(self, p, parts, seen, done, other, sems):
        self.p = p
        self.parts = parts
        self.seen = seen
        self.done = done
        self.other = other
        (self.ss, self.rs, self.fs, self.fr) = sems

    def move(self, g, s, slot, to):
        return remote(
            self.parts[g].at[s], self.seen[g].at[slot], self.ss.at[g, s], self.rs.at[g, slot], fsdp=to
        )

    def arrived(self, g, slot):
        self.move(g, 0, slot, self.p.z).wait_recv()

    def by_rows(self, g, body):
        @pl.loop(0, self.parts[g].shape[1] // 128)
        def _(i):
            body(pl.ds(at128(i * 128), 128))

    def add(self, g, s, slot):
        def body(at):
            total = self.parts[g][s, at, :].astype(F32) + self.seen[g][slot, at, :].astype(F32)
            self.parts[g][s, at, :] = total.astype(BF16)

        self.by_rows(g, body)

    def stage(self, g, k):
        p = self.p
        n = p.n

        @pl.when(p.z == k)
        def _():
            for s in range(n - 1, k, -1):
                if k > 0:
                    self.arrived(g, s)
                    self.add(g, s, s)
                self.move(g, s, s, k + 1).start()

        @pl.when(p.z == n - 1 - k)
        def _():
            z = n - 1 - k
            for s in range(0, z):
                if k > 0:
                    self.arrived(g, s)
                    self.add(g, s, s)
                self.move(g, s, n if s == z - 1 else s, z - 1).start()

    def last(self, g):
        p = self.p
        n = p.n

        @pl.when(p.z > 0)
        def _():
            self.arrived(g, p.z)
            self.add(g, p.z, p.z)

        @pl.when(p.z < n - 1)
        def _():
            self.arrived(g, n)
            self.add(g, p.z, n)

        if self.other[g] is not None:
            self.across(g).start()
            return
        self.block(g, p.x, p.c)[...] = self.mine(g)[...]
        self.spread(g, p.b, 0, p.ic, self.mine(g)).start()
        self.spread(g, p.b, 1, p.xp, self.mine(g)).start()

    def mine(self, g):
        p = self.p
        if self.done[g].shape[1] != 256:
            return self.parts[g].at[p.z]
        half = self.done[g].shape[0] // 2
        skip = self.parts[g].shape[1] - half
        return self.parts[g].at[p.z, pl.ds(pl.multiple_of(p.x * skip, 16), half), :]

    def block(self, g, x, c):
        if self.done[g].shape[1] != 256:
            w = self.done[g].shape[1] // 2
            return self.done[g].at[pl.ds(at128(c * 128), 128), pl.ds(at128(x * w), w)]
        half = self.done[g].shape[0] // 2
        return self.done[g].at[pl.ds(pl.multiple_of(x * half, 16), half), pl.ds(at128(c * 128), 128)]

    def spread(self, g, slot, which, to, src=None):
        dst = self.block(g, slot // 2, slot % 2)
        return remote(dst if src is None else src, dst, self.fs.at[g, which], self.fr.at[g, slot], ctx=to)

    def side(self, g, c):
        return self.done[g].at[:, pl.ds(at128(c * 128), 128)]

    def across(self, g):
        p = self.p
        return remote(self.parts[g].at[p.z], self.other[g], self.fs.at[g, 0], self.fr.at[g, 0], ctx=p.xp)

    def beside(self, g, c):
        ref = self.side(g, c)
        return remote(ref, ref, self.fs.at[g, 1], self.fr.at[g, 1], ctx=self.p.ic)

    def relay(self, g):
        p = self.p
        if self.other[g] is not None:
            self.across(g).wait_recv()

            side = self.side(g, p.c)

            def body(at):
                total = self.parts[g][p.z, at, :].astype(F32) + self.other[g][at, :].astype(F32)
                side[at, :] = total.astype(BF16)

            self.by_rows(g, body)
            self.beside(g, p.c).start()
            return
        self.spread(g, p.xp, 1, p.xp).wait_recv()
        self.spread(g, p.xp, 2, p.ic).start()

    def finish(self, g):
        p = self.p
        if self.other[g] is not None:
            self.beside(g, 1 - p.c).wait_recv()
            self.beside(g, p.c).wait_send()
            self.across(g).wait_send()
        else:
            self.spread(g, p.ic, 0, p.ic).wait_recv()
            self.spread(g, p.dg, 2, p.ic).wait_recv()
            self.spread(g, p.b, 0, p.ic, self.mine(g)).wait_send()
            self.spread(g, p.b, 1, p.xp, self.mine(g)).wait_send()
            self.spread(g, p.xp, 2, p.ic).wait_send()

        @pl.loop(0, p.n)
        def _(s):
            @pl.when(s != p.z)
            def _():
                self.move(g, s, 0, p.z).wait_send()


class Columns:
    def __init__(self, p, k, src, dst, sems):
        self.p = p
        self.k = k
        self.src = src
        self.dst = dst
        self.send, self.recv = sems

    def slot(self, b):
        rows = self.src.shape[0]
        return self.dst.at[pl.ds(pl.multiple_of(b * rows, rows), rows), :]

    def copy(self, peer, which):
        p = self.p
        w = self.dst.shape[1]
        part = self.src.at[:, pl.ds(at128((peer % 2) * w), w)]
        return remote(part, self.slot(p.b), self.send.at[self.k, which], self.recv.at[self.k, p.b], ctx=peer)

    def start(self):
        p = self.p
        w = self.dst.shape[1]
        for which, peer in enumerate((p.xp, p.dg, p.ic)):
            self.copy(peer, which).start()
        self.slot(p.b)[...] = self.src[:, pl.ds(at128(p.c * w), w)]

    def wait(self):
        p = self.p
        for peer in (p.ic, p.xp, p.dg):
            remote(self.slot(peer), self.slot(peer), self.send.at[self.k, 0], self.recv.at[self.k, peer], ctx=peer).wait_recv()

    def drain(self):
        p = self.p
        for which, peer in enumerate((p.xp, p.dg, p.ic)):
            self.copy(peer, which).wait_send()


class Pair:
    def __init__(self, p, k, src, dst, sems):
        self.p = p
        self.k = k
        self.src = src
        self.dst = dst
        self.send, self.recv = sems

    def slot(self, c):
        rows = self.src.shape[0]
        return self.dst.at[pl.ds(pl.multiple_of(c * rows, rows), rows), :]

    def part(self, c):
        w = self.dst.shape[1]
        if w == self.src.shape[1]:
            return self.src
        return self.src.at[:, pl.ds(at128(c * w), w)]

    def copy(self):
        p = self.p
        return remote(self.part(1 - p.c), self.slot(p.c), self.send.at[self.k], self.recv.at[self.k], ctx=p.ic)

    def start(self):
        c = self.p.c
        self.copy().start()
        self.slot(c)[...] = self.part(c)[...]

    def wait(self):
        p = self.p
        remote(self.part(1 - p.c), self.slot(1 - p.c), self.send.at[self.k], self.recv.at[self.k], ctx=p.ic).wait_recv()

    def drain(self):
        self.copy().wait_send()


class Halves:
    def __init__(self, p, k, src, dst, step, sems):
        self.p = p
        self.k = k
        self.src = src
        self.dst = dst
        self.step = step
        self.send, self.recv = sems

    def slot(self, b):
        rows = self.src.shape[0]
        return self.dst.at[pl.ds(pl.multiple_of(b * rows, rows), rows), :]

    def part(self, x):
        return self.src.at[:, pl.ds(at128(x * self.step), self.dst.shape[1])]

    def to(self, src, slot, which, peer):
        return remote(src, self.slot(slot), self.send.at[self.k, which], self.recv.at[self.k, slot], ctx=peer)

    def start(self):
        p = self.p
        self.to(self.part(1 - p.x), p.b, 0, p.xp).start()
        self.to(self.part(p.x), p.b, 1, p.ic).start()
        self.slot(p.b)[...] = self.src[:, pl.ds(at128(p.x * self.step), self.dst.shape[1])]

    def relay(self):
        p = self.p
        self.to(self.slot(p.xp), p.xp, 2, p.ic).wait_recv()
        self.to(self.slot(p.xp), p.xp, 2, p.ic).start()

    def wait(self):
        p = self.p
        self.to(self.slot(p.ic), p.ic, 1, p.ic).wait_recv()
        self.to(self.slot(p.dg), p.dg, 1, p.ic).wait_recv()

    def drain(self):
        p = self.p
        self.to(self.part(1 - p.x), p.b, 0, p.xp).wait_send()
        self.to(self.part(p.x), p.b, 1, p.ic).wait_send()
        self.to(self.slot(p.xp), p.xp, 2, p.ic).wait_send()


def mega_kernel(n, names, *refs):
    r = SimpleNamespace(**dict(zip(names, refs)))
    p = Place(n)
    z, b, x, c = p.z, p.b, p.x, p.c
    rows_here = r.x.shape[0]
    width = r.x.shape[1]
    half_d = width // 2
    heads = r.wv.shape[1] // HEAD_V
    qk = r.wq.shape[1]
    vw = r.wv.shape[1]
    ff = r.wd.shape[0]
    ffp = r.hid.shape[1]
    order = [s * 256 + cc * 128 for cc in range(2) for s in range(n)]
    blocks = width // 256
    D = r.lsem

    fqkv, fo, fg, fu, fd = r.fqkv, r.fo, r.fg, r.fu, r.fd
    local = []

    def bring(src, dst):
        copy = pltpu.make_async_copy(src, dst, D.at[len(local)])
        copy.start()
        local.append(copy)
        return copy

    get_x = bring(r.x, r.xv)
    need = {}
    for cc in range(2):
        rows = pl.ds(at128((cc * n + z) * 128), 128)
        src = slice(cc * 128, cc * 128 + 128)
        need.setdefault("qkv", []).extend(
            (
                bring(r.wq.at[src, :], fqkv.at[rows, 0:qk]),
                bring(r.wk.at[src, :], fqkv.at[rows, qk : 2 * qk]),
                bring(r.wv.at[src, :], fqkv.at[rows, 2 * qk : 2 * qk + vw]),
            )
        )
    for cc in range(2):
        cols = pl.ds(at128((cc * n + z) * 128), 128)
        need.setdefault("o", []).append(bring(r.wo.at[:, cc * 128 : cc * 128 + 128], fo.at[:, cols]))
    for key, src, dst in (("g", r.wg, fg), ("u", r.wu, fu), ("d", r.wd, fd)):
        for cc in range(2):
            cols = pl.ds(at128((cc * n + z) * 128), 128)
            need.setdefault(key, []).append(bring(src.at[:, cc * 128 : cc * 128 + 128], dst.at[0:ff, cols]))
    get_teacher = bring(r.teacher, r.tv)

    pieces, first = [], []

    def split(total, parts):
        unit = total // 16
        edge = [(unit * i // parts) * 16 for i in range(parts + 1)]
        return [(edge[i], edge[i + 1] - edge[i]) for i in range(parts)]

    for key, ref, kind, total, parts in (
        ("qkv", fqkv, "row", 64, 1),
        ("o", fo, "col", vw // 2, 1),
        ("g", fg, "col", ff // 2, 2),
        ("u", fu, "col", ff // 2, 2),
        ("d", fd, "col", ff // 2, 2),
    ):
        for i, (lo, size) in enumerate(split(total, parts)):
            pieces.append((ref, kind, (lo, ref.shape[1]) if kind == "row" else (lo, total), size))
            first.append(need[key] if i == 0 else [])
    gather = Gather(p, pieces, r.gs)
    ng = len(pieces)

    def own(g):
        for copy in first[g]:
            copy.wait()
        gather.own(g)

    entry_barrier(p)
    own(0)
    own(1)

    r.gains[...] = jnp.concatenate(
        [r.attn_gain[...].astype(F32).reshape(1, -1), r.ffn_gain[...].astype(F32).reshape(1, -1)]
        + [jnp.zeros((6, width // n), F32)],
        axis=0,
    )
    segment = r.segment[...].astype(F32)
    r.segrow[...] = jnp.broadcast_to(segment, (8, rows_here))
    r.segcol[...] = jnp.transpose(jnp.broadcast_to(segment, (128, rows_here)))
    r.valid[...] = jnp.transpose(jnp.broadcast_to(r.real[...].astype(F32), (128, rows_here)))
    gsend, grecv, gath = r.gnsem[0], r.gnsem[1], r.gath
    for s in range(n):

        @pl.when(z != s)
        def _():
            remote(r.gains, gath.at[z], gsend.at[s], grecv.at[z], fsdp=s).start()

    gath[z] = r.gains[...]
    segs, segr = r.segsem[0], r.segsem[1]
    for i, peer in enumerate((p.ic, p.xp, p.dg)):
        remote(r.segrow, r.segall.at[b], segs.at[i], segr.at[b], ctx=peer).start()
    r.segall[b] = r.segrow[...]

    pad = ffp - ff
    if pad:
        for ref in (fg, fu, fd):
            ref[ff:ffp, :] = jnp.zeros((pad, width), BF16)

    for s in range(n):

        @pl.when(z != s)
        def _():
            remote(r.gains, gath.at[s], gsend.at[s], grecv.at[s], fsdp=s).wait_recv()

    for row in range(2):
        r.gain[row : row + 1, :] = jnp.concatenate(
            [gath[s, row : row + 1, cc * 128 : cc * 128 + 128] for cc in range(2) for s in range(n)], axis=1
        )

    events = [(g - 0.7, "own", g, 0) for g in range(2, ng)]
    for g in range(ng):
        for h in range(1, n):
            events.append((g + 0.6 * h, "hop", g, h))
            events.append((g + 0.6 * h + 0.8, "cross", g, h))
    events.sort()
    passed = [0]

    def advance(until):
        while passed[0] < len(events) and events[passed[0]][0] <= until:
            _, kind, g, h = events[passed[0]]
            if kind == "own":
                own(g)
            elif kind == "hop":
                gather.hop(g, h)
            else:
                gather.hop_cross(g, h)
            passed[0] += 1

    def ready(g_from, g_to):
        advance(max(e[0] for e in events if e[1] == "cross" and e[2] < g_to))
        for g in range(g_from, g_to):
            gather.finish(g)

    send_n1 = Pair(p, 0, r.n1, r.n1c, r.psem)
    send_da = Pair(p, 1, r.da, r.dac, r.psem)
    send_dy = Pair(p, 2, r.dy, r.dyc, r.psem)
    send_hid = Pair(p, 3, r.hid, r.hidx, r.psem)
    send_mix = Pair(p, 4, r.mix, r.mixx, r.psem)
    send_dqkv = Pair(p, 5, r.dqkv, r.dqkvx, r.psem)
    send_n2 = Columns(p, 0, r.n2, r.n2c, r.csem)
    fh = r.dgx.shape[1]
    send_dg = Halves(p, 0, r.dg, r.dgx, ffp - fh, r.hsem)
    send_du = Halves(p, 1, r.du, r.dux, ffp - fh, r.hsem)
    ysend, yrecv = r.ysend, r.yrecv

    def y_copy(i, ch):
        return remote(ysend.at[i, ch], yrecv.at[i, ch], r.ysem[0].at[i, ch], r.ysem[1].at[i, ch], tp=1 - p.t)

    def y_put(i, ch, value):
        ysend[i, ch] = value.astype(BF16)
        y_copy(i, ch).start()

    def y_wait(i, between=()):
        for ch in range(blocks):
            y_copy(i, ch).wait_recv()
            if ch < len(between):
                between[ch]()

    def y_rows(i, rs):
        if i == 1:
            parts = [(s, slice(cc * 128, cc * 128 + 128)) for cc in range(2) for s in range(n)]
            return jnp.concatenate(
                [ysend[1, s, rs, at].astype(F32) + yrecv[1, s, rs, at].astype(F32) for s, at in parts], axis=1
            )
        return jnp.concatenate(
            [ysend[i, ch, rs, :].astype(F32) + yrecv[i, ch, rs, :].astype(F32) for ch in range(blocks)], axis=1
        )

    step_rows = 32
    row_steps = rows_here // step_rows

    def per_rows(body):
        @pl.loop(0, row_steps)
        def _(i):
            body(pl.ds(pl.multiple_of(i * step_rows, step_rows), step_rows))

    def x_rows(rs):
        return jnp.concatenate([r.xv[rs, o : o + 128] for o in order], axis=1).astype(F32)

    def rsq(v):
        return lax.rsqrt(jnp.mean(v * v, axis=1, keepdims=True) + EPSILON)

    get_x.wait()

    def norm_one(rs):
        v = x_rows(rs)
        r.n1[rs, :] = (v * rsq(v) * r.gain[0:1, :]).astype(BF16)

    per_rows(norm_one)
    ready(0, 1)
    kv = r.kv
    first_chunk = mm(r.n1[...], fqkv[:, 0 : 2 * qk])
    r.q[...] = first_chunk[:, 0:qk].astype(BF16)
    kv[b, :, 0:qk] = first_chunk[:, qk : 2 * qk].astype(BF16)
    for ch in range(vw // 256):
        lo = ch * 256
        kv[b, :, qk + lo : qk + lo + 256] = mm(r.n1[...], fqkv[:, 2 * qk + lo : 2 * qk + lo + 256]).astype(BF16)

    kvs, kvr = r.kvsem

    def kv_copy(slot, which, peer):
        return remote(kv.at[slot], kv.at[slot], kvs.at[which], kvr.at[slot], ctx=peer)

    @pl.when(x == 0)
    def _():
        kv_copy(b, 0, p.xp).start()

    @pl.when(c == 0)
    def _():
        kv_copy(b, 1, p.ic).start()

    for i, peer in enumerate((p.ic, p.xp, p.dg)):
        remote(r.segrow, r.segall.at[peer], segs.at[i], segr.at[peer], ctx=peer).wait_recv()
    mask, num, den = r.mask, r.num, r.den
    num[...] = jnp.zeros_like(num)
    den[...] = jnp.zeros_like(den)
    lane = lax.broadcasted_iota(jnp.int32, (1, 128), 1)

    def q_of(h):
        keep = (lane // FEAT) == h
        return jnp.where(keep, r.q[...], jnp.zeros((), BF16))

    def attend_block(j):
        same = r.segcol[:, 0:1] == r.segall[j, 0:1, :]
        ri = lax.broadcasted_iota(jnp.int32, (rows_here, rows_here), 0)
        ci = lax.broadcasted_iota(jnp.int32, (rows_here, rows_here), 1)
        reach = ri + jnp.where(j == b, 0, rows_here) >= ci
        mask[j] = jnp.where(same & reach, 1.0, 0.0)

        @pl.loop(0, heads // 2)
        def _(pair):
            at = pl.ds(at128(pair * 128), 128)
            vpair = kv[j, :, pl.ds(at128(qk + pair * 128), 128)]
            sums = []
            for e in range(2):
                s = mm_nt(q_of(pair * 2 + e), kv[j, :, 0:qk]) * 0.25
                w = (1.0 + s + 0.5 * s * s) * mask[j]
                sums.append((mm(w.astype(BF16), vpair), jnp.sum(w, axis=1, keepdims=True)))
            low_half = lane < HEAD_V
            num[:, at] += jnp.where(low_half, sums[0][0], sums[1][0])
            den[:, at] += jnp.where(low_half, sums[0][1], sums[1][1])

    attend_block(b)
    advance(3.3)

    @pl.when(x == 1)
    def _():
        kv_copy(c, 2, p.ic).wait_recv()
        kv_copy(c, 2, p.ic).start()

    @pl.when(c == 1)
    def _():
        kv_copy(p.ic, 1, p.ic).wait_recv()

    @pl.when(x == 1)
    def _():
        kv_copy(1 - c, 2, p.ic).wait_recv()

    for m in range(1, 4):

        @pl.when(b >= m)
        def _():
            attend_block(b - m)

        advance(3.3 + 0.3 * m)

    inv = 1.0 / den[...]
    den[...] = inv
    num[...] = num[...] * inv
    r.mix[...] = num[...].astype(BF16)

    ready(1, 2)
    for ch in range(blocks):
        y_put(0, ch, mm(r.mix[...], fo[:, ch * 256 : ch * 256 + 256]))
    send_mix.start()
    send_n1.start()
    advance(4.5)
    y_wait(0, [lambda u=u: advance(u) for u in (5.0, 5.7, 6.3)])

    def norm_two(rs):
        v = x_rows(rs) + y_rows(0, rs)
        r.mid[rs, :] = v
        r.n2[rs, :] = (v * rsq(v) * r.gain[1:2, :]).astype(BF16)

    per_rows(norm_two)

    red = Reduce(
        p,
        [r.part[i] for i in range(5)],
        [r.seen[i] for i in range(5)],
        [r.out_d, r.out_g, r.out_u, r.out_o, r.out_q],
        [r.other, None, None, None, None],
        r.rsem,
    )
    turned = r.turned

    def turn(src):
        w = src.shape[1]

        @pl.loop(0, src.shape[0] // rows_here)
        def _(i):
            at = pl.ds(pl.multiple_of(i * rows_here, rows_here), rows_here)
            turned[0:w, at] = jnp.transpose(src[at, :])

    def grad_cols(g, rhs):
        rows = r.part[g].shape[1]

        @pl.loop(0, -(-rows // 256))
        def _(i):
            at = pl.ds(at128(jnp.minimum(i * 256, rows - 256)), 256)
            res = mm(turned[at, 0 : rhs.shape[0]], rhs[...]).astype(BF16)
            for s in range(n):
                r.part[g][s, at, :] = res[:, s * 128 : s * 128 + 128]

    fchunks = -(-ffp // 256)

    def per_ff(body):
        @pl.loop(0, fchunks)
        def _(i):
            body(at128(jnp.minimum(i * 256, ffp - 256)))

    ready(2, 6)

    def wide(ref, off):
        return ref[pl.ds(off, 256), :]

    def forward_ff(off):
        g = mm_nt(r.n2[...], wide(fg, off))
        u = mm_nt(r.n2[...], wide(fu, off))
        r.g[:, pl.ds(off, 256)] = g
        r.u[:, pl.ds(off, 256)] = u
        sig = 1.0 / (1.0 + jnp.exp(-g))
        r.hid[:, pl.ds(off, 256)] = (g * sig * u).astype(BF16)

    per_ff(forward_ff)
    send_hid.start()

    def down_block(s):
        for cc in range(2):
            cols = pl.ds(at128((cc * n + s) * 128), 128)
            ysend[1, s, :, cc * 128 : cc * 128 + 128] = mm(r.hid[...], fd[:, cols]).astype(BF16)
        y_copy(1, s).start()

    advance(ng - 1)
    down_block(z)
    for h in range(1, n):
        advance(ng - 1 + 0.6 * h + 0.81)
        for s, there in ((z + h, z + h < n), (z - h, z - h >= 0)):

            @pl.when(there)
            def _():
                for g in range(6, ng):
                    gather.whole(g, s)
                down_block(s)

    advance(2 * ng)
    send_n2.start()
    get_teacher.wait()
    small = r.small
    small[...] = jnp.zeros_like(small)
    send_hid.wait()
    turn(r.hidx)
    y_wait(1)

    def finish_forward(rs):
        y = r.mid[rs, :] + y_rows(1, rs)
        t = jnp.concatenate([r.tv[rs, o : o + 128] for o in order], axis=1).astype(F32)
        m = (y - t) * r.valid[rs, 0:1]
        r.mis[rs, :] = m
        r.dy[rs, :] = m.astype(BF16)
        yb = y.astype(BF16)
        for i, o in enumerate(order):
            r.layer_out[rs, o : o + 128] = yb[:, i * 128 : i * 128 + 128]
        small[2:3, :] += jnp.sum(m * m, axis=0, keepdims=True)
        small[3:4, :] += jnp.broadcast_to(jnp.sum(r.valid[rs, :], axis=0, keepdims=True)[:, 0:1], (1, width))

    per_rows(finish_forward)
    send_dy.start()

    def backward_ff(off):
        dh = mm_nt(r.dy[...], fd[pl.ds(off, 256), :])
        g = r.g[:, pl.ds(off, 256)]
        u = r.u[:, pl.ds(off, 256)]
        sig = 1.0 / (1.0 + jnp.exp(-g))
        r.dg[:, pl.ds(off, 256)] = (dh * u * sig * (1.0 + g * (1.0 - sig))).astype(BF16)
        r.du[:, pl.ds(off, 256)] = (dh * g * sig).astype(BF16)

    per_ff(backward_ff)
    send_dg.start()
    send_du.start()
    send_dy.wait()
    grad_cols(0, r.dyc)
    red.stage(0, 0)
    for ch in range(blocks):
        cols = slice(ch * 256, ch * 256 + 256)
        y_put(2, ch, mm(r.dg[...], fg[:, cols]) + mm(r.du[...], fu[:, cols]))

    send_dg.relay()

    y_wait(2)

    def norm_back(i, row, v, base, rs):
        dn = y_rows(i, rs)
        inv_root = rsq(v)
        w = dn * r.gain[row : row + 1, :]
        small[row : row + 1, :] += jnp.sum(dn * v * inv_root, axis=0, keepdims=True)
        m = jnp.mean(w * v, axis=1, keepdims=True)
        return base + inv_root * w - v * (inv_root * inv_root * inv_root * m)

    def middle_back(rs):
        d = norm_back(2, 1, r.mid[rs, :], r.mis[rs, :], rs)
        r.mis[rs, :] = d
        r.da[rs, :] = d.astype(BF16)

    per_rows(middle_back)
    send_da.start()
    send_n2.wait()
    send_dg.wait()
    turn(r.dgx)
    grad_cols(1, r.n2c)
    red.stage(1, 0)

    dnum, dden = r.dnum, r.dden
    for ch in range(vw // 256):
        at = slice(ch * 256, ch * 256 + 256)
        d = mm_nt(r.da[...], fo[at, :]) * den[:, at]
        dnum[:, at] = d.astype(BF16)
        dden[:, at] = d * num[:, at]
    send_du.relay()
    send_da.wait()
    send_mix.wait()
    turn(r.mixx)

    def out_half(dst, xx):
        rows = vw // 2
        res = mm(turned[pl.ds(pl.multiple_of(xx * rows, 128), rows), 0 : 2 * rows_here], r.dac[...]).astype(BF16)
        for s in range(n):
            dst[s] = res[:, s * 128 : s * 128 + 128]

    def halve(i, g, make):
        give, got = r.give[i], r.got[i]
        make(give, 1 - x)
        half_copy(i).start()
        make(r.part[g], x)

    def half_copy(i):
        return remote(r.give[i], r.got[i], r.presem[0].at[i], r.presem[1].at[i], ctx=p.xp)

    def joined(i, g):
        half_copy(i).wait_recv()
        for s in range(n):
            r.part[g][s] = (r.part[g][s].astype(F32) + r.got[i][s].astype(F32)).astype(BF16)

    halve(0, 3, out_half)
    send_du.wait()
    turn(r.dux)
    grad_cols(2, r.n2c)
    red.stage(2, 0)
    dkvp, dkv, dq = r.dkvp, r.dkv, r.dqf
    dq[...] = jnp.zeros_like(dq)

    def back_block(j):
        dkv[...] = jnp.zeros_like(dkv)

        @pl.loop(0, heads // 2)
        def _(pair):
            at = pl.ds(at128(pair * 128), 128)
            vat = pl.ds(at128(qk + pair * 128), 128)
            dv = []
            for e in range(2):
                h = pair * 2 + e
                qh = q_of(h)
                keep_v = (lane // HEAD_V) == e
                keep_q = (lane // FEAT) == h
                s = mm_nt(qh, kv[j, :, 0:qk]) * 0.25
                w = ((1.0 + s + 0.5 * s * s) * mask[j]).astype(BF16)
                dn = jnp.where(keep_v, dnum[:, at], jnp.zeros((), BF16))
                dd = jnp.sum(jnp.where(keep_v, dden[:, at], 0.0), axis=1, keepdims=True)
                dw = mm_nt(dn, kv[j, :, vat]) - dd
                ds = (dw * (1.0 + s) * (0.25 * mask[j])).astype(BF16)
                dv.append(mm_tn(w, dn))
                kh = jnp.where(keep_q, kv[j, :, 0:qk], jnp.zeros((), BF16))
                dq[...] += mm(ds, kh)
                dkv[:, 0:qk] += mm_tn(ds, qh)
            dkv[:, vat] = dv[0] + dv[1]

    @pl.loop(0, b)
    def _(j):
        back_block(j)
        dkvp[j] = dkv[...].astype(BF16)

    red.stage(0, 1)
    dks, dkr = r.dksem
    back = r.back

    def dk_copy(src, slot, which, peer):
        return remote(src, back.at[slot], dks.at[which], dkr.at[slot], ctx=peer)

    @pl.when(c == 1)
    def _():
        dk_copy(dkvp.at[p.ic], 0, 0, p.ic).start()

    @pl.when(x == 1)
    def _():
        dk_copy(dkvp.at[1 - c], 1, 1, p.ic).start()

    @pl.when(x == 1)
    def _():
        dk_copy(dkvp.at[1 - c], 1, 1, p.ic).wait_recv()
        dkvp[b] = (dkvp[c].astype(F32) + back[1].astype(F32)).astype(BF16)
        dk_copy(dkvp.at[b], 2, 2, p.xp).start()

    back_block(b)

    @pl.when(c == 0)
    def _():
        dk_copy(dkvp.at[b], 0, 0, p.ic).wait_recv()
        dkv[...] += back[0].astype(F32)

    dqkv = r.dqkv
    dqkv[:, 0:qk] = dq[...].astype(BF16)
    joined(0, 3)
    red.stage(3, 0)
    red.stage(1, 1)

    @pl.when(x == 0)
    def _():
        dk_copy(dkvp.at[b], 2, 2, p.xp).wait_recv()
        dkv[...] += back[2].astype(F32)

    dqkv[:, qk : 2 * qk + vw] = dkv[...].astype(BF16)
    send_dqkv.start()
    for ch in range(blocks):
        y_put(3, ch, mm_nt(dqkv[...], fqkv[ch * 256 : ch * 256 + 256, :]))
    send_n1.wait()
    turn(r.n1c)
    send_dqkv.wait()

    def qkv_half(dst, xx):
        cols = (2 * qk + vw) // 2
        rhs = r.dqkvx[:, pl.ds(at128(xx * cols), cols)]
        res = mm(turned[0:half_d, 0 : 2 * rows_here], rhs).astype(BF16)
        for s in range(n):
            dst[s] = res[s * 128 : s * 128 + 128, :]

    halve(1, 4, qkv_half)
    red.stage(0, 2)
    joined(1, 4)
    red.stage(4, 0)
    red.stage(2, 1)
    red.last(0)

    y_wait(3)

    def input_back(rs):
        d = norm_back(3, 0, x_rows(rs), r.mis[rs, :], rs).astype(BF16)
        for i, o in enumerate(order):
            r.grad_in[rs, o : o + 128] = d[:, i * 128 : i * 128 + 128]

    per_rows(input_back)

    sms, smr = r.smsem
    parts, lines = r.smctx, r.smz
    for i, peer in enumerate((p.ic, p.xp, p.dg)):
        remote(small, parts.at[b], sms.at[0, i], smr.at[0, b], ctx=peer).start()
    parts[b] = small[...]
    red.stage(3, 1)
    red.stage(1, 2)
    for i, peer in enumerate((p.ic, p.xp, p.dg)):
        remote(small, parts.at[peer], sms.at[0, i], smr.at[0, peer], ctx=peer).wait_recv()
    lines[n] = parts[0] + parts[1] + parts[2] + parts[3]
    for s in range(n):

        @pl.when(z != s)
        def _():
            remote(lines.at[n], lines.at[z], sms.at[1, s], smr.at[1, z], fsdp=s).start()

    red.last(1)
    red.stage(4, 1)
    red.stage(2, 2)
    red.last(2)
    red.relay(0)
    red.stage(3, 2)
    red.last(3)
    red.stage(4, 2)
    red.relay(1)
    red.last(4)
    for s in range(n):

        @pl.when(z != s)
        def _():
            remote(lines.at[n], lines.at[s], sms.at[1, s], smr.at[1, s], fsdp=s).wait_recv()

    total = jnp.zeros_like(small)
    for s in range(n):
        total += jnp.where(z == s, lines[n], lines[s])
    r.gain[...] = total
    for cc in range(2):
        at = pl.ds(at128((cc * n + z) * 128), 128)
        r.grad_attn[0:1, cc * 128 : cc * 128 + 128] = r.gain[0:1, at]
        r.grad_ffn[0:1, cc * 128 : cc * 128 + 128] = r.gain[1:2, at]
    r.loss[...] = jnp.sum(total[2:3, :], axis=1, keepdims=True) / (total[3:4, 0:1] * width)
    red.relay(2)
    red.relay(3)
    red.relay(4)
    for g in (4, 0, 1, 2, 3):
        red.finish(g)
        if g == 4:
            r.grad_q[...] = r.out_q[:, 0:qk].astype(F32)
            r.grad_k[...] = r.out_q[:, qk : 2 * qk].astype(F32)
            r.grad_v[...] = r.out_q[:, 2 * qk : 2 * qk + vw].astype(F32)

    for i in range(2):
        half_copy(i).wait_send()
    gather.drain()
    for k in (send_n1, send_da, send_n2, send_dy, send_hid, send_dg, send_du, send_mix, send_dqkv):
        k.drain()
    for i in range(4):
        for ch in range(blocks):
            y_copy(i, ch).wait_send()
    for s in range(n):

        @pl.when(z != s)
        def _():
            remote(r.gains, gath.at[z], gsend.at[s], grecv.at[z], fsdp=s).wait_send()
            remote(lines.at[n], lines.at[z], sms.at[1, s], smr.at[1, z], fsdp=s).wait_send()

    for i, peer in enumerate((p.ic, p.xp, p.dg)):
        remote(r.segrow, r.segall.at[b], segs.at[i], segr.at[b], ctx=peer).wait_send()
        remote(small, parts.at[b], sms.at[0, i], smr.at[0, b], ctx=peer).wait_send()

    @pl.when(x == 0)
    def _():
        kv_copy(b, 0, p.xp).wait_send()

    @pl.when(c == 0)
    def _():
        kv_copy(b, 1, p.ic).wait_send()

    @pl.when(x == 1)
    def _():
        kv_copy(c, 2, p.ic).wait_send()
        dk_copy(dkvp.at[1 - c], 1, 1, p.ic).wait_send()
        dk_copy(dkvp.at[b], 2, 2, p.xp).wait_send()

    @pl.when(c == 1)
    def _():
        dk_copy(dkvp.at[p.ic], 0, 0, p.ic).wait_send()


def mega(n, layer_in, segment_ids, valid_mask, teacher, attn_gain, w_query, w_key, w_value, w_out, ffn_gain, w_gate, w_up, w_down):
    x = layer_in[0]
    rows, width = x.shape
    qk, vw, ff = w_query.shape[1], w_value.shape[1], w_gate.shape[1]
    ffp = up_to(ff, 128)
    fh = up_to(ffp // 2, 256)
    half_d = width // 2
    blocks = width // 256
    inputs = dict(
        x=x,
        teacher=teacher[0],
        wq=w_query,
        wk=w_key,
        wv=w_value,
        wo=w_out,
        wg=w_gate.T,
        wu=w_up.T,
        wd=w_down,
        attn_gain=attn_gain,
        ffn_gain=ffn_gain,
        segment=segment_ids,
        real=valid_mask,
    )
    hbm = list(inputs)[:9]
    outs = dict(
        layer_out=((rows, width), BF16),
        grad_in=((rows, width), BF16),
        out_d=((ffp, width // n), BF16),
        out_g=((ffp, width // n), BF16),
        out_u=((ffp, width // n), BF16),
        out_o=((vw, width // n), BF16),
        grad_q=((width // n, qk), F32),
        grad_k=((width // n, qk), F32),
        grad_v=((width // n, vw), F32),
        grad_attn=((1, width // n), F32),
        grad_ffn=((1, width // n), F32),
        loss=((1, 1), F32),
    )
    dma = pltpu.SemaphoreType.DMA
    ng = 8
    vm = pltpu.VMEM
    piece = [(ffp, 128), (fh, 128), (fh, 128), (vw // 2, 128), (128, (2 * qk + vw) // 2)]
    scratch = dict(
        lsem=dma((20,)),
        gs=[dma((ng, n)) for _ in range(9)],
        gnsem=[dma((n,)), dma((n,))],
        segsem=[dma((3,)), dma((4,))],
        psem=[dma((6,)), dma((6,))],
        csem=[dma((1, 3)), dma((1, 4))],
        hsem=[dma((2, 3)), dma((2, 4))],
        ysem=[dma((4, blocks)), dma((4, blocks))],
        kvsem=[dma((3,)), dma((4,))],
        dksem=[dma((3,)), dma((3,))],
        rsem=[dma((5, n)), dma((5, n + 1)), dma((5, 3)), dma((5, 4))],
        smsem=[dma((2, max(n, 3))), dma((2, max(n, 4)))],
        fqkv=vm((width, 2 * qk + vw), BF16),
        fo=vm((vw, width), BF16),
        fg=vm((ffp, width), BF16),
        fu=vm((ffp, width), BF16),
        fd=vm((ffp, width), BF16),
        xv=vm((rows, width), BF16),
        tv=vm((rows, width), BF16),
        gath=vm((n, 8, width // n), F32),
        gain=vm((8, width), F32),
        gains=vm((8, width // n), F32),
        segrow=vm((8, rows), F32),
        segcol=vm((rows, 128), F32),
        valid=vm((rows, 128), F32),
        segall=vm((4, 8, rows), F32),
        n1=vm((rows, width), BF16),
        n2=vm((rows, width), BF16),
        dy=vm((rows, width), BF16),
        da=vm((rows, width), BF16),
        n1c=vm((2 * rows, half_d), BF16),
        n2c=vm((4 * rows, half_d), BF16),
        dyc=vm((2 * rows, half_d), BF16),
        dac=vm((2 * rows, half_d), BF16),
        hid=vm((rows, ffp), BF16),
        dg=vm((rows, ffp), BF16),
        du=vm((rows, ffp), BF16),
        mix=vm((rows, vw), BF16),
        dqkv=vm((rows, 2 * qk + vw), BF16),
        hidx=vm((2 * rows, ffp), BF16),
        dgx=vm((4 * rows, fh), BF16),
        dux=vm((4 * rows, fh), BF16),
        mixx=vm((2 * rows, vw), BF16),
        dqkvx=vm((2 * rows, 2 * qk + vw), BF16),
        ysend=vm((4, max(blocks, n), rows, 256), BF16),
        yrecv=vm((4, blocks, rows, 256), BF16),
        q=vm((rows, qk), BF16),
        kv=vm((4, rows, qk + vw), BF16),
        mask=vm((4, rows, rows), F32),
        num=vm((rows, vw), F32),
        den=vm((rows, vw), F32),
        mid=vm((rows, width), F32),
        mis=vm((rows, width), F32),
        g=vm((rows, ffp), F32),
        u=vm((rows, ffp), F32),
        small=vm((8, width), F32),
        smctx=vm((4, 8, width), F32),
        smz=vm((n + 1, 8, width), F32),
        dnum=vm((rows, vw), BF16),
        dden=vm((rows, vw), F32),
        dqf=vm((rows, qk), F32),
        dkv=vm((rows, qk + vw), F32),
        dkvp=vm((4, rows, qk + vw), BF16),
        back=vm((3, rows, qk + vw), BF16),
        turned=vm((max(ffp, half_d), 4 * rows), BF16),
        part=[vm((n,) + s, BF16) for s in piece],
        seen=[vm((n + 1,) + s, BF16) for s in piece],
        other=vm(piece[0], BF16),
        give=[vm((n,) + piece[i], BF16) for i in (3, 4)],
        got=[vm((n,) + piece[i], BF16) for i in (3, 4)],
        presem=[dma((2,)), dma((2,))],
        out_q=vm((width // n, 2 * qk + vw), BF16),
    )
    flat, layout = [], []
    for k, v in scratch.items():
        if isinstance(v, list):
            layout.append((k, len(v)))
            flat.extend(v)
        else:
            layout.append((k, 0))
            flat.append(v)

    def kernel(*refs):
        names = list(inputs) + list(outs)
        bound = list(refs[: len(names)])
        at = len(names)
        for k, count in layout:
            names.append(k)
            if count:
                bound.append(refs[at : at + count])
                at += count
            else:
                bound.append(refs[at])
                at += 1
        mega_kernel(n, names, *bound)

    res = pl.pallas_call(
        kernel,
        out_shape=[jax.ShapeDtypeStruct(*v) for v in outs.values()],
        in_specs=[pl.BlockSpec(memory_space=pl.ANY if k in hbm else pltpu.VMEM) for k in inputs],
        out_specs=[pl.BlockSpec(memory_space=pltpu.VMEM)] * len(outs),
        scratch_shapes=flat,
        compiler_params=pltpu.CompilerParams(
            collective_id=0, has_side_effects=True, vmem_limit_bytes=67043328
        ),
        name="block_step",
    )(*inputs.values())
    o = SimpleNamespace(**dict(zip(outs, res)))

    return (
        o.layer_out[None],
        o.grad_in[None],
        o.grad_attn[0],
        o.grad_q,
        o.grad_k,
        o.grad_v,
        o.out_o.astype(F32),
        o.grad_ffn[0],
        o.out_g[:ff].astype(F32).T,
        o.out_u[:ff].astype(F32).T,
        o.out_d[:ff].astype(F32),
        o.loss[0, 0],
    )


def per_device(*arrays):
    n = lax.axis_size("fsdp")
    layer_in, w_query, w_value = arrays[0], arrays[5], arrays[7]
    fits = (
        lax.axis_size("ctx") == 4
        and lax.axis_size("tp") == 2
        and layer_in.shape[0] == 1
        and w_query.shape[0] == 256
        and w_query.shape[1] == 128
        and w_value.shape[1] % 512 == 0
        and layer_in.shape[1] % 256 == 0
    )
    return mega(n, *arrays) if fits else general(*arrays)


def solution(mesh):
    placed = (
        P("fsdp", "ctx", None),
        P("fsdp", "ctx"),
        P("fsdp", "ctx"),
        P("fsdp", "ctx", None),
        P("fsdp"),
        P("fsdp", "tp"),
        P("fsdp", "tp"),
        P("fsdp", "tp"),
        P("tp", "fsdp"),
        P("fsdp"),
        P("fsdp", "tp"),
        P("fsdp", "tp"),
        P("tp", "fsdp"),
    )
    return jax.shard_map(
        per_device,
        mesh=mesh,
        in_specs=placed,
        out_specs=(
            P("fsdp", "ctx", None),
            P("fsdp", "ctx", None),
            P("fsdp"),
            P("fsdp", "tp"),
            P("fsdp", "tp"),
            P("fsdp", "tp"),
            P("tp", "fsdp"),
            P("fsdp"),
            P("fsdp", "tp"),
            P("fsdp", "tp"),
            P("tp", "fsdp"),
            P(),
        ),
        check_vma=False,
    )
```

```python
from functools import partial
from types import SimpleNamespace
import math

import jax
import jax.numpy as jnp
from jax import lax
from jax.experimental import pallas as pl
from jax.experimental.pallas import tpu as pltpu
from jax.sharding import PartitionSpec as P

FEAT = 16
HEAD_V = 64


EPSILON = 1e-05
HIGH = lax.Precision.HIGHEST
QUAD_SCALE = 1.0 / (4.0 * math.sqrt(2.0))


def entering(x, axis, join, neutral):
    place = lax.axis_index(axis)
    gathered = jax.tree.map(
        lambda a, kind: lax.all_gather(a.astype(kind), axis),
        x,
        (jnp.bfloat16, jnp.bfloat16, jnp.bfloat16),
    )
    state = jax.tree.map(lambda a, e: jnp.zeros_like(a) + jnp.asarray(e, a.dtype), x, neutral)

    def one(lap, state):
        return join(
            state,
            jax.tree.map(
                lambda a, own: lax.dynamic_index_in_dim(a, lap, 0, False).astype(own.dtype),
                gathered,
                x,
            ),
        )

    return lax.fori_loop(0, place, one, state)


def entering_2(x, axis, combine, identity):
    devices, here = (lax.axis_size(axis), lax.axis_index(axis))
    everything = jax.tree.map(
        lambda part, kind: lax.all_gather(part.astype(kind), axis),
        x,
        jax.tree.map(lambda a: jnp.bfloat16 if a.dtype == jnp.float32 else a.dtype, x),
    )
    start = jax.tree.map(
        lambda part, zero: jnp.broadcast_to(jnp.asarray(zero, part.dtype), part.shape), x, identity
    )

    def lap(k, before):
        at = devices - 1 - k
        reached = at > here
        new = combine(
            before, jax.tree.map(lambda part, own: part[at].astype(own.dtype), everything, x)
        )
        return jax.tree.map(lambda a, b: jnp.where(reached, a, b), new, before)

    return lax.fori_loop(0, devices, lap, start)


def product(left_side, right_side):
    return jnp.dot(left_side, right_side, preferred_element_type=jnp.float32)


def product_left_t(left_side, right_side):
    return lax.dot_general(
        left_side, right_side, (((0,), (0,)), ((), ())), preferred_element_type=jnp.float32
    )


def product_right_t(left_side, right_side):
    return lax.dot_general(
        left_side, right_side, (((1,), (1,)), ((), ())), preferred_element_type=jnp.float32
    )


def features(vectors):
    lead_dims = vectors.shape[:-1]
    feat_width = vectors.shape[-1]
    square = (vectors[..., :, None] * vectors[..., None, :]).reshape(
        lead_dims + (feat_width * feat_width,)
    )
    return jnp.concatenate(
        [jnp.ones(lead_dims + (1,), jnp.float32), 0.5 * vectors, QUAD_SCALE * square], axis=-1
    )


def attend(query_rows, key_rows, value_rows, prev_state, prev_norm, segment, prev_id):
    scores = jnp.einsum("slhf,smhf->shlm", query_rows, key_rows, precision=HIGH) * 0.25
    kernel = 1.0 + scores + 0.5 * scores * scores
    places = jnp.arange(segment.shape[1])
    allowed = (places[:, None] >= places[None, :])[None] & (
        segment[:, :, None] == segment[:, None, :]
    )
    kernel = jnp.where(allowed[:, None], kernel, 0.0)
    carried = (segment.astype(jnp.float32) == prev_id[:, None]).astype(jnp.float32)
    mapped = features(query_rows) * carried[:, :, None, None]
    numerator = jnp.einsum("shlm,smhv->slhv", kernel, value_rows, precision=HIGH) + jnp.einsum(
        "slht,shtv->slhv", mapped, prev_state, precision=HIGH
    )
    denominator = jnp.einsum("shlm->slh", kernel) + jnp.einsum(
        "slht,sht->slh", mapped, prev_norm, precision=HIGH
    )
    return numerator / denominator[..., None]


def summarize(key_rows, value_rows, segment):
    closing = (segment == segment[:, -1:]).astype(jnp.float32)
    mapped = features(key_rows) * closing[:, :, None, None]
    return (
        jnp.einsum("slht,slhv->shtv", mapped, value_rows, precision=HIGH),
        jnp.sum(mapped, axis=1),
    )


def rms_forward(values_in, gain_vec):
    inv_root = lax.rsqrt(jnp.mean(values_in * values_in, axis=-1, keepdims=True) + EPSILON)
    return (values_in * inv_root * gain_vec, inv_root)


def rms_backward(values_in, inv_root, gain_vec, grad_normed):
    weighted = grad_normed * gain_vec
    grad_gain = jnp.sum(grad_normed * values_in * inv_root, axis=0)
    grad_values = inv_root * weighted - values_in * inv_root**3 * jnp.mean(
        weighted * values_in, axis=-1, keepdims=True
    )
    return (grad_values, grad_gain)


def chain_combine(earlier, later):
    is_fresh = later[0] < 0
    same_doc = later[0] == earlier[0]

    def pick(early_part, late_part):
        expand = (-1,) + (1,) * (early_part.ndim - 1)
        with_early = late_part + jnp.where(same_doc.reshape(expand), early_part, 0.0)
        return jnp.where(is_fresh.reshape(expand), early_part, with_early)

    return (
        jnp.where(is_fresh, earlier[0], later[0]),
        pick(earlier[1], later[1]),
        pick(earlier[2], later[2]),
    )


def tp_forward(partial_sum):
    return lax.psum(partial_sum, "tp")


def tp_backward(partial_sum):
    return lax.psum(partial_sum.astype(jnp.bfloat16), "tp").astype(jnp.float32)


def general(
    layer_in,
    segment_ids,
    valid_mask,
    teacher,
    attn_gain,
    w_query,
    w_key,
    w_value,
    w_out,
    ffn_gain,
    w_gate,
    w_up,
    w_down,
):
    full_weights = (
        lax.all_gather(attn_gain, "fsdp", axis=0, tiled=True),
        lax.all_gather(w_query, "fsdp", axis=0, tiled=True),
        lax.all_gather(w_key, "fsdp", axis=0, tiled=True),
        lax.all_gather(w_value, "fsdp", axis=0, tiled=True),
        lax.all_gather(w_out, "fsdp", axis=1, tiled=True),
        lax.all_gather(ffn_gain, "fsdp", axis=0, tiled=True),
        lax.all_gather(w_gate, "fsdp", axis=0, tiled=True),
        lax.all_gather(w_up, "fsdp", axis=0, tiled=True),
        lax.all_gather(w_down, "fsdp", axis=1, tiled=True),
    )
    (
        gain_one,
        full_query,
        full_key,
        full_value,
        full_out,
        gain_two,
        full_gate,
        full_up,
        full_down,
    ) = full_weights
    seq_count, shard_len, model_width = layer_in.shape
    row_count = seq_count * shard_len
    heads_here = full_query.shape[1] // FEAT
    rows_in = layer_in.reshape(row_count, model_width).astype(jnp.float32)
    normed_full, root_one = rms_forward(rows_in, gain_one.astype(jnp.float32))
    normed_one = normed_full.astype(jnp.bfloat16)
    query_rows = product(normed_one, full_query).reshape(seq_count, shard_len, heads_here, FEAT)
    key_rows = product(normed_one, full_key).reshape(seq_count, shard_len, heads_here, FEAT)
    value_rows = product(normed_one, full_value).reshape(seq_count, shard_len, heads_here, HEAD_V)
    last_id = segment_ids[:, -1].astype(jnp.float32)
    first_id = segment_ids[:, 0].astype(jnp.float32)
    (out_state, out_norm), summary_pull = jax.vjp(
        partial(summarize, segment=segment_ids), key_rows, value_rows
    )
    blank_state = jnp.zeros_like(out_state)
    blank_norm = jnp.zeros_like(out_norm)
    no_doc = jnp.full_like(last_id, -1.0)
    prev_id, prev_state, prev_norm = entering(
        (last_id, out_state, out_norm), "ctx", chain_combine, (no_doc, blank_state, blank_norm)
    )
    attended, attend_pull = jax.vjp(
        partial(attend, segment=segment_ids, prev_id=prev_id),
        query_rows,
        key_rows,
        value_rows,
        prev_state,
        prev_norm,
    )
    mixed_heads = attended.reshape(row_count, heads_here * HEAD_V).astype(jnp.bfloat16)
    head_sum = product(mixed_heads, full_out)
    teacher_rows = teacher.reshape(row_count, model_width).astype(jnp.float32)
    weight_rows = valid_mask.reshape(row_count, 1).astype(jnp.float32)
    middle = rows_in + tp_forward(head_sum)
    normed_mid, root_two = rms_forward(middle, gain_two.astype(jnp.float32))
    normed_two = normed_mid.astype(jnp.bfloat16)
    gate_rows = product(normed_two, full_gate)
    up_rows = product(normed_two, full_up)
    sigmoid_gate = jax.nn.sigmoid(gate_rows)
    silu_gate = gate_rows * sigmoid_gate
    hidden = (silu_gate * up_rows).astype(jnp.bfloat16)
    down_sum = product(hidden, full_down)
    output = middle + tp_forward(down_sum)
    misfit = (output - teacher_rows) * weight_rows
    layer_rows = output.astype(jnp.bfloat16)
    grad_rows = misfit.astype(jnp.bfloat16)
    sum_squares = jnp.sum(misfit * misfit)
    sum_valid = jnp.sum(weight_rows)
    grad_down = product_left_t(hidden, grad_rows)
    grad_hidden = product_right_t(grad_rows, full_down)
    grad_gate_rows = (
        grad_hidden * up_rows * sigmoid_gate * (1.0 + gate_rows * (1.0 - sigmoid_gate))
    ).astype(jnp.bfloat16)
    grad_up_rows = (grad_hidden * silu_gate).astype(jnp.bfloat16)
    grad_gate = product_left_t(normed_two, grad_gate_rows)
    grad_up = product_left_t(normed_two, grad_up_rows)
    normed_two_terms = product_right_t(grad_gate_rows, full_gate) + product_right_t(
        grad_up_rows, full_up
    )
    grad_normed_two = tp_backward(normed_two_terms)
    grad_mid_norm, grad_ffn_gain = rms_backward(
        middle, root_two, gain_two.astype(jnp.float32), grad_normed_two
    )
    grad_middle = misfit + grad_mid_norm
    grad_branch = grad_middle.astype(jnp.bfloat16)
    grad_out = product_left_t(mixed_heads, grad_branch)
    grad_mixed = product_right_t(grad_branch, full_out).reshape(
        seq_count, shard_len, heads_here, HEAD_V
    )
    grad_q_near, grad_k_near, grad_v_near, grad_prev_state, grad_prev_norm = attend_pull(grad_mixed)
    next_id, later_state, later_norm = entering_2(
        (first_id, grad_prev_state, grad_prev_norm),
        "ctx",
        chain_combine,
        (no_doc, blank_state, blank_norm),
    )
    continues = (next_id == last_id).astype(jnp.float32)
    grad_k_far, grad_v_far = summary_pull(
        (later_state * continues[:, None, None, None], later_norm * continues[:, None, None])
    )
    grad_query_rows = grad_q_near.reshape(row_count, heads_here * FEAT).astype(jnp.bfloat16)
    grad_key_rows = (
        (grad_k_near + grad_k_far).reshape(row_count, heads_here * FEAT).astype(jnp.bfloat16)
    )
    grad_value_rows = (
        (grad_v_near + grad_v_far).reshape(row_count, heads_here * HEAD_V).astype(jnp.bfloat16)
    )
    grad_query = product_left_t(normed_one, grad_query_rows)
    grad_key = product_left_t(normed_one, grad_key_rows)
    grad_value = product_left_t(normed_one, grad_value_rows)
    normed_one_terms = (
        product_right_t(grad_query_rows, full_query)
        + product_right_t(grad_key_rows, full_key)
        + product_right_t(grad_value_rows, full_value)
    )
    grad_normed_one = tp_backward(normed_one_terms)
    grad_rows_in, grad_attn_gain = rms_backward(
        rows_in, root_one, gain_one.astype(jnp.float32), grad_normed_one
    )
    grad_in_rows = (grad_middle + grad_rows_in).astype(jnp.bfloat16)
    total_sq, total_valid = lax.psum((sum_squares, sum_valid), ("fsdp", "ctx"))
    loss_value = total_sq / (total_valid * model_width)
    grad_in = grad_in_rows.reshape(seq_count, shard_len, model_width)
    layer_out = layer_rows.reshape(seq_count, shard_len, model_width)
    owned = (
        lax.psum_scatter(
            grad_attn_gain.astype(jnp.bfloat16), "fsdp", scatter_dimension=0, tiled=True
        ).astype(jnp.float32),
        lax.psum_scatter(
            grad_query.astype(jnp.bfloat16), "fsdp", scatter_dimension=0, tiled=True
        ).astype(jnp.float32),
        lax.psum_scatter(
            grad_key.astype(jnp.bfloat16), "fsdp", scatter_dimension=0, tiled=True
        ).astype(jnp.float32),
        lax.psum_scatter(
            grad_value.astype(jnp.bfloat16), "fsdp", scatter_dimension=0, tiled=True
        ).astype(jnp.float32),
        lax.psum_scatter(
            grad_out.astype(jnp.bfloat16), "fsdp", scatter_dimension=1, tiled=True
        ).astype(jnp.float32),
        lax.psum_scatter(
            grad_ffn_gain.astype(jnp.bfloat16), "fsdp", scatter_dimension=0, tiled=True
        ).astype(jnp.float32),
        lax.psum_scatter(
            grad_gate.astype(jnp.bfloat16), "fsdp", scatter_dimension=0, tiled=True
        ).astype(jnp.float32),
        lax.psum_scatter(
            grad_up.astype(jnp.bfloat16), "fsdp", scatter_dimension=0, tiled=True
        ).astype(jnp.float32),
        lax.psum_scatter(
            grad_down.astype(jnp.bfloat16), "fsdp", scatter_dimension=1, tiled=True
        ).astype(jnp.float32),
    )
    shares = (
        lax.psum(owned[0].astype(jnp.bfloat16), "ctx").astype(jnp.float32),
        lax.psum(owned[1].astype(jnp.bfloat16), "ctx").astype(jnp.float32),
        lax.psum(owned[2].astype(jnp.bfloat16), "ctx").astype(jnp.float32),
        lax.psum(owned[3].astype(jnp.bfloat16), "ctx").astype(jnp.float32),
        lax.psum(owned[4].astype(jnp.bfloat16), "ctx").astype(jnp.float32),
        lax.psum(owned[5].astype(jnp.bfloat16), "ctx").astype(jnp.float32),
        lax.psum(owned[6].astype(jnp.bfloat16), "ctx").astype(jnp.float32),
        lax.psum(owned[7].astype(jnp.bfloat16), "ctx").astype(jnp.float32),
        lax.psum(owned[8].astype(jnp.bfloat16), "ctx").astype(jnp.float32),
    )
    return (
        layer_out,
        grad_in,
        shares[0],
        shares[1],
        shares[2],
        shares[3],
        shares[4],
        shares[5],
        shares[6],
        shares[7],
        shares[8],
        loss_value,
    )


MESH = pl.DeviceIdType.MESH
F32 = jnp.float32
BF16 = jnp.bfloat16


def up_to(size, step):
    return -(-size // step) * step


def mm(a, b):
    return jnp.dot(a, b, preferred_element_type=F32)


def mm_nt(a, b):
    return lax.dot_general(a, b, (((1,), (1,)), ((), ())), preferred_element_type=F32)


def mm_tn(a, b):
    return lax.dot_general(a, b, (((0,), (0,)), ((), ())), preferred_element_type=F32)


def at128(offset):
    return pl.multiple_of(offset, 128)


class Place:
    def __init__(self, n):
        self.n = n
        self.z = lax.axis_index("fsdp")
        self.b = lax.axis_index("ctx")
        self.t = lax.axis_index("tp")
        self.x = self.b // 2
        self.c = self.b % 2
        self.ic = self.x * 2 + (1 - self.c)
        self.xp = (1 - self.x) * 2 + self.c
        self.dg = (1 - self.x) * 2 + (1 - self.c)


def remote(src, dst, send, recv, **where):
    return pltpu.make_async_remote_copy(
        src_ref=src, dst_ref=dst, send_sem=send, recv_sem=recv, device_id=where, device_id_type=MESH
    )


def entry_barrier(p):
    sem = pltpu.get_barrier_semaphore()
    for s in range(p.n):

        @pl.when(p.z != s)
        def _():
            pl.semaphore_signal(sem, inc=1, device_id={"fsdp": s}, device_id_type=MESH)

    for peer in (p.ic, p.xp, p.dg):
        pl.semaphore_signal(sem, inc=1, device_id={"ctx": peer}, device_id_type=MESH)
    pl.semaphore_signal(sem, inc=1, device_id={"tp": 1 - p.t}, device_id_type=MESH)
    pl.semaphore_wait(sem, p.n - 1 + 4)


class Gather:
    def __init__(self, p, pieces, sems):
        self.p = p
        self.pieces = pieces
        (self.zr, self.xr, self.i1r, self.i2r, self.zsl, self.zsr, self.xs, self.i1s, self.i2s) = sems

    def quarter(self, g, s, x, c):
        ref, kind, lo, size = self.pieces[g]
        n = self.p.n
        if kind == "row":
            return ref.at[pl.ds(pl.multiple_of((c * n + s) * 128 + x * 64 + lo[0], 16), size), 0 : lo[1]]
        half = lo[1]
        return ref.at[
            pl.ds(pl.multiple_of(x * half + lo[0], 16), size), pl.ds(at128((c * n + s) * 128), 128)
        ]

    def copy(self, g, s, x, c, send, recv, **where):
        ref = self.quarter(g, s, x, c)
        return remote(ref, ref, send.at[g, s], recv.at[g, s], **where)

    def left(self, g, s):
        return self.copy(g, s, self.p.x, self.p.c, self.zsl, self.zr, fsdp=self.p.z - 1)

    def right(self, g, s):
        return self.copy(g, s, self.p.x, self.p.c, self.zsr, self.zr, fsdp=self.p.z + 1)

    def chip(self, g, s, x, c, second):
        if second:
            return self.copy(g, s, x, c, self.i2s, self.i2r, ctx=self.p.ic)
        return self.copy(g, s, x, c, self.i1s, self.i1r, ctx=self.p.ic)

    def cross(self, g, s, x, c):
        return self.copy(g, s, x, c, self.xs, self.xr, ctx=self.p.xp)

    def own(self, g):
        p = self.p

        @pl.when(p.z > 0)
        def _():
            self.left(g, p.z).start()

        @pl.when(p.z < p.n - 1)
        def _():
            self.right(g, p.z).start()

    def hop(self, g, h):
        p = self.p
        for d in (1, -1):
            s = p.z + d * h
            there = (s < p.n) if d == 1 else (s >= 0)

            @pl.when(there)
            def _():
                self.copy(g, s, p.x, p.c, self.zsl, self.zr, fsdp=p.z).wait_recv()
                if d == 1:

                    @pl.when(p.z > 0)
                    def _():
                        self.left(g, s).start()

                else:

                    @pl.when(p.z < p.n - 1)
                    def _():
                        self.right(g, s).start()

                self.cross(g, s, p.x, p.c).start()
                self.chip(g, s, p.x, p.c, False).start()

    def hop_cross(self, g, h):
        p = self.p
        for d in (1, -1):
            s = p.z + d * h
            there = (s < p.n) if d == 1 else (s >= 0)

            @pl.when(there)
            def _():
                self.cross(g, s, 1 - p.x, p.c).wait_recv()
                self.chip(g, s, 1 - p.x, p.c, True).start()

    def whole(self, g, s):
        p = self.p
        self.chip(g, s, p.x, 1 - p.c, False).wait_recv()
        self.chip(g, s, 1 - p.x, 1 - p.c, True).wait_recv()

    def finish(self, g):
        p = self.p

        @pl.loop(0, p.n)
        def _(s):
            @pl.when(s != p.z)
            def _():
                self.whole(g, s)

    def drain(self):
        p = self.p
        for g in range(len(self.pieces)):

            @pl.loop(0, p.n)
            def _(s):
                @pl.when((s >= p.z) & (p.z > 0))
                def _():
                    self.left(g, s).wait_send()

                @pl.when((s <= p.z) & (p.z < p.n - 1))
                def _():
                    self.right(g, s).wait_send()

                @pl.when(s != p.z)
                def _():
                    self.cross(g, s, p.x, p.c).wait_send()
                    self.chip(g, s, p.x, p.c, False).wait_send()
                    self.chip(g, s, 1 - p.x, p.c, True).wait_send()


class Reduce:
    def __init__(self, p, parts, seen, done, other, sems):
        self.p = p
        self.parts = parts
        self.seen = seen
        self.done = done
        self.other = other
        (self.ss, self.rs, self.fs, self.fr) = sems

    def move(self, g, s, slot, to):
        return remote(
            self.parts[g].at[s], self.seen[g].at[slot], self.ss.at[g, s], self.rs.at[g, slot], fsdp=to
        )

    def arrived(self, g, slot):
        self.move(g, 0, slot, self.p.z).wait_recv()

    def by_rows(self, g, body):
        @pl.loop(0, self.parts[g].shape[1] // 128)
        def _(i):
            body(pl.ds(at128(i * 128), 128))

    def add(self, g, s, slot):
        def body(at):
            total = self.parts[g][s, at, :].astype(F32) + self.seen[g][slot, at, :].astype(F32)
            self.parts[g][s, at, :] = total.astype(BF16)

        self.by_rows(g, body)

    def stage(self, g, k):
        p = self.p
        n = p.n

        @pl.when(p.z == k)
        def _():
            for s in range(n - 1, k, -1):
                if k > 0:
                    self.arrived(g, s)
                    self.add(g, s, s)
                self.move(g, s, s, k + 1).start()

        @pl.when(p.z == n - 1 - k)
        def _():
            z = n - 1 - k
            for s in range(0, z):
                if k > 0:
                    self.arrived(g, s)
                    self.add(g, s, s)
                self.move(g, s, n if s == z - 1 else s, z - 1).start()

    def last(self, g):
        p = self.p
        n = p.n

        @pl.when(p.z > 0)
        def _():
            self.arrived(g, p.z)
            self.add(g, p.z, p.z)

        @pl.when(p.z < n - 1)
        def _():
            self.arrived(g, n)
            self.add(g, p.z, n)

        if self.other[g] is not None:
            self.across(g).start()
            return
        self.block(g, p.x, p.c)[...] = self.mine(g)[...]
        self.spread(g, p.b, 0, p.ic, self.mine(g)).start()
        self.spread(g, p.b, 1, p.xp, self.mine(g)).start()

    def mine(self, g):
        p = self.p
        if self.done[g].shape[1] != 256:
            return self.parts[g].at[p.z]
        half = self.done[g].shape[0] // 2
        skip = self.parts[g].shape[1] - half
        return self.parts[g].at[p.z, pl.ds(pl.multiple_of(p.x * skip, 16), half), :]

    def block(self, g, x, c):
        if self.done[g].shape[1] != 256:
            w = self.done[g].shape[1] // 2
            return self.done[g].at[pl.ds(at128(c * 128), 128), pl.ds(at128(x * w), w)]
        half = self.done[g].shape[0] // 2
        return self.done[g].at[pl.ds(pl.multiple_of(x * half, 16), half), pl.ds(at128(c * 128), 128)]

    def spread(self, g, slot, which, to, src=None):
        dst = self.block(g, slot // 2, slot % 2)
        return remote(dst if src is None else src, dst, self.fs.at[g, which], self.fr.at[g, slot], ctx=to)

    def side(self, g, c):
        return self.done[g].at[:, pl.ds(at128(c * 128), 128)]

    def across(self, g):
        p = self.p
        return remote(self.parts[g].at[p.z], self.other[g], self.fs.at[g, 0], self.fr.at[g, 0], ctx=p.xp)

    def beside(self, g, c):
        ref = self.side(g, c)
        return remote(ref, ref, self.fs.at[g, 1], self.fr.at[g, 1], ctx=self.p.ic)

    def relay(self, g):
        p = self.p
        if self.other[g] is not None:
            self.across(g).wait_recv()

            side = self.side(g, p.c)

            def body(at):
                total = self.parts[g][p.z, at, :].astype(F32) + self.other[g][at, :].astype(F32)
                side[at, :] = total.astype(BF16)

            self.by_rows(g, body)
            self.beside(g, p.c).start()
            return
        self.spread(g, p.xp, 1, p.xp).wait_recv()
        self.spread(g, p.xp, 2, p.ic).start()

    def finish(self, g):
        p = self.p
        if self.other[g] is not None:
            self.beside(g, 1 - p.c).wait_recv()
            self.beside(g, p.c).wait_send()
            self.across(g).wait_send()
        else:
            self.spread(g, p.ic, 0, p.ic).wait_recv()
            self.spread(g, p.dg, 2, p.ic).wait_recv()
            self.spread(g, p.b, 0, p.ic, self.mine(g)).wait_send()
            self.spread(g, p.b, 1, p.xp, self.mine(g)).wait_send()
            self.spread(g, p.xp, 2, p.ic).wait_send()

        @pl.loop(0, p.n)
        def _(s):
            @pl.when(s != p.z)
            def _():
                self.move(g, s, 0, p.z).wait_send()


class Columns:
    def __init__(self, p, k, src, dst, sems):
        self.p = p
        self.k = k
        self.src = src
        self.dst = dst
        self.send, self.recv = sems

    def slot(self, b):
        rows = self.src.shape[0]
        return self.dst.at[pl.ds(pl.multiple_of(b * rows, rows), rows), :]

    def copy(self, peer, which):
        p = self.p
        w = self.dst.shape[1]
        part = self.src.at[:, pl.ds(at128((peer % 2) * w), w)]
        return remote(part, self.slot(p.b), self.send.at[self.k, which], self.recv.at[self.k, p.b], ctx=peer)

    def start(self):
        p = self.p
        w = self.dst.shape[1]
        for which, peer in enumerate((p.xp, p.dg, p.ic)):
            self.copy(peer, which).start()
        self.slot(p.b)[...] = self.src[:, pl.ds(at128(p.c * w), w)]

    def wait(self):
        p = self.p
        for peer in (p.ic, p.xp, p.dg):
            remote(self.slot(peer), self.slot(peer), self.send.at[self.k, 0], self.recv.at[self.k, peer], ctx=peer).wait_recv()

    def drain(self):
        p = self.p
        for which, peer in enumerate((p.xp, p.dg, p.ic)):
            self.copy(peer, which).wait_send()


class Pair:
    def __init__(self, p, k, src, dst, sems):
        self.p = p
        self.k = k
        self.src = src
        self.dst = dst
        self.send, self.recv = sems

    def slot(self, c):
        rows = self.src.shape[0]
        return self.dst.at[pl.ds(pl.multiple_of(c * rows, rows), rows), :]

    def part(self, c):
        w = self.dst.shape[1]
        if w == self.src.shape[1]:
            return self.src
        return self.src.at[:, pl.ds(at128(c * w), w)]

    def copy(self):
        p = self.p
        return remote(self.part(1 - p.c), self.slot(p.c), self.send.at[self.k], self.recv.at[self.k], ctx=p.ic)

    def start(self):
        c = self.p.c
        self.copy().start()
        self.slot(c)[...] = self.part(c)[...]

    def wait(self):
        p = self.p
        remote(self.part(1 - p.c), self.slot(1 - p.c), self.send.at[self.k], self.recv.at[self.k], ctx=p.ic).wait_recv()

    def drain(self):
        self.copy().wait_send()


class Halves:
    def __init__(self, p, k, src, dst, step, sems):
        self.p = p
        self.k = k
        self.src = src
        self.dst = dst
        self.step = step
        self.send, self.recv = sems

    def slot(self, b):
        rows = self.src.shape[0]
        return self.dst.at[pl.ds(pl.multiple_of(b * rows, rows), rows), :]

    def part(self, x):
        return self.src.at[:, pl.ds(at128(x * self.step), self.dst.shape[1])]

    def to(self, src, slot, which, peer):
        return remote(src, self.slot(slot), self.send.at[self.k, which], self.recv.at[self.k, slot], ctx=peer)

    def start(self):
        p = self.p
        self.to(self.part(1 - p.x), p.b, 0, p.xp).start()
        self.to(self.part(p.x), p.b, 1, p.ic).start()
        self.slot(p.b)[...] = self.src[:, pl.ds(at128(p.x * self.step), self.dst.shape[1])]

    def relay(self):
        p = self.p
        self.to(self.slot(p.xp), p.xp, 2, p.ic).wait_recv()
        self.to(self.slot(p.xp), p.xp, 2, p.ic).start()

    def wait(self):
        p = self.p
        self.to(self.slot(p.ic), p.ic, 1, p.ic).wait_recv()
        self.to(self.slot(p.dg), p.dg, 1, p.ic).wait_recv()

    def drain(self):
        p = self.p
        self.to(self.part(1 - p.x), p.b, 0, p.xp).wait_send()
        self.to(self.part(p.x), p.b, 1, p.ic).wait_send()
        self.to(self.slot(p.xp), p.xp, 2, p.ic).wait_send()


def mega_kernel(n, names, *refs):
    r = SimpleNamespace(**dict(zip(names, refs)))
    p = Place(n)
    z, b, x, c = p.z, p.b, p.x, p.c
    rows_here = r.x.shape[0]
    width = r.x.shape[1]
    half_d = width // 2
    heads = r.wv.shape[1] // HEAD_V
    qk = r.wq.shape[1]
    vw = r.wv.shape[1]
    ff = r.wd.shape[0]
    ffp = r.hid.shape[1]
    order = [s * 256 + cc * 128 for cc in range(2) for s in range(n)]
    blocks = width // 256
    D = r.lsem

    fqkv, fo, fg, fu, fd = r.fqkv, r.fo, r.fg, r.fu, r.fd
    local = []

    def bring(src, dst):
        copy = pltpu.make_async_copy(src, dst, D.at[len(local)])
        copy.start()
        local.append(copy)
        return copy

    get_x = bring(r.x, r.xv)
    need = {}
    for cc in range(2):
        rows = pl.ds(at128((cc * n + z) * 128), 128)
        src = slice(cc * 128, cc * 128 + 128)
        need.setdefault("qkv", []).extend(
            (
                bring(r.wq.at[src, :], fqkv.at[rows, 0:qk]),
                bring(r.wk.at[src, :], fqkv.at[rows, qk : 2 * qk]),
                bring(r.wv.at[src, :], fqkv.at[rows, 2 * qk : 2 * qk + vw]),
            )
        )
    for cc in range(2):
        cols = pl.ds(at128((cc * n + z) * 128), 128)
        need.setdefault("o", []).append(bring(r.wo.at[:, cc * 128 : cc * 128 + 128], fo.at[:, cols]))
    for key, src, dst in (("g", r.wg, fg), ("u", r.wu, fu), ("d", r.wd, fd)):
        for cc in range(2):
            cols = pl.ds(at128((cc * n + z) * 128), 128)
            need.setdefault(key, []).append(bring(src.at[:, cc * 128 : cc * 128 + 128], dst.at[0:ff, cols]))
    get_teacher = bring(r.teacher, r.tv)

    pieces, first = [], []

    def split(total, parts):
        unit = total // 16
        edge = [(unit * i // parts) * 16 for i in range(parts + 1)]
        return [(edge[i], edge[i + 1] - edge[i]) for i in range(parts)]

    for key, ref, kind, total, parts in (
        ("qkv", fqkv, "row", 64, 1),
        ("o", fo, "col", vw // 2, 1),
        ("g", fg, "col", ff // 2, 2),
        ("u", fu, "col", ff // 2, 2),
        ("d", fd, "col", ff // 2, 2),
    ):
        for i, (lo, size) in enumerate(split(total, parts)):
            pieces.append((ref, kind, (lo, ref.shape[1]) if kind == "row" else (lo, total), size))
            first.append(need[key] if i == 0 else [])
    gather = Gather(p, pieces, r.gs)
    ng = len(pieces)

    def own(g):
        for copy in first[g]:
            copy.wait()
        gather.own(g)

    entry_barrier(p)
    own(0)
    own(1)

    r.gains[...] = jnp.concatenate(
        [r.attn_gain[...].astype(F32).reshape(1, -1), r.ffn_gain[...].astype(F32).reshape(1, -1)]
        + [jnp.zeros((6, width // n), F32)],
        axis=0,
    )
    segment = r.segment[...].astype(F32)
    r.segrow[...] = jnp.broadcast_to(segment, (8, rows_here))
    r.segcol[...] = jnp.transpose(jnp.broadcast_to(segment, (128, rows_here)))
    r.valid[...] = jnp.transpose(jnp.broadcast_to(r.real[...].astype(F32), (128, rows_here)))
    gsend, grecv, gath = r.gnsem[0], r.gnsem[1], r.gath
    for s in range(n):

        @pl.when(z != s)
        def _():
            remote(r.gains, gath.at[z], gsend.at[s], grecv.at[z], fsdp=s).start()

    gath[z] = r.gains[...]
    segs, segr = r.segsem[0], r.segsem[1]
    for i, peer in enumerate((p.ic, p.xp, p.dg)):
        remote(r.segrow, r.segall.at[b], segs.at[i], segr.at[b], ctx=peer).start()
    r.segall[b] = r.segrow[...]

    pad = ffp - ff
    if pad:
        for ref in (fg, fu, fd):
            ref[ff:ffp, :] = jnp.zeros((pad, width), BF16)

    for s in range(n):

        @pl.when(z != s)
        def _():
            remote(r.gains, gath.at[s], gsend.at[s], grecv.at[s], fsdp=s).wait_recv()

    for row in range(2):
        r.gain[row : row + 1, :] = jnp.concatenate(
            [gath[s, row : row + 1, cc * 128 : cc * 128 + 128] for cc in range(2) for s in range(n)], axis=1
        )

    events = [(g - 0.7, "own", g, 0) for g in range(2, ng)]
    for g in range(ng):
        for h in range(1, n):
            events.append((g + 0.6 * h, "hop", g, h))
            events.append((g + 0.6 * h + 0.8, "cross", g, h))
    events.sort()
    passed = [0]

    def advance(until):
        while passed[0] < len(events) and events[passed[0]][0] <= until:
            _, kind, g, h = events[passed[0]]
            if kind == "own":
                own(g)
            elif kind == "hop":
                gather.hop(g, h)
            else:
                gather.hop_cross(g, h)
            passed[0] += 1

    def ready(g_from, g_to):
        advance(max(e[0] for e in events if e[1] == "cross" and e[2] < g_to))
        for g in range(g_from, g_to):
            gather.finish(g)

    send_n1 = Pair(p, 0, r.n1, r.n1c, r.psem)
    send_da = Pair(p, 1, r.da, r.dac, r.psem)
    send_dy = Pair(p, 2, r.dy, r.dyc, r.psem)
    send_hid = Pair(p, 3, r.hid, r.hidx, r.psem)
    send_mix = Pair(p, 4, r.mix, r.mixx, r.psem)
    send_dqkv = Pair(p, 5, r.dqkv, r.dqkvx, r.psem)
    send_n2 = Columns(p, 0, r.n2, r.n2c, r.csem)
    fh = r.dgx.shape[1]
    send_dg = Halves(p, 0, r.dg, r.dgx, ffp - fh, r.hsem)
    send_du = Halves(p, 1, r.du, r.dux, ffp - fh, r.hsem)
    ysend, yrecv = r.ysend, r.yrecv

    def y_copy(i, ch):
        return remote(ysend.at[i, ch], yrecv.at[i, ch], r.ysem[0].at[i, ch], r.ysem[1].at[i, ch], tp=1 - p.t)

    def y_put(i, ch, value):
        ysend[i, ch] = value.astype(BF16)
        y_copy(i, ch).start()

    def y_wait(i, between=()):
        for ch in range(blocks):
            y_copy(i, ch).wait_recv()
            if ch < len(between):
                between[ch]()

    def y_rows(i, rs):
        if i == 1:
            parts = [(s, slice(cc * 128, cc * 128 + 128)) for cc in range(2) for s in range(n)]
            return jnp.concatenate(
                [ysend[1, s, rs, at].astype(F32) + yrecv[1, s, rs, at].astype(F32) for s, at in parts], axis=1
            )
        return jnp.concatenate(
            [ysend[i, ch, rs, :].astype(F32) + yrecv[i, ch, rs, :].astype(F32) for ch in range(blocks)], axis=1
        )

    step_rows = 32
    row_steps = rows_here // step_rows

    def per_rows(body):
        @pl.loop(0, row_steps)
        def _(i):
            body(pl.ds(pl.multiple_of(i * step_rows, step_rows), step_rows))

    def x_rows(rs):
        return jnp.concatenate([r.xv[rs, o : o + 128] for o in order], axis=1).astype(F32)

    def rsq(v):
        return lax.rsqrt(jnp.mean(v * v, axis=1, keepdims=True) + EPSILON)

    get_x.wait()

    def norm_one(rs):
        v = x_rows(rs)
        r.n1[rs, :] = (v * rsq(v) * r.gain[0:1, :]).astype(BF16)

    per_rows(norm_one)
    ready(0, 1)
    kv = r.kv
    first_chunk = mm(r.n1[...], fqkv[:, 0 : 2 * qk])
    r.q[...] = first_chunk[:, 0:qk].astype(BF16)
    kv[b, :, 0:qk] = first_chunk[:, qk : 2 * qk].astype(BF16)
    for ch in range(vw // 256):
        lo = ch * 256
        kv[b, :, qk + lo : qk + lo + 256] = mm(r.n1[...], fqkv[:, 2 * qk + lo : 2 * qk + lo + 256]).astype(BF16)

    kvs, kvr = r.kvsem

    def kv_copy(slot, which, peer):
        return remote(kv.at[slot], kv.at[slot], kvs.at[which], kvr.at[slot], ctx=peer)

    @pl.when(x == 0)
    def _():
        kv_copy(b, 0, p.xp).start()

    @pl.when(c == 0)
    def _():
        kv_copy(b, 1, p.ic).start()

    for i, peer in enumerate((p.ic, p.xp, p.dg)):
        remote(r.segrow, r.segall.at[peer], segs.at[i], segr.at[peer], ctx=peer).wait_recv()
    mask, num, den = r.mask, r.num, r.den
    num[...] = jnp.zeros_like(num)
    den[...] = jnp.zeros_like(den)
    lane = lax.broadcasted_iota(jnp.int32, (1, 128), 1)

    def q_of(h):
        keep = (lane // FEAT) == h
        return jnp.where(keep, r.q[...], jnp.zeros((), BF16))

    def attend_block(j):
        same = r.segcol[:, 0:1] == r.segall[j, 0:1, :]
        ri = lax.broadcasted_iota(jnp.int32, (rows_here, rows_here), 0)
        ci = lax.broadcasted_iota(jnp.int32, (rows_here, rows_here), 1)
        reach = ri + jnp.where(j == b, 0, rows_here) >= ci
        mask[j] = jnp.where(same & reach, 1.0, 0.0)

        @pl.loop(0, heads // 2)
        def _(pair):
            at = pl.ds(at128(pair * 128), 128)
            vpair = kv[j, :, pl.ds(at128(qk + pair * 128), 128)]
            sums = []
            for e in range(2):
                s = mm_nt(q_of(pair * 2 + e), kv[j, :, 0:qk]) * 0.25
                w = (1.0 + s + 0.5 * s * s) * mask[j]
                sums.append((mm(w.astype(BF16), vpair), jnp.sum(w, axis=1, keepdims=True)))
            low_half = lane < HEAD_V
            num[:, at] += jnp.where(low_half, sums[0][0], sums[1][0])
            den[:, at] += jnp.where(low_half, sums[0][1], sums[1][1])

    attend_block(b)
    advance(3.3)

    @pl.when(x == 1)
    def _():
        kv_copy(c, 2, p.ic).wait_recv()
        kv_copy(c, 2, p.ic).start()

    @pl.when(c == 1)
    def _():
        kv_copy(p.ic, 1, p.ic).wait_recv()

    @pl.when(x == 1)
    def _():
        kv_copy(1 - c, 2, p.ic).wait_recv()

    for m in range(1, 4):

        @pl.when(b >= m)
        def _():
            attend_block(b - m)

        advance(3.3 + 0.3 * m)

    inv = 1.0 / den[...]
    den[...] = inv
    num[...] = num[...] * inv
    r.mix[...] = num[...].astype(BF16)

    ready(1, 2)
    for ch in range(blocks):
        y_put(0, ch, mm(r.mix[...], fo[:, ch * 256 : ch * 256 + 256]))
    send_mix.start()
    send_n1.start()
    advance(4.5)
    y_wait(0, [lambda u=u: advance(u) for u in (5.0, 5.7, 6.3)])

    def norm_two(rs):
        v = x_rows(rs) + y_rows(0, rs)
        r.mid[rs, :] = v
        r.n2[rs, :] = (v * rsq(v) * r.gain[1:2, :]).astype(BF16)

    per_rows(norm_two)

    red = Reduce(
        p,
        [r.part[i] for i in range(5)],
        [r.seen[i] for i in range(5)],
        [r.out_d, r.out_g, r.out_u, r.out_o, r.out_q],
        [r.other, None, None, None, None],
        r.rsem,
    )
    turned = r.turned

    def turn(src):
        w = src.shape[1]

        @pl.loop(0, src.shape[0] // rows_here)
        def _(i):
            at = pl.ds(pl.multiple_of(i * rows_here, rows_here), rows_here)
            turned[0:w, at] = jnp.transpose(src[at, :])

    def grad_cols(g, rhs):
        rows = r.part[g].shape[1]

        @pl.loop(0, -(-rows // 256))
        def _(i):
            at = pl.ds(at128(jnp.minimum(i * 256, rows - 256)), 256)
            res = mm(turned[at, 0 : rhs.shape[0]], rhs[...]).astype(BF16)
            for s in range(n):
                r.part[g][s, at, :] = res[:, s * 128 : s * 128 + 128]

    fchunks = -(-ffp // 256)

    def per_ff(body):
        @pl.loop(0, fchunks)
        def _(i):
            body(at128(jnp.minimum(i * 256, ffp - 256)))

    ready(2, 6)

    def wide(ref, off):
        return ref[pl.ds(off, 256), :]

    def forward_ff(off):
        g = mm_nt(r.n2[...], wide(fg, off))
        u = mm_nt(r.n2[...], wide(fu, off))
        r.g[:, pl.ds(off, 256)] = g
        r.u[:, pl.ds(off, 256)] = u
        sig = 1.0 / (1.0 + jnp.exp(-g))
        r.hid[:, pl.ds(off, 256)] = (g * sig * u).astype(BF16)

    per_ff(forward_ff)
    send_hid.start()

    def down_block(s):
        for cc in range(2):
            cols = pl.ds(at128((cc * n + s) * 128), 128)
            ysend[1, s, :, cc * 128 : cc * 128 + 128] = mm(r.hid[...], fd[:, cols]).astype(BF16)
        y_copy(1, s).start()

    advance(ng - 1)
    down_block(z)
    for h in range(1, n):
        advance(ng - 1 + 0.6 * h + 0.81)
        for s, there in ((z + h, z + h < n), (z - h, z - h >= 0)):

            @pl.when(there)
            def _():
                for g in range(6, ng):
                    gather.whole(g, s)
                down_block(s)

    advance(2 * ng)
    send_n2.start()
    get_teacher.wait()
    small = r.small
    small[...] = jnp.zeros_like(small)
    send_hid.wait()
    turn(r.hidx)
    y_wait(1)

    def finish_forward(rs):
        y = r.mid[rs, :] + y_rows(1, rs)
        t = jnp.concatenate([r.tv[rs, o : o + 128] for o in order], axis=1).astype(F32)
        m = (y - t) * r.valid[rs, 0:1]
        r.mis[rs, :] = m
        r.dy[rs, :] = m.astype(BF16)
        yb = y.astype(BF16)
        for i, o in enumerate(order):
            r.layer_out[rs, o : o + 128] = yb[:, i * 128 : i * 128 + 128]
        small[2:3, :] += jnp.sum(m * m, axis=0, keepdims=True)
        small[3:4, :] += jnp.broadcast_to(jnp.sum(r.valid[rs, :], axis=0, keepdims=True)[:, 0:1], (1, width))

    per_rows(finish_forward)
    send_dy.start()

    def backward_ff(off):
        dh = mm_nt(r.dy[...], fd[pl.ds(off, 256), :])
        g = r.g[:, pl.ds(off, 256)]
        u = r.u[:, pl.ds(off, 256)]
        sig = 1.0 / (1.0 + jnp.exp(-g))
        r.dg[:, pl.ds(off, 256)] = (dh * u * sig * (1.0 + g * (1.0 - sig))).astype(BF16)
        r.du[:, pl.ds(off, 256)] = (dh * g * sig).astype(BF16)

    per_ff(backward_ff)
    send_dg.start()
    send_du.start()
    send_dy.wait()
    grad_cols(0, r.dyc)
    red.stage(0, 0)
    for ch in range(blocks):
        cols = slice(ch * 256, ch * 256 + 256)
        y_put(2, ch, mm(r.dg[...], fg[:, cols]) + mm(r.du[...], fu[:, cols]))

    send_dg.relay()

    y_wait(2)

    def norm_back(i, row, v, base, rs):
        dn = y_rows(i, rs)
        inv_root = rsq(v)
        w = dn * r.gain[row : row + 1, :]
        small[row : row + 1, :] += jnp.sum(dn * v * inv_root, axis=0, keepdims=True)
        m = jnp.mean(w * v, axis=1, keepdims=True)
        return base + inv_root * w - v * (inv_root * inv_root * inv_root * m)

    def middle_back(rs):
        d = norm_back(2, 1, r.mid[rs, :], r.mis[rs, :], rs)
        r.mis[rs, :] = d
        r.da[rs, :] = d.astype(BF16)

    per_rows(middle_back)
    send_da.start()
    send_n2.wait()
    send_dg.wait()
    turn(r.dgx)
    grad_cols(1, r.n2c)
    red.stage(1, 0)

    dnum, dden = r.dnum, r.dden
    for ch in range(vw // 256):
        at = slice(ch * 256, ch * 256 + 256)
        d = mm_nt(r.da[...], fo[at, :]) * den[:, at]
        dnum[:, at] = d.astype(BF16)
        dden[:, at] = d * num[:, at]
    send_du.relay()
    send_da.wait()
    send_mix.wait()
    turn(r.mixx)

    def out_half(dst, xx):
        rows = vw // 2
        res = mm(turned[pl.ds(pl.multiple_of(xx * rows, 128), rows), 0 : 2 * rows_here], r.dac[...]).astype(BF16)
        for s in range(n):
            dst[s] = res[:, s * 128 : s * 128 + 128]

    def halve(i, g, make):
        give, got = r.give[i], r.got[i]
        make(give, 1 - x)
        half_copy(i).start()
        make(r.part[g], x)

    def half_copy(i):
        return remote(r.give[i], r.got[i], r.presem[0].at[i], r.presem[1].at[i], ctx=p.xp)

    def joined(i, g):
        half_copy(i).wait_recv()
        for s in range(n):
            r.part[g][s] = (r.part[g][s].astype(F32) + r.got[i][s].astype(F32)).astype(BF16)

    halve(0, 3, out_half)
    dkvp, dkv, dq = r.dkvp, r.dkv, r.dqf
    dq[...] = jnp.zeros_like(dq)

    def back_block(j):
        dkv[...] = jnp.zeros_like(dkv)

        @pl.loop(0, heads // 2)
        def _(pair):
            at = pl.ds(at128(pair * 128), 128)
            vat = pl.ds(at128(qk + pair * 128), 128)
            dv = []
            for e in range(2):
                h = pair * 2 + e
                qh = q_of(h)
                keep_v = (lane // HEAD_V) == e
                keep_q = (lane // FEAT) == h
                s = mm_nt(qh, kv[j, :, 0:qk]) * 0.25
                w = ((1.0 + s + 0.5 * s * s) * mask[j]).astype(BF16)
                dn = jnp.where(keep_v, dnum[:, at], jnp.zeros((), BF16))
                dd = jnp.sum(jnp.where(keep_v, dden[:, at], 0.0), axis=1, keepdims=True)
                dw = mm_nt(dn, kv[j, :, vat]) - dd
                ds = (dw * (1.0 + s) * (0.25 * mask[j])).astype(BF16)
                dv.append(mm_tn(w, dn))
                kh = jnp.where(keep_q, kv[j, :, 0:qk], jnp.zeros((), BF16))
                dq[...] += mm(ds, kh)
                dkv[:, 0:qk] += mm_tn(ds, qh)
            dkv[:, vat] = dv[0] + dv[1]

    @pl.loop(0, b)
    def _(j):
        back_block(j)
        dkvp[j] = dkv[...].astype(BF16)

    red.stage(0, 1)
    dks, dkr = r.dksem
    back = r.back

    def dk_copy(src, slot, which, peer):
        return remote(src, back.at[slot], dks.at[which], dkr.at[slot], ctx=peer)

    @pl.when(c == 1)
    def _():
        dk_copy(dkvp.at[p.ic], 0, 0, p.ic).start()

    @pl.when(x == 1)
    def _():
        dk_copy(dkvp.at[1 - c], 1, 1, p.ic).start()

    @pl.when(x == 1)
    def _():
        dk_copy(dkvp.at[1 - c], 1, 1, p.ic).wait_recv()
        dkvp[b] = (dkvp[c].astype(F32) + back[1].astype(F32)).astype(BF16)
        dk_copy(dkvp.at[b], 2, 2, p.xp).start()

    send_du.wait()
    turn(r.dux)
    grad_cols(2, r.n2c)
    red.stage(2, 0)
    back_block(b)

    @pl.when(c == 0)
    def _():
        dk_copy(dkvp.at[b], 0, 0, p.ic).wait_recv()
        dkv[...] += back[0].astype(F32)

    dqkv = r.dqkv
    dqkv[:, 0:qk] = dq[...].astype(BF16)
    joined(0, 3)
    red.stage(3, 0)
    red.stage(1, 1)

    @pl.when(x == 0)
    def _():
        dk_copy(dkvp.at[b], 2, 2, p.xp).wait_recv()
        dkv[...] += back[2].astype(F32)

    dqkv[:, qk : 2 * qk + vw] = dkv[...].astype(BF16)
    send_dqkv.start()
    for ch in range(blocks):
        y_put(3, ch, mm_nt(dqkv[...], fqkv[ch * 256 : ch * 256 + 256, :]))
    send_n1.wait()
    turn(r.n1c)
    send_dqkv.wait()

    def qkv_half(dst, xx):
        cols = (2 * qk + vw) // 2
        rhs = r.dqkvx[:, pl.ds(at128(xx * cols), cols)]
        res = mm(turned[0:half_d, 0 : 2 * rows_here], rhs).astype(BF16)
        for s in range(n):
            dst[s] = res[s * 128 : s * 128 + 128, :]

    halve(1, 4, qkv_half)
    red.stage(0, 2)
    joined(1, 4)
    red.stage(4, 0)
    red.stage(2, 1)
    red.last(0)

    y_wait(3)

    def input_back(rs):
        d = norm_back(3, 0, x_rows(rs), r.mis[rs, :], rs).astype(BF16)
        for i, o in enumerate(order):
            r.grad_in[rs, o : o + 128] = d[:, i * 128 : i * 128 + 128]

    per_rows(input_back)

    sms, smr = r.smsem
    parts, lines = r.smctx, r.smz
    for i, peer in enumerate((p.ic, p.xp, p.dg)):
        remote(small, parts.at[b], sms.at[0, i], smr.at[0, b], ctx=peer).start()
    parts[b] = small[...]
    red.stage(3, 1)
    red.stage(1, 2)
    for i, peer in enumerate((p.ic, p.xp, p.dg)):
        remote(small, parts.at[peer], sms.at[0, i], smr.at[0, peer], ctx=peer).wait_recv()
    lines[n] = parts[0] + parts[1] + parts[2] + parts[3]
    for s in range(n):

        @pl.when(z != s)
        def _():
            remote(lines.at[n], lines.at[z], sms.at[1, s], smr.at[1, z], fsdp=s).start()

    red.last(1)
    red.stage(4, 1)
    red.stage(2, 2)
    red.last(2)
    red.relay(0)
    red.stage(3, 2)
    red.last(3)
    red.stage(4, 2)
    red.relay(1)
    red.last(4)
    red.relay(2)
    red.relay(3)
    red.relay(4)
    for s in range(n):

        @pl.when(z != s)
        def _():
            remote(lines.at[n], lines.at[s], sms.at[1, s], smr.at[1, s], fsdp=s).wait_recv()

    total = jnp.zeros_like(small)
    for s in range(n):
        total += jnp.where(z == s, lines[n], lines[s])
    r.gain[...] = total
    for cc in range(2):
        at = pl.ds(at128((cc * n + z) * 128), 128)
        r.grad_attn[0:1, cc * 128 : cc * 128 + 128] = r.gain[0:1, at]
        r.grad_ffn[0:1, cc * 128 : cc * 128 + 128] = r.gain[1:2, at]
    r.loss[...] = jnp.sum(total[2:3, :], axis=1, keepdims=True) / (total[3:4, 0:1] * width)
    for g in (4, 0, 1, 2, 3):
        red.finish(g)
        if g == 4:
            r.grad_q[...] = r.out_q[:, 0:qk].astype(F32)
            r.grad_k[...] = r.out_q[:, qk : 2 * qk].astype(F32)
            r.grad_v[...] = r.out_q[:, 2 * qk : 2 * qk + vw].astype(F32)

    for i in range(2):
        half_copy(i).wait_send()
    gather.drain()
    for k in (send_n1, send_da, send_n2, send_dy, send_hid, send_dg, send_du, send_mix, send_dqkv):
        k.drain()
    for i in range(4):
        for ch in range(blocks):
            y_copy(i, ch).wait_send()
    for s in range(n):

        @pl.when(z != s)
        def _():
            remote(r.gains, gath.at[z], gsend.at[s], grecv.at[z], fsdp=s).wait_send()
            remote(lines.at[n], lines.at[z], sms.at[1, s], smr.at[1, z], fsdp=s).wait_send()

    for i, peer in enumerate((p.ic, p.xp, p.dg)):
        remote(r.segrow, r.segall.at[b], segs.at[i], segr.at[b], ctx=peer).wait_send()
        remote(small, parts.at[b], sms.at[0, i], smr.at[0, b], ctx=peer).wait_send()

    @pl.when(x == 0)
    def _():
        kv_copy(b, 0, p.xp).wait_send()

    @pl.when(c == 0)
    def _():
        kv_copy(b, 1, p.ic).wait_send()

    @pl.when(x == 1)
    def _():
        kv_copy(c, 2, p.ic).wait_send()
        dk_copy(dkvp.at[1 - c], 1, 1, p.ic).wait_send()
        dk_copy(dkvp.at[b], 2, 2, p.xp).wait_send()

    @pl.when(c == 1)
    def _():
        dk_copy(dkvp.at[p.ic], 0, 0, p.ic).wait_send()


def mega(n, layer_in, segment_ids, valid_mask, teacher, attn_gain, w_query, w_key, w_value, w_out, ffn_gain, w_gate, w_up, w_down):
    x = layer_in[0]
    rows, width = x.shape
    qk, vw, ff = w_query.shape[1], w_value.shape[1], w_gate.shape[1]
    ffp = up_to(ff, 128)
    fh = up_to(ffp // 2, 256)
    half_d = width // 2
    blocks = width // 256
    inputs = dict(
        x=x,
        teacher=teacher[0],
        wq=w_query,
        wk=w_key,
        wv=w_value,
        wo=w_out,
        wg=w_gate.T,
        wu=w_up.T,
        wd=w_down,
        attn_gain=attn_gain,
        ffn_gain=ffn_gain,
        segment=segment_ids,
        real=valid_mask,
    )
    hbm = list(inputs)[:9]
    outs = dict(
        layer_out=((rows, width), BF16),
        grad_in=((rows, width), BF16),
        out_d=((ffp, width // n), BF16),
        out_g=((ffp, width // n), BF16),
        out_u=((ffp, width // n), BF16),
        out_o=((vw, width // n), BF16),
        grad_q=((width // n, qk), F32),
        grad_k=((width // n, qk), F32),
        grad_v=((width // n, vw), F32),
        grad_attn=((1, width // n), F32),
        grad_ffn=((1, width // n), F32),
        loss=((1, 1), F32),
    )
    dma = pltpu.SemaphoreType.DMA
    ng = 8
    vm = pltpu.VMEM
    piece = [(ffp, 128), (fh, 128), (fh, 128), (vw // 2, 128), (128, (2 * qk + vw) // 2)]
    scratch = dict(
        lsem=dma((20,)),
        gs=[dma((ng, n)) for _ in range(9)],
        gnsem=[dma((n,)), dma((n,))],
        segsem=[dma((3,)), dma((4,))],
        psem=[dma((6,)), dma((6,))],
        csem=[dma((1, 3)), dma((1, 4))],
        hsem=[dma((2, 3)), dma((2, 4))],
        ysem=[dma((4, blocks)), dma((4, blocks))],
        kvsem=[dma((3,)), dma((4,))],
        dksem=[dma((3,)), dma((3,))],
        rsem=[dma((5, n)), dma((5, n + 1)), dma((5, 3)), dma((5, 4))],
        smsem=[dma((2, max(n, 3))), dma((2, max(n, 4)))],
        fqkv=vm((width, 2 * qk + vw), BF16),
        fo=vm((vw, width), BF16),
        fg=vm((ffp, width), BF16),
        fu=vm((ffp, width), BF16),
        fd=vm((ffp, width), BF16),
        xv=vm((rows, width), BF16),
        tv=vm((rows, width), BF16),
        gath=vm((n, 8, width // n), F32),
        gain=vm((8, width), F32),
        gains=vm((8, width // n), F32),
        segrow=vm((8, rows), F32),
        segcol=vm((rows, 128), F32),
        valid=vm((rows, 128), F32),
        segall=vm((4, 8, rows), F32),
        n1=vm((rows, width), BF16),
        n2=vm((rows, width), BF16),
        dy=vm((rows, width), BF16),
        da=vm((rows, width), BF16),
        n1c=vm((2 * rows, half_d), BF16),
        n2c=vm((4 * rows, half_d), BF16),
        dyc=vm((2 * rows, half_d), BF16),
        dac=vm((2 * rows, half_d), BF16),
        hid=vm((rows, ffp), BF16),
        dg=vm((rows, ffp), BF16),
        du=vm((rows, ffp), BF16),
        mix=vm((rows, vw), BF16),
        dqkv=vm((rows, 2 * qk + vw), BF16),
        hidx=vm((2 * rows, ffp), BF16),
        dgx=vm((4 * rows, fh), BF16),
        dux=vm((4 * rows, fh), BF16),
        mixx=vm((2 * rows, vw), BF16),
        dqkvx=vm((2 * rows, 2 * qk + vw), BF16),
        ysend=vm((4, max(blocks, n), rows, 256), BF16),
        yrecv=vm((4, blocks, rows, 256), BF16),
        q=vm((rows, qk), BF16),
        kv=vm((4, rows, qk + vw), BF16),
        mask=vm((4, rows, rows), F32),
        num=vm((rows, vw), F32),
        den=vm((rows, vw), F32),
        mid=vm((rows, width), F32),
        mis=vm((rows, width), F32),
        g=vm((rows, ffp), F32),
        u=vm((rows, ffp), F32),
        small=vm((8, width), F32),
        smctx=vm((4, 8, width), F32),
        smz=vm((n + 1, 8, width), F32),
        dnum=vm((rows, vw), BF16),
        dden=vm((rows, vw), F32),
        dqf=vm((rows, qk), F32),
        dkv=vm((rows, qk + vw), F32),
        dkvp=vm((4, rows, qk + vw), BF16),
        back=vm((3, rows, qk + vw), BF16),
        turned=vm((max(ffp, half_d), 4 * rows), BF16),
        part=[vm((n,) + s, BF16) for s in piece],
        seen=[vm((n + 1,) + s, BF16) for s in piece],
        other=vm(piece[0], BF16),
        give=[vm((n,) + piece[i], BF16) for i in (3, 4)],
        got=[vm((n,) + piece[i], BF16) for i in (3, 4)],
        presem=[dma((2,)), dma((2,))],
        out_q=vm((width // n, 2 * qk + vw), BF16),
    )
    flat, layout = [], []
    for k, v in scratch.items():
        if isinstance(v, list):
            layout.append((k, len(v)))
            flat.extend(v)
        else:
            layout.append((k, 0))
            flat.append(v)

    def kernel(*refs):
        names = list(inputs) + list(outs)
        bound = list(refs[: len(names)])
        at = len(names)
        for k, count in layout:
            names.append(k)
            if count:
                bound.append(refs[at : at + count])
                at += count
            else:
                bound.append(refs[at])
                at += 1
        mega_kernel(n, names, *bound)

    res = pl.pallas_call(
        kernel,
        out_shape=[jax.ShapeDtypeStruct(*v) for v in outs.values()],
        in_specs=[pl.BlockSpec(memory_space=pl.ANY if k in hbm else pltpu.VMEM) for k in inputs],
        out_specs=[pl.BlockSpec(memory_space=pltpu.VMEM)] * len(outs),
        scratch_shapes=flat,
        compiler_params=pltpu.CompilerParams(
            collective_id=0, has_side_effects=True, vmem_limit_bytes=67043328
        ),
        name="block_step",
    )(*inputs.values())
    o = SimpleNamespace(**dict(zip(outs, res)))

    return (
        o.layer_out[None],
        o.grad_in[None],
        o.grad_attn[0],
        o.grad_q,
        o.grad_k,
        o.grad_v,
        o.out_o.astype(F32),
        o.grad_ffn[0],
        o.out_g[:ff].astype(F32).T,
        o.out_u[:ff].astype(F32).T,
        o.out_d[:ff].astype(F32),
        o.loss[0, 0],
    )


def per_device(*arrays):
    n = lax.axis_size("fsdp")
    layer_in, w_query, w_value = arrays[0], arrays[5], arrays[7]
    fits = (
        lax.axis_size("ctx") == 4
        and lax.axis_size("tp") == 2
        and layer_in.shape[0] == 1
        and w_query.shape[0] == 256
        and w_query.shape[1] == 128
        and w_value.shape[1] % 512 == 0
        and layer_in.shape[1] % 256 == 0
    )
    return mega(n, *arrays) if fits else general(*arrays)


def solution(mesh):
    placed = (
        P("fsdp", "ctx", None),
        P("fsdp", "ctx"),
        P("fsdp", "ctx"),
        P("fsdp", "ctx", None),
        P("fsdp"),
        P("fsdp", "tp"),
        P("fsdp", "tp"),
        P("fsdp", "tp"),
        P("tp", "fsdp"),
        P("fsdp"),
        P("fsdp", "tp"),
        P("fsdp", "tp"),
        P("tp", "fsdp"),
    )
    return jax.shard_map(
        per_device,
        mesh=mesh,
        in_specs=placed,
        out_specs=(
            P("fsdp", "ctx", None),
            P("fsdp", "ctx", None),
            P("fsdp"),
            P("fsdp", "tp"),
            P("fsdp", "tp"),
            P("fsdp", "tp"),
            P("tp", "fsdp"),
            P("fsdp"),
            P("fsdp", "tp"),
            P("fsdp", "tp"),
            P("tp", "fsdp"),
            P(),
        ),
        check_vma=False,
    )
```
